1024 devices in a mesh: pipe: 8 (over z), dp: 4 (over x_lo, core), expert: 32 (over y, x_hi).
Axes of the slice: x: 8 (x_hi: 4, x_lo: 2; x = x_hi * 2 + x_lo), y: 8, z: 8, core: 2. Of those that a mesh axis runs over, the one named last changes fastest.
Arguments:
- cotangent: bfloat16 [8, 8192, 7168], P('pipe', ('dp', 'expert')), may hold values from -6 to 6
- routes: int32 [8, 2, 8192, 8], P('pipe', None, ('dp', 'expert')), may hold values from 0 to 255, as said below
- gates: bfloat16 [8, 2, 8192, 8], P('pipe', None, ('dp', 'expert')), may hold values from 0.099609375 to 1
- gate_pre: bfloat16 [8, 2, 4, 32, 2, 4096], P('pipe', None, 'dp', None, None, 'expert'), may hold values from -6 to 6
- up_pre: bfloat16 [8, 2, 4, 32, 2, 4096], P('pipe', None, 'dp', None, None, 'expert'), may hold values from -6 to 6
- w_gate: bfloat16 [8, 7168, 4096], P('pipe', None, 'expert'), may hold values from -0.0625 to 0.0625
- w_up: bfloat16 [8, 7168, 4096], P('pipe', None, 'expert'), may hold values from -0.0625 to 0.0625
- w_down: bfloat16 [8, 4096, 7168], P('pipe', 'expert'), may hold values from -0.125 to 0.125
Outputs:
- down_grad: float32 [8, 4096, 7168], P('pipe', 'expert', 'dp')
The draws below stay inside these ranges and needn't reach their ends.
Inputs may be any that keep to these rules, and one draw needn't show every extreme that they name: `routes`: each token names 8 different experts. At one section and step the tokens of one device name each of the experts 0 to 1 at least once and at most 2 times; at every section and step, in some replica every device names one of them exactly 2 times.
All inputs are finite; a program needn't handle non-finite values.
Results may differ from the reference program's by a relative error of at most 0.0095.
Values may be sent and summed in bfloat16 or wider, within the bound.
A program may use at most 64 MiB of HBM per device.

```python
import math
import jax
import jax.numpy as jnp
from jax import lax

D = 7168
FFE = 2048
EXPERTS = 256
TOPK = 8
EXP_FL = 2
STEPS = 2
TOK_DEV = 64
CAP = 2
TOKENS = 8192
N_PIPE = 8
N_DP = 4
N_EXPERT = 32


def draw_routes(key, part):
    keys = jax.random.split(key, 6)
    lead = (N_PIPE, STEPS, N_DP, N_EXPERT)
    counts = jax.random.randint(keys[0], lead + (EXP_FL,), 1, CAP + 1)
    full_rep = jax.random.randint(keys[1], (N_PIPE, STEPS, 1, 1, 1), 0, N_DP)
    full_exp = jax.random.randint(keys[2], (N_PIPE, STEPS, 1, 1, 1), 0, EXP_FL)
    rep_index = jnp.arange(N_DP).reshape(1, 1, N_DP, 1, 1)
    exp_index = jnp.arange(EXP_FL).reshape(1, 1, 1, 1, EXP_FL)
    counts = jnp.where((rep_index == full_rep) & (exp_index == full_exp), CAP, counts)
    scores = jax.random.randint(keys[3], lead + (EXP_FL, TOK_DEV), 0, 1 << 20) * TOK_DEV + jnp.arange(TOK_DEV)
    ranking = jnp.argsort(jnp.argsort(scores, axis=-1), axis=-1)
    chosen = ranking < counts[..., None]
    chosen = jnp.moveaxis(chosen, -2, -1)
    others = jax.random.randint(keys[4], lead + (TOK_DEV, EXPERTS - EXP_FL), 0, 1 << 16) * EXPERTS + jnp.arange(EXPERTS - EXP_FL)
    picked = lax.top_k(others, TOPK)[1] + EXP_FL
    head = jnp.where(chosen, jnp.arange(EXP_FL), picked[..., :EXP_FL])
    named = jnp.concatenate([head, picked[..., EXP_FL:]], axis=-1)
    order = jax.random.randint(keys[5], lead + (TOK_DEV, TOPK), 0, 1 << 20) * TOPK + jnp.arange(TOPK)
    shuffle = jnp.argsort(order, axis=-1)
    named = jnp.take_along_axis(named, shuffle, axis=-1)
    return named.reshape(N_PIPE, STEPS, N_DP * N_EXPERT * TOK_DEV, TOPK).astype(jnp.int32)


def steps_of(own_key, shape, cuts, least, largest):
    def one(axis_at, shards_of):
        heights = jax.random.uniform(jax.random.fold_in(jax.random.fold_in(own_key, 6), axis_at), (shards_of,), jnp.float32, least / len(cuts), largest / len(cuts))
        return jnp.repeat(jnp.exp(heights), shape[axis_at] // shards_of).reshape((-1,) + (1,) * (len(shape) - axis_at - 1))

    level = one(*cuts[0])
    for cut in cuts[1:]:
        level = level * one(*cut)
    return level


def scatter_about(rng, dims, scale, reach, pieces=(), held_as=jnp.bfloat16):
    entries = scale * jax.random.normal(rng, dims, jnp.float32)
    if pieces:
        entries = entries * steps_of(rng, dims, pieces, -0.22, 0.18)
    return jnp.clip(entries, -reach, reach).astype(held_as)


def setup_inputs(seed: int = 0) -> dict:
    arg_keys = jax.random.split(jax.random.key(seed), 9)
    cotangent = scatter_about(arg_keys[0], (N_PIPE, TOKENS, D), 1.0, 6.0, ((0, 8), (1, 128)))
    routes = draw_routes(jax.random.fold_in(arg_keys[8], 71), 0)
    gates = jnp.clip(jnp.exp(math.log(1.0) - 2.306499 * jax.random.uniform(arg_keys[2], (N_PIPE, STEPS, TOKENS, TOPK), jnp.float32) ** steps_of(arg_keys[2], (N_PIPE, STEPS, TOKENS, TOPK), ((0, 8), (2, 128)), -0.2, 0.2)), 0.099609375, 1.0).astype(jnp.bfloat16)
    gate_pre = scatter_about(arg_keys[3], (N_PIPE, STEPS, N_DP, N_EXPERT, CAP, EXP_FL * FFE), 1.0, 6.0, ((0, 8), (2, 4), (5, 32)))
    up_pre = scatter_about(arg_keys[4], (N_PIPE, STEPS, N_DP, N_EXPERT, CAP, EXP_FL * FFE), 1.0, 6.0, ((0, 8), (2, 4), (5, 32)))
    w_gate = scatter_about(arg_keys[5], (N_PIPE, D, EXP_FL * FFE), D ** -0.5, 0.0625, ((0, 8), (2, 32)))
    w_up = scatter_about(arg_keys[6], (N_PIPE, D, EXP_FL * FFE), D ** -0.5, 0.0625, ((0, 8), (2, 32)))
    w_down = scatter_about(arg_keys[7], (N_PIPE, EXP_FL * FFE, D), FFE ** -0.5, 0.125, ((0, 8), (1, 32)))
    return {"cotangent": cotangent, "routes": routes, "gates": gates, "gate_pre": gate_pre, "up_pre": up_pre, "w_gate": w_gate, "w_up": w_up, "w_down": w_down}


def slot_tables(ids, weights):
    match = (ids[..., None] == jnp.arange(EXP_FL, dtype=jnp.int32)).astype(jnp.float32)
    hit = jnp.sum(match, axis=2)
    gate_sum = jnp.sum(match * weights.astype(jnp.float32)[..., None, None].reshape(match.shape[:3] + (1,)), axis=2)
    rank = jnp.cumsum(hit, axis=1) - 1.0
    slots = jnp.arange(CAP, dtype=jnp.float32)
    select = hit[..., None] * (rank[..., None] == slots).astype(jnp.float32)
    select = jnp.transpose(select, (0, 2, 3, 1))
    slot_gate = jnp.einsum('bect,bte->bec', select, gate_sum)
    return select, slot_gate


def reference(cotangent, routes, gates, gate_pre, up_pre, w_gate, w_up, w_down):
    blocks = N_DP * N_EXPERT
    split = N_EXPERT // EXP_FL
    hidden = FFE // split
    state = cotangent
    total = jnp.zeros((N_PIPE, EXP_FL * FFE, D), jnp.float32)
    for step in range(STEPS):
        produced = []
        for section in range(N_PIPE):
            grad_in = state[section].reshape(blocks, TOK_DEV, D)
            ids = routes[section, step].reshape(blocks, TOK_DEV, TOPK)
            weights = gates[section, step].reshape(blocks, TOK_DEV, TOPK)
            select, slot_gate = slot_tables(ids, weights)
            rows = jnp.einsum('bect,btd->becd', select, grad_in.astype(jnp.float32)).astype(jnp.bfloat16)
            grad_out = grad_in.astype(jnp.float32)
            pre_gate_all = gate_pre[section, step].reshape(blocks * CAP, EXP_FL * FFE)
            pre_up_all = up_pre[section, step].reshape(blocks * CAP, EXP_FL * FFE)
            for expert in range(EXP_FL):
                lower = expert * FFE
                flat_rows = rows[:, expert].reshape(blocks * CAP, D)
                gate_col = slot_gate[:, expert].reshape(blocks * CAP, 1)
                pre_u = pre_gate_all[:, lower:lower + FFE].astype(jnp.float32)
                pre_v = pre_up_all[:, lower:lower + FFE].astype(jnp.float32)
                down_rows = w_down[section, lower:lower + FFE]
                grad_act = gate_col * jnp.dot(flat_rows, down_rows.T, preferred_element_type=jnp.float32)
                sig = jax.nn.sigmoid(pre_u)
                act = pre_u * sig
                dsilu = sig * (1.0 + pre_u * (1.0 - sig))
                d_gate = (grad_act * pre_v * dsilu).astype(jnp.bfloat16)
                d_up = (grad_act * act).astype(jnp.bfloat16)
                scaled = (gate_col * act * pre_v).astype(jnp.bfloat16)
                term = jnp.dot(scaled.T, flat_rows, preferred_element_type=jnp.float32)
                total = total.at[section, lower:lower + FFE].add(term)
                if step + 1 < STEPS:
                    gate_cols = w_gate[section][:, lower:lower + FFE].reshape(D, split, hidden).astype(jnp.float32)
                    up_cols = w_up[section][:, lower:lower + FFE].reshape(D, split, hidden).astype(jnp.float32)
                    dg = d_gate.reshape(blocks * CAP, split, hidden).astype(jnp.float32)
                    du = d_up.reshape(blocks * CAP, split, hidden).astype(jnp.float32)
                    parts = jnp.einsum('rjh,djh->jrd', dg, gate_cols) + jnp.einsum('rjh,djh->jrd', du, up_cols)
                    parts = parts.astype(jnp.bfloat16).astype(jnp.float32)
                    summed = jnp.sum(parts, axis=0).reshape(blocks, CAP, D)
                    grad_out = grad_out + jnp.einsum('bct,bcd->btd', select[:, expert], summed)
            produced.append(grad_out.astype(jnp.bfloat16).reshape(TOKENS, D))
        if step + 1 < STEPS:
            state = jnp.stack(produced[1:] + [jnp.zeros((TOKENS, D), jnp.bfloat16)])
    return total
```

```python
import functools

import jax
import jax.numpy as jnp
from jax import lax
from jax.experimental import pallas as pl
from jax.experimental.pallas import tpu as pltpu
from jax.sharding import PartitionSpec as P

MESH = pl.DeviceIdType.MESH
BF = jnp.bfloat16
F32 = jnp.float32

D = 7168
TOK = 64
HID = 128
Q = 1792
H = 896
FAR = (4, 3, 5, 2, 6, 1, 7)
ROW = tuple((dx, dc) for dx in FAR for dc in (0, 1)) + ((0, 1),)


def dot(a, b, dims):
    return lax.dot_general(a, b, (dims, ((), ())), preferred_element_type=F32)


def one_hot_rows(source):
    i = lax.broadcasted_iota(jnp.int32, (128, 128), 0)
    j = lax.broadcasted_iota(jnp.int32, (128, 128), 1)
    return (source(i) == j).astype(F32).astype(BF)


def kernel(
    cot, routes, gates, gate_pre, up_pre, w_gate, w_up, w_down, out,
    g_v, ids_v, gat_v, w2, w13, sel_s, sel_in, rows_a, rows_b, base_v, m_out, uv, coef, perm, avt,
    xa, a2, yb, b2, ha, hb, dx, pa, pb, ra1, rb1, ta, tb, ra2, rb2, za, zb,
    ld, s_send, r_xa, r_yb, r_ha, r_hb, r_dx, r_ra1, r_rb1, r_ra2, r_rb2, r_uv, r_sel, r_base,
):
    p = lax.axis_index("pipe")
    r = lax.axis_index("dp")
    s = lax.axis_index("expert")
    y = s // 4
    x = (s % 4) * 2 + r // 2
    c = r % 2

    def dev(p_, x_, y_, c_):
        return (p_, (x_ % 2) * 2 + c_, y_ * 4 + x_ // 2)

    sends = []

    def send(src, dst, recv, target, like, when=None):
        k = len(sends)
        sends.append((like, when))
        pltpu.make_async_remote_copy(
            src_ref=src, dst_ref=dst, send_sem=s_send.at[k], recv_sem=recv, device_id=target, device_id_type=MESH
        ).start()

    def arrived(dst, recv):
        pltpu.make_async_copy(dst, dst, recv).wait()

    up = (p + 1) % 8
    down = (p + 7) % 8

    q0 = pl.multiple_of(r * Q, 128)
    loads = [
        pltpu.make_async_copy(routes.at[0], ids_v, ld.at[0]),
        pltpu.make_async_copy(gates.at[0], gat_v, ld.at[1]),
        pltpu.make_async_copy(cot.at[0], g_v, ld.at[2]),
        pltpu.make_async_copy(w_down.at[0, :, pl.ds(q0, Q)], w2, ld.at[3]),
        pltpu.make_async_copy(w_gate.at[0, pl.ds(q0, Q)], w13.at[:, 0:HID], ld.at[4]),
        pltpu.make_async_copy(w_up.at[0, pl.ds(q0, Q)], w13.at[:, HID : 2 * HID], ld.at[5]),
        pltpu.make_async_copy(gate_pre.at[0, :, 0], uv.at[r, 0], ld.at[6]),
        pltpu.make_async_copy(up_pre.at[0, :, 0], uv.at[r, 1], ld.at[7]),
    ]
    for cp in loads:
        cp.start()

    barrier = pltpu.get_barrier_semaphore()
    peers = [((x + dx_) % 8, y, (c + dc) % 2, p) for dx_, dc in ROW]
    peers += [(x, (y + dy) % 8, c, p) for dy in FAR]
    peers += [(x, y, c, up), (x, y, c, down)]
    for x_, y_, c_, p_ in peers:
        pl.semaphore_signal(barrier, inc=1, device_id=dev(p_, x_, y_, c_), device_id_type=MESH)

    loads[0].wait()
    loads[1].wait()
    lane = lax.broadcasted_iota(jnp.int32, (TOK, 128), 1)
    tri = (
        lax.broadcasted_iota(jnp.int32, (TOK, TOK), 0) >= lax.broadcasted_iota(jnp.int32, (TOK, TOK), 1)
    ).astype(F32).astype(BF)
    for t in range(2):
        ids = ids_v[t]
        gat = gat_v[t].astype(F32)
        hit = jnp.zeros((TOK, 128), F32)
        gsum = jnp.zeros((TOK, 128), F32)
        for e in range(2):
            match = (ids == e).astype(F32)
            mine = (lane >= 2 * e) & (lane < 2 * e + 2)
            hit = jnp.where(mine, jnp.sum(match, axis=1, keepdims=True), hit)
            gsum = jnp.where(mine, jnp.sum(match * gat, axis=1, keepdims=True), gsum)
        rank = dot(tri, hit.astype(BF), ((1,), (0,))) - 1.0
        slot = (lane & 1).astype(F32)
        sel = hit * (rank == slot).astype(F32)
        if t == 0:
            sel_s[0] = sel.astype(BF)
        sel_s[1 + t] = (sel * gsum).astype(BF)

    def put_rows(rows):
        for e in range(2):
            for q in range(4):
                rows_a[0, q, e] = rows[2 * e : 2 * e + 2, q * Q : q * Q + H].astype(BF)
                rows_b[0, e, :, q * H : (q + 1) * H] = rows[2 * e : 2 * e + 2, q * Q + H : (q + 1) * Q].astype(BF)

    loads[2].wait()
    put_rows(dot(sel_s[1], g_v[...], ((0,), (0,))))
    pl.semaphore_wait(barrier, len(peers))

    def first_stage(t):
        src = c * 8 + x
        for dx_, dc in ROW:
            x_, c_ = (x + dx_) % 8, (c + dc) % 2
            q_ = (x_ % 2) * 2 + c_
            send(rows_a.at[t, q_], xa.at[t, :, src], r_xa.at[t, src], dev(p, x_, y, c_), lambda: rows_a.at[0, 0])
        for dy in FAR:
            y_ = (y + dy) % 8
            send(rows_b.at[t, y_ // 4], yb.at[t, y], r_yb.at[t, y], dev(p, x, y_, c), lambda: rows_b.at[0, 0])
        xa[t, :, src] = rows_a[t, r]
        yb[t, y] = rows_b[t, y // 4]

    def second_a(t, k):
        for dx_ in FAR + (0,):
            i = k * 8 + (x + dx_) % 8
            if dx_ == 0:
                @pl.when(c != k)
                def _():
                    arrived(xa.at[t, :, i], r_xa.at[t, i])
            else:
                arrived(xa.at[t, :, i], r_xa.at[t, i])
        for e in range(2):
            a2[t, k, e] = xa[t, e, k * 8 : k * 8 + 8].reshape(16, H)
        for dy in FAR:
            y_ = (y + dy) % 8
            send(a2.at[t, k, y_ // 4], ha.at[t, k, y], r_ha.at[t, k, y], dev(p, x, y_, c), lambda: b2.at[0, 0])
        ha[t, k, y] = a2[t, k, y // 4]

    def second_b(t):
        for dy in FAR:
            y_ = (y + dy) % 8
            arrived(yb.at[t, y_], r_yb.at[t, y_])
        for q in range(4):
            b2[t, q] = yb[t, :, :, q * H : (q + 1) * H].reshape(16, H)

    def second_b_send(t, k):
        for dx_, dc in ROW:
            x_, c_ = (x + dx_) % 8, k if dc == 0 else 1 - k
            q_ = (x_ % 2) * 2 + c_
            send(b2.at[t, q_], hb.at[t, k, x], r_hb.at[t, k, x], dev(p, x_, y, c_), lambda: b2.at[0, 0], when=k)
        hb[t, k, x] = b2[t, r]

    def second_stage(t):
        for k in range(2):
            second_a(t, k)
            if k == 0:
                second_b(t)
            pl.when(c == k)(functools.partial(second_b_send, t, k))

    def dispatched(t, k):
        for dy in FAR:
            y_ = (y + dy) % 8
            arrived(ha.at[t, k, y_], r_ha.at[t, k, y_])
        for dx_ in FAR + (0,):
            x_ = (x + dx_) % 8
            if dx_ == 0:
                @pl.when(c != k)
                def _():
                    arrived(hb.at[t, k, x_], r_hb.at[t, k, x_])
            else:
                arrived(hb.at[t, k, x_], r_hb.at[t, k, x_])

    first_stage(0)
    send(sel_s.at[2], sel_in, r_sel, dev(up, x, y, c), lambda: sel_in)
    loads[6].wait()
    loads[7].wait()
    others = [(dxl, dc) for dxl in (0, 1) for dc in (0, 1) if (dxl, dc) != (0, 0)]

    def peer(dxl, dc):
        xl, c_ = (r // 2 + dxl) % 2, (c + dc) % 2
        return xl * 2 + c_

    for dxl, dc in others:
        send(uv.at[r], uv.at[r], r_uv.at[r], (p, peer(dxl, dc), s), lambda: uv.at[0])
    second_stage(0)

    arrived(sel_in, r_sel)
    base_v[...] = dot(sel_in[...], g_v[...], ((0,), (0,)))[0:8]
    m_out[...] = dot(sel_in[...], sel_s[0], ((0,), (0,)))[0:8]

    perm[0] = one_hot_rows(lambda i: ((i >> 1) & 1) * 64 + (i >> 4) * 8 + ((i >> 2) & 3) * 2 + (i & 1))
    perm[1] = one_hot_rows(lambda i: ((i >> 1) & 7) * 16 + (i >> 4) * 2 + (i & 1))
    for dxl, dc in others:
        i = peer(dxl, dc)
        arrived(uv.at[i], r_uv.at[i])
    for k in range(2):
        for t in range(2):
            u, v = (
                jnp.concatenate([uv[i, h, t].reshape(TOK, HID) for i in (k, 2 + k)], axis=0) for h in range(2)
            )
            both = dot(perm[0], jnp.concatenate([u, v], axis=1), ((1,), (0,)))
            u, v = both[:, 0:HID], both[:, HID : 2 * HID]
            sig = jax.nn.sigmoid(u)
            act = u * sig
            if t == 0:
                coef[k, 0] = v * (sig * (1.0 + u * (1.0 - sig)))
                coef[k, 1] = act
            av = (act * v).astype(BF)
            avt[0, :, t * 256 + k * 128 : t * 256 + k * 128 + 128] = av.astype(F32).T.astype(BF)
            avt[1, :, t * 256 + k * 128 : t * 256 + k * 128 + 128] = dot(perm[1], av, ((1,), (0,))).T.astype(BF)
    loads[3].wait()
    loads[4].wait()
    loads[5].wait()

    for k in range(2):
        dispatched(0, k)
        d_b = dot(hb[0, k].reshape(128, H), w2[:, H:Q], ((1,), (1,)))
        d_a = dot(ha[0, k].reshape(128, H), w2[:, 0:H], ((1,), (1,)))
        d_a = d_a + dot(perm[1], d_b.astype(BF), ((0,), (0,)))
        dx[k, r] = d_a.astype(BF)
        for dxl, dc in others:
            send(dx.at[k, r], dx.at[k, r], r_dx.at[k, r], (p, peer(dxl, dc), s), lambda: dx.at[0, 0])

    for k in range(2):
        for dxl, dc in others:
            i = peer(dxl, dc)
            arrived(dx.at[k, i], r_dx.at[k, i])
        d_act = (dx[k, 0].astype(F32) + dx[k, 1].astype(F32)) + (dx[k, 2].astype(F32) + dx[k, 3].astype(F32))
        d_gu = jnp.concatenate([(d_act * coef[k, 0]).astype(BF), (d_act * coef[k, 1]).astype(BF)], axis=1)
        pa[k] = dot(d_gu, w13[0:H, :], ((1,), (1,))).astype(BF).reshape(8, 16, H)
        for dy in FAR:
            y_ = (y + dy) % 8
            send(pa.at[k, y_], ra1.at[k, y], r_ra1.at[k, y], dev(p, x, y_, c), lambda: pa.at[0, 0])
        ra1[k, y] = pa[k, y]
        d_gu = dot(perm[1], d_gu, ((1,), (0,))).astype(BF)
        pb[k] = dot(d_gu, w13[H:Q, :], ((1,), (1,))).astype(BF).reshape(8, 16, H)

        def return_b(x_, when=None):
            send(pb.at[k, x_], rb1.at[r, s % 4], r_rb1.at[r, s % 4], dev(p, x_, y, k), lambda: pb.at[0, 0], when)

        for dx_ in FAR:
            return_b((x + dx_) % 8)
        pl.when(c != k)(functools.partial(return_b, x, 1 - k))

        @pl.when(c == k)
        def _():
            rb1[r, s % 4] = pb[k, x]

    for part in range(2):
        rows = (ha, hb)[part][0].reshape(256, H)
        out[0, :, part * H : (part + 1) * H] = dot(avt[part, :, 0:256], rows, ((1,), (0,)))

    def return_second_b():
        for q in range(4):
            acc = rb1[q, 0].astype(F32)
            for h in range(1, 4):
                acc = acc + rb1[q, h].astype(F32)
            tb[:, :, q * H : (q + 1) * H] = acc.astype(BF).reshape(8, 2, H)

    def wait_rb1():
        for dx_, dc in ROW:
            x_, c_ = (x + dx_) % 8, (c + dc) % 2
            q_ = (x_ % 2) * 2 + c_
            arrived(rb1.at[q_, x_ // 2], r_rb1.at[q_, x_ // 2])

    for k in range(2):
        for dy in FAR:
            y_ = (y + dy) % 8
            arrived(ra1.at[k, y_], r_ra1.at[k, y_])
        for e in range(2):
            acc = ra1[k, 4 * e].astype(F32)
            for h in range(1, 4):
                acc = acc + ra1[k, 4 * e + h].astype(F32)
            ta[k, :, e] = acc.astype(BF).reshape(8, 2, H)

        def return_a(x_, when=None):
            send(ta.at[k, x_], ra2.at[r, s % 4], r_ra2.at[r, s % 4], dev(p, x_, y, k), lambda: ta.at[0, 0], when)

        for dx_ in FAR:
            return_a((x + dx_) % 8)
        pl.when(c != k)(functools.partial(return_a, x, 1 - k))

        def own_chunk():
            ra2[r, s % 4] = ta[k, x]
            wait_rb1()
            return_second_b()
            for dy in FAR:
                y_ = (y + dy) % 8
                send(tb.at[y_], rb2.at[y], r_rb2.at[y], dev(p, x, y_, c), lambda: tb.at[0], k)
            rb2[y] = tb[y]

        pl.when(c == k)(own_chunk)

    alive = jnp.where(p > 0, 1.0, 0.0).astype(F32)
    mix = m_out[...] * alive

    def mixed(e, cols, back):
        acc = base_v[2 * e : 2 * e + 2, cols] * alive
        for f in range(2):
            for h in range(2):
                acc = acc + mix[2 * e : 2 * e + 2, 2 * f + h : 2 * f + h + 1] * back[f][h : h + 1, :]
        return acc.astype(BF)

    for dy in FAR:
        y_ = (y + dy) % 8
        arrived(rb2.at[y_], r_rb2.at[y_])
    back = []
    for f in range(2):
        acc = rb2[4 * f].astype(F32)
        for h in range(1, 4):
            acc = acc + rb2[4 * f + h].astype(F32)
        back.append(acc)
    for q in range(4):
        for e in range(2):
            zb[e, :, q * H : (q + 1) * H] = mixed(
                e, slice(q * Q + H, (q + 1) * Q), [b[:, q * H : (q + 1) * H] for b in back]
            )
    send(zb, rows_b.at[1], r_base.at[1], dev(down, x, y, c), lambda: zb)
    for dx_, dc in ROW:
        x_, c_ = (x + dx_) % 8, (c + dc) % 2
        q_ = (x_ % 2) * 2 + c_
        arrived(ra2.at[q_, x_ // 2], r_ra2.at[q_, x_ // 2])
    for q in range(4):
        back = []
        for f in range(2):
            acc = ra2[q, 0, f].astype(F32)
            for h in range(1, 4):
                acc = acc + ra2[q, h, f].astype(F32)
            back.append(acc)
        for e in range(2):
            za[q, e] = mixed(e, slice(q * Q, q * Q + H), back)
    send(za, rows_a.at[1], r_base.at[0], dev(down, x, y, c), lambda: za)
    arrived(rows_b.at[1], r_base.at[1])
    arrived(rows_a.at[1], r_base.at[0])

    first_stage(1)
    second_stage(1)
    for k in range(2):
        dispatched(1, k)
        for part in range(2):
            cols = slice(part * H, (part + 1) * H)
            rows = (ha, hb)[part][1, k].reshape(128, H)
            out[0, :, cols] += dot(avt[part, :, 256 + k * 128 : 384 + k * 128], rows, ((1,), (0,)))

    for k, (like, when) in enumerate(sends):
        def drained(like=like, k=k):
            pltpu.make_async_copy(like(), like(), s_send.at[k]).wait()

        if when is None:
            drained()
        else:
            pl.when(c == when)(drained)
    assert len(sends) <= N_SENDS, len(sends)


N_SENDS = 256


def body(*arguments):
    hbm = pl.BlockSpec(memory_space=pl.ANY)
    dma = pltpu.SemaphoreType.DMA
    return pl.pallas_call(
        kernel,
        out_shape=jax.ShapeDtypeStruct((1, HID, Q), F32),
        in_specs=[hbm] * 8,
        out_specs=pl.BlockSpec(memory_space=pltpu.VMEM),
        scratch_shapes=[
            pltpu.VMEM((TOK, D), BF),
            pltpu.VMEM((2, TOK, 8), jnp.int32),
            pltpu.VMEM((2, TOK, 8), BF),
            pltpu.VMEM((HID, Q), BF),
            pltpu.VMEM((Q, 2 * HID), BF),
            pltpu.VMEM((3, TOK, 128), BF),
            pltpu.VMEM((TOK, 128), BF),
            pltpu.VMEM((2, 4, 2, 2, H), BF),
            pltpu.VMEM((2, 2, 2, 4 * H), BF),
            pltpu.VMEM((8, D), F32),
            pltpu.VMEM((8, 128), F32),
            pltpu.VMEM((4, 2, 2, 32, 2, HID), BF),
            pltpu.VMEM((2, 2, 128, HID), F32),
            pltpu.VMEM((2, 128, 128), BF),
            pltpu.VMEM((2, HID, 512), BF),
            pltpu.VMEM((2, 2, 16, 2, H), BF),
            pltpu.VMEM((2, 2, 2, 16, H), BF),
            pltpu.VMEM((2, 8, 2, 4 * H), BF),
            pltpu.VMEM((2, 4, 16, H), BF),
            pltpu.VMEM((2, 2, 8, 16, H), BF),
            pltpu.VMEM((2, 2, 8, 16, H), BF),
            pltpu.VMEM((2, 4, 128, HID), BF),
            pltpu.VMEM((2, 8, 16, H), BF),
            pltpu.VMEM((2, 8, 16, H), BF),
            pltpu.VMEM((2, 8, 16, H), BF),
            pltpu.VMEM((4, 4, 16, H), BF),
            pltpu.VMEM((2, 8, 2, 2, H), BF),
            pltpu.VMEM((8, 2, 4 * H), BF),
            pltpu.VMEM((4, 4, 2, 2, H), BF),
            pltpu.VMEM((8, 2, 4 * H), BF),
            pltpu.VMEM((4, 2, 2, H), BF),
            pltpu.VMEM((2, 2, 4 * H), BF),
            dma((8,)),
            dma((N_SENDS,)),
            dma((2, 16)),
            dma((2, 8)),
            dma((2, 2, 8)),
            dma((2, 2, 8)),
            dma((2, 4)),
            dma((2, 8)),
            dma((4, 4)),
            dma((4, 4)),
            dma((8,)),
            dma((4,)),
            dma,
            dma((2,)),
        ],
        compiler_params=pltpu.CompilerParams(collective_id=0, has_side_effects=True),
        name="cooldown",
    )(*arguments)


def solution(mesh):
    in_specs = (
        P("pipe", ("dp", "expert"), None),
        P("pipe", None, ("dp", "expert"), None),
        P("pipe", None, ("dp", "expert"), None),
        P("pipe", None, "dp", None, None, "expert"),
        P("pipe", None, "dp", None, None, "expert"),
        P("pipe", None, "expert"),
        P("pipe", None, "expert"),
        P("pipe", "expert", None),
    )
    out_specs = P("pipe", "expert", "dp")
    return jax.shard_map(body, mesh=mesh, in_specs=in_specs, out_specs=out_specs, check_vma=False)
```

```python
import functools

import jax
import jax.numpy as jnp
from jax import lax
from jax.experimental import pallas as pl
from jax.experimental.pallas import tpu as pltpu
from jax.sharding import PartitionSpec as P

MESH = pl.DeviceIdType.MESH
BF = jnp.bfloat16
F32 = jnp.float32

D = 7168
TOK = 64
HID = 128
Q = 1792
H = 896
K = 4
FAR = (4, 3, 5, 2, 6, 1, 7)
ROW = tuple((dx, dc) for dx in FAR for dc in (0, 1)) + ((0, 1),)


def dot(a, b, dims):
    return lax.dot_general(a, b, (dims, ((), ())), preferred_element_type=F32)


def kernel(
    cot, routes, gates, gate_pre, up_pre, w_gate, w_up, w_down, out,
    g_v, ids_v, gat_v, w2, w13, sel_s, sel_in, rows_a, rows_b, base_v, base_o, base_in, m_v, m_in, uv, coef, perm, avt, total,
    xa, a2, yb, b2, ha, hb, hd, dx, pa, pb, ra1, rb1, ta, tb, ra2, rb2,
    ld, st, snd, r_xa, r_yb, r_ha, r_hb, r_dx, r_ra1, r_rb1, r_ra2, r_rb2, r_one,
):
    p = lax.axis_index("pipe")
    r = lax.axis_index("dp")
    s = lax.axis_index("expert")
    y = s // 4
    xh = s % 4
    x = xh * 2 + r // 2
    c = r % 2
    up = (p + 1) % 8
    down = (p + 7) % 8
    mine = (r + y) % 4
    half = y // 4

    def dev(p_, x_, y_, c_):
        return (p_, (x_ % 2) * 2 + c_, y_ * 4 + x_ // 2)

    def send(src, dst, kind, recv, target):
        pltpu.make_async_remote_copy(
            src_ref=src, dst_ref=dst, send_sem=snd.at[kind], recv_sem=recv, device_id=target, device_id_type=MESH
        ).start()

    def arrived(like, sem):
        pltpu.make_async_copy(like, like, sem).wait()

    D1A, D1B, D2A, D2B, DX, R1A, R1B, R2A, R2B, UV, SEL, BASE, MM, D1A1, D1B1 = range(15)

    barrier = pltpu.get_barrier_semaphore()
    peers = [((x + ox) % 8, y, (c + oc) % 2, p) for ox, oc in ROW]
    peers += [(x, (y + oy) % 8, c, p) for oy in FAR]
    peers += [(x, y, c, up), (x, y, c, down)]
    for x_, y_, c_, p_ in peers:
        pl.semaphore_signal(barrier, inc=1, device_id=dev(p_, x_, y_, c_), device_id_type=MESH)

    q0 = pl.multiple_of(r * Q, 128)
    loads = [
        pltpu.make_async_copy(routes.at[0], ids_v, ld.at[0]),
        pltpu.make_async_copy(gates.at[0], gat_v, ld.at[1]),
        pltpu.make_async_copy(cot.at[0], g_v, ld.at[2]),
        pltpu.make_async_copy(w_down.at[0, :, pl.ds(q0, Q)], w2, ld.at[3]),
        pltpu.make_async_copy(w_gate.at[0, pl.ds(q0, Q)], w13.at[:, 0:HID], ld.at[4]),
        pltpu.make_async_copy(w_up.at[0, pl.ds(q0, Q)], w13.at[:, HID : 2 * HID], ld.at[5]),
        pltpu.make_async_copy(gate_pre.at[0, :, 0], uv.at[r, 0], ld.at[6]),
        pltpu.make_async_copy(up_pre.at[0, :, 0], uv.at[r, 1], ld.at[7]),
    ]
    for cp in loads:
        cp.start()

    loads[0].wait()
    loads[1].wait()
    row = lax.broadcasted_iota(jnp.int32, (8, TOK), 0)
    upto = (
        lax.broadcasted_iota(jnp.int32, (TOK, TOK), 0) <= lax.broadcasted_iota(jnp.int32, (TOK, TOK), 1)
    ).astype(F32).astype(BF)
    for t in range(2):
        ids = ids_v[t]
        gat = gat_v[t].astype(F32)
        hit = jnp.zeros((8, TOK), F32)
        gsum = jnp.zeros((8, TOK), F32)
        for e in range(2):
            match = (ids == e).astype(F32)
            of_e = (row >= 2 * e) & (row < 2 * e + 2)
            hit = jnp.where(of_e, jnp.sum(match, axis=0, keepdims=True), hit)
            gsum = jnp.where(of_e, jnp.sum(match * gat, axis=0, keepdims=True), gsum)
        rank = dot(hit.astype(BF), upto, ((1,), (0,))) - 1.0
        sel = hit * (rank == (row & 1).astype(F32)).astype(F32)
        if t == 0:
            sel_s[0] = sel.astype(BF)
        sel_s[1 + t] = (sel * gsum).astype(BF)

    loads[2].wait()
    rows = dot(sel_s[1], g_v[...], ((1,), (0,)))
    for e in range(2):
        for q in range(4):
            rows_a[0, q, e] = rows[2 * e : 2 * e + 2, q * Q : q * Q + H].astype(BF)
            rows_b[0, e, :, q * H : (q + 1) * H] = rows[2 * e : 2 * e + 2, q * Q + H : (q + 1) * Q].astype(BF)

    pl.semaphore_wait(barrier, len(peers))

    def first_a(t):
        for ox, oc in ROW:
            x_, c_ = (x + ox) % 8, (c + oc) % 2
            q_ = (x_ % 2) * 2 + c_
            send(rows_a.at[t, q_], xa.at[t, mine, xh], (D1A, D1A1)[t], r_xa.at[t, mine], dev(p, x_, y, c_))
        xa[t, mine, xh] = rows_a[t, r]

    def first_b(t):
        for oy in FAR + (0,) * t:
            y_ = (y + oy) % 8
            send(
                rows_b.at[t, y_ // 4], yb.at[t, y % 4, half], (D1B, D1B1)[t], r_yb.at[t, mine], dev((p, down)[t], x, y_, c)
            )
        if t == 0:
            yb[t, y % 4, half] = rows_b[t, half]

    def second(t, k):
        @pl.when(mine == k)
        def _():
            arrived(xa.at[t, k, 0:3], r_xa.at[t, k])

        @pl.when(mine != k)
        def _():
            arrived(xa.at[t, k], r_xa.at[t, k])

        for e in range(2):
            a2[t, k, e] = jnp.concatenate([xa[t, k, h, e] for h in range(4)], axis=0)
        for oy in FAR:
            y_ = (y + oy) % 8
            send(a2.at[t, k, y_ // 4], ha.at[t, k, y], D2A, r_ha.at[t, k], dev(p, x, y_, c))
        ha[t, k, y] = a2[t, k, half]
        v = (k + 4 - r) % 4
        if t == 0:
            @pl.when(mine == k)
            def _():
                arrived(yb.at[t, k, 0], r_yb.at[t, k])

            @pl.when(mine != k)
            def _():
                arrived(yb.at[t, k], r_yb.at[t, k])
        else:
            arrived(yb.at[t, k], r_yb.at[t, k])
        for h in range(2):
            for q in range(4):
                b2[t, k, q, 2 * h : 2 * h + 2, :] = yb[t, v, h, :, q * H : (q + 1) * H]
        for ox, oc in ROW:
            x_, c_ = (x + ox) % 8, (c + oc) % 2
            q_ = (x_ % 2) * 2 + c_
            send(b2.at[t, k, q_], hb.at[t, k, r * 4 + xh], D2B, r_hb.at[t, k], dev(p, x_, y, c_))
        hb[t, k, r * 4 + xh] = b2[t, k, r]

    def dispatched(t, k):
        arrived(ha.at[t, k, 0:7], r_ha.at[t, k])
        arrived(hb.at[t, k, 0:15], r_hb.at[t, k])
        hd[t, k] = hb[t, k].reshape(64, H)

    others = [(ol, oc) for ol in (0, 1) for oc in (0, 1) if (ol, oc) != (0, 0)]

    def peer(ol, oc):
        return ((r // 2 + ol) % 2) * 2 + (c + oc) % 2

    first_a(0)
    first_b(0)
    send(sel_s.at[2], sel_in, SEL, r_one.at[0], dev(up, x, y, c))
    loads[6].wait()
    loads[7].wait()
    for ol, oc in others:
        send(uv.at[r], uv.at[r], UV, r_one.at[1], (p, peer(ol, oc), s))
    for k in range(K):
        second(0, k)

    arrived(sel_in, r_one.at[0])
    base_v[...] = dot(sel_in[...], g_v[...], ((1,), (0,)))
    m_v[...] = dot(sel_in[...], sel_s[0], ((1,), (1,)))
    for e in range(2):
        for q in range(4):
            base_o[q, e] = base_v[2 * e : 2 * e + 2, q * Q : q * Q + H]
    send(base_o, base_in, BASE, r_one.at[2], dev(down, x, y, c))
    send(m_v, m_in, MM, r_one.at[3], dev(down, x, y, c))

    arrived(uv.at[0:3], r_one.at[1])
    i64 = lax.broadcasted_iota(jnp.int32, (64, 64), 0)
    j64 = lax.broadcasted_iota(jnp.int32, (64, 64), 1)
    for k in range(K):
        src = ((((k + 4) - (i64 >> 4)) & 3) + ((i64 >> 1) & 1) * 4) * 8 + ((i64 >> 2) & 3) * 2 + (i64 & 1)
        perm[k] = (src == j64).astype(F32).astype(BF)
        for t in range(2):
            u, v = (
                jnp.concatenate(
                    [uv[(k - yy) % 4, h, t, 4 * yy : 4 * yy + 4].astype(F32).reshape(8, HID) for yy in range(8)], axis=0
                )
                for h in range(2)
            )
            sig = jax.nn.sigmoid(u)
            act = u * sig
            if t == 0:
                coef[k, 0] = v * (sig * (1.0 + u * (1.0 - sig)))
                coef[k, 1] = act
            av = (act * v).astype(BF)
            avt[0, t, k] = av.astype(F32).T.astype(BF)
            avt[1, t, k] = dot(perm[k], av, ((1,), (0,))).T.astype(BF)
    loads[3].wait()
    loads[4].wait()
    loads[5].wait()

    def hidden_gradient(k):
        dispatched(0, k)
        d_b = dot(hd[0, k], w2[:, H:Q], ((1,), (1,)))
        d_a = dot(ha[0, k].reshape(64, H), w2[:, 0:H], ((1,), (1,)))
        d_a = d_a + dot(perm[k], d_b.astype(BF), ((0,), (0,)))
        dx[k, r] = d_a.astype(BF)
        for ol, oc in others:
            send(dx.at[k, r], dx.at[k, r], DX, r_dx.at[k], (p, peer(ol, oc), s))

    def input_gradient(k):
        arrived(dx.at[k, 0:3], r_dx.at[k])
        d_act = (dx[k, 0].astype(F32) + dx[k, 1].astype(F32)) + (dx[k, 2].astype(F32) + dx[k, 3].astype(F32))
        d_gu = jnp.concatenate([(d_act * coef[k, 0]).astype(BF), (d_act * coef[k, 1]).astype(BF)], axis=1)
        pa[k] = dot(d_gu, w13[0:H, :], ((1,), (1,))).astype(BF).reshape(8, 8, H)
        for oy in FAR:
            y_ = (y + oy) % 8
            send(pa.at[k, y_], ra1.at[k, y], R1A, r_ra1.at[k], dev(p, x, y_, c))
        ra1[k, y] = pa[k, y]
        d_gu = dot(perm[k], d_gu, ((1,), (0,))).astype(BF)
        pb[k] = dot(d_gu, w13[H:Q, :], ((1,), (1,))).astype(BF).reshape(16, 4, H)
        for ox, oc in ROW:
            x_, c_ = (x + ox) % 8, (c + oc) % 2
            i_ = ((x_ % 2) * 2 + c_) * 4 + x_ // 2
            send(pb.at[k, i_], rb1.at[k, r * 4 + xh], R1B, r_rb1.at[k], dev(p, x_, y, c_))
        rb1[k, r * 4 + xh] = pb[k, r * 4 + xh]

    def to_sources(k):
        arrived(ra1.at[k, 0:7], r_ra1.at[k])
        for e in range(2):
            acc = ra1[k, 4 * e].astype(F32)
            for h in range(1, 4):
                acc = acc + ra1[k, 4 * e + h].astype(F32)
            for h in range(4):
                ta[k, h, e] = acc[2 * h : 2 * h + 2].astype(BF)
        r_ = (k + 8 - y) % 4
        for h in range(4):
            send(ta.at[k, h], ra2.at[r * 4 + xh], R2A, r_ra2, (down, r_, y * 4 + h))
        arrived(rb1.at[k, 0:15], r_rb1.at[k])
        for q in range(4):
            acc = rb1[k, 4 * q].astype(F32)
            for h in range(1, 4):
                acc = acc + rb1[k, 4 * q + h].astype(F32)
            for h in range(2):
                tb[k, h, :, q * H : (q + 1) * H] = acc[2 * h : 2 * h + 2].astype(BF)
        v = (k + 4 - r) % 4
        for h in range(2):

            def go(h=h):
                send(tb.at[k, h], rb2.at[y], R2B, r_rb2, dev(p, x, v + 4 * h, c))

            pl.when(v + 4 * h != y)(go)

            @pl.when(v + 4 * h == y)
            def _(h=h):
                rb2[y] = tb[k, h]

    def mixed(e, base, m, back):
        for f in range(2):
            for h in range(2):
                base = base + m[2 * e : 2 * e + 2, 2 * f + h : 2 * f + h + 1] * back[f][h : h + 1, :]
        return base.astype(BF)

    def next_rows():
        arrived(rb2.at[0:7], r_rb2)
        alive = jnp.where(p > 0, 1.0, 0.0).astype(F32)
        m = m_v[...] * alive
        back = []
        for f in range(2):
            acc = rb2[4 * f].astype(F32)
            for h in range(1, 4):
                acc = acc + rb2[4 * f + h].astype(F32)
            back.append(acc)
        for q in range(4):
            for e in range(2):
                rows_b[1, e, :, q * H : (q + 1) * H] = mixed(
                    e,
                    base_v[2 * e : 2 * e + 2, q * Q + H : (q + 1) * Q] * alive,
                    m,
                    [b[:, q * H : (q + 1) * H] for b in back],
                )
        first_b(1)
        arrived(ra2, r_ra2)
        alive = jnp.where(p < 7, 1.0, 0.0).astype(F32)
        m = m_in[...] * alive
        for q in range(4):
            back = []
            for f in range(2):
                acc = ra2[4 * q, f].astype(F32)
                for h in range(1, 4):
                    acc = acc + ra2[4 * q + h, f].astype(F32)
                back.append(acc)
            for e in range(2):
                rows_a[1, q, e] = mixed(e, base_in[q, e] * alive, m, back)
        first_a(1)

    def gather_rows(k):
        pl.when(mine == k)(next_rows)

    hidden_gradient(0)
    hidden_gradient(1)
    input_gradient(0)
    hidden_gradient(2)
    input_gradient(1)
    hidden_gradient(3)
    input_gradient(2)
    to_sources(0)
    input_gradient(3)
    for part in range(2):
        left = jnp.concatenate([avt[part, 0, k] for k in range(K)], axis=1)
        right = (ha, hd)[part][0].reshape(K * 64, H)
        out[0, :, part * H : (part + 1) * H] = dot(left, right, ((1,), (0,)))
    arrived(base_in, r_one.at[2])
    arrived(m_in, r_one.at[3])
    to_sources(1)
    gather_rows(0)
    to_sources(2)
    gather_rows(1)
    to_sources(3)
    second(1, 0)
    gather_rows(2)
    second(1, 1)
    gather_rows(3)
    second(1, 2)
    second(1, 3)
    stores = []
    for k in range(K):
        dispatched(1, k)
        for part in range(2):
            cols = slice(part * H, (part + 1) * H)
            right = ha[1, k].reshape(64, H) if part == 0 else hd[1, k]
            out[0, :, cols] += dot(avt[part, 1, k], right, ((1,), (0,)))

    arrived(ra2.at[0:15], snd.at[D1A])
    arrived(ra2.at[0:15], snd.at[D1A1])
    arrived(rb2.at[0:7], snd.at[D1B])
    arrived(rb2, snd.at[D1B1])
    arrived(ha.at[:, :, 0:7], snd.at[D2A])
    arrived(hb.at[:, :, 0:15], snd.at[D2B])
    arrived(dx.at[:, 0:3], snd.at[DX])
    arrived(ra1.at[:, 0:7], snd.at[R1A])
    arrived(rb1.at[:, 0:15], snd.at[R1B])
    arrived(ra2, snd.at[R2A])
    arrived(rb2.at[0:7], snd.at[R2B])
    arrived(uv.at[0:3], snd.at[UV])
    arrived(sel_in, snd.at[SEL])
    arrived(base_in, snd.at[BASE])
    arrived(m_in, snd.at[MM])
    for cp in stores:
        cp.wait()


def body(cotangent, routes, gates, *others):
    hbm = pl.BlockSpec(memory_space=pl.ANY)
    dma = pltpu.SemaphoreType.DMA
    vmem = pltpu.VMEM
    return pl.pallas_call(
        kernel,
        out_shape=vmem((1, HID, Q), F32),
        in_specs=[hbm] * 8,
        out_specs=pl.BlockSpec(memory_space=vmem),
        scratch_shapes=[
            vmem((TOK, D), BF),
            vmem((2, 8, TOK), jnp.int32),
            vmem((2, 8, TOK), BF),
            vmem((HID, Q), BF),
            vmem((Q, 2 * HID), BF),
            vmem((3, 8, TOK), BF),
            vmem((8, TOK), BF),
            vmem((2, 4, 2, 2, H), BF),
            vmem((2, 2, 2, 4 * H), BF),
            vmem((8, D), F32),
            vmem((4, 2, 2, H), F32),
            vmem((4, 2, 2, H), F32),
            vmem((8, 8), F32),
            vmem((8, 8), F32),
            vmem((4, 2, 2, 32, 2, HID), BF),
            vmem((K, 2, 64, HID), F32),
            vmem((K, 64, 64), BF),
            vmem((2, 2, K, HID, 64), BF),
            vmem((HID, Q), F32),
            vmem((2, K, 4, 2, 2, H), BF),
            vmem((2, K, 2, 8, H), BF),
            vmem((2, 4, 2, 2, 4 * H), BF),
            vmem((2, K, 4, 4, H), BF),
            vmem((2, K, 8, 8, H), BF),
            vmem((2, K, 16, 4, H), BF),
            vmem((2, K, 64, H), BF),
            vmem((K, 4, 64, HID), BF),
            vmem((K, 8, 8, H), BF),
            vmem((K, 16, 4, H), BF),
            vmem((K, 8, 8, H), BF),
            vmem((K, 16, 4, H), BF),
            vmem((K, 4, 2, 2, H), BF),
            vmem((K, 2, 2, 4 * H), BF),
            vmem((16, 2, 2, H), BF),
            vmem((8, 2, 4 * H), BF),
            dma((8,)),
            dma((2,)),
            dma((15,)),
            dma((2, K)),
            dma((2, K)),
            dma((2, K)),
            dma((2, K)),
            dma((K,)),
            dma((K,)),
            dma((K,)),
            dma,
            dma,
            dma((4,)),
        ],
        compiler_params=pltpu.CompilerParams(collective_id=0, has_side_effects=True),
        name="cooldown",
    )(cotangent, jnp.swapaxes(routes, 2, 3), jnp.swapaxes(gates, 2, 3), *others)


def solution(mesh):
    in_specs = (
        P("pipe", ("dp", "expert"), None),
        P("pipe", None, ("dp", "expert"), None),
        P("pipe", None, ("dp", "expert"), None),
        P("pipe", None, "dp", None, None, "expert"),
        P("pipe", None, "dp", None, None, "expert"),
        P("pipe", None, "expert"),
        P("pipe", None, "expert"),
        P("pipe", "expert", None),
    )
    out_specs = P("pipe", "expert", "dp")
    return jax.shard_map(body, mesh=mesh, in_specs=in_specs, out_specs=out_specs, check_vma=False)
```

```python
import functools

import jax
import jax.numpy as jnp
from jax import lax
from jax.experimental import pallas as pl
from jax.experimental.pallas import tpu as pltpu
from jax.sharding import PartitionSpec as P

MESH = pl.DeviceIdType.MESH
BF = jnp.bfloat16
F32 = jnp.float32

D = 7168
TOK = 64
HID = 128
Q = 1792
HA = 1024
HB = Q - HA
K = 4
FAR = (4, 3, 5, 2, 6, 1, 7)
ROW = tuple((dx, dc) for dx in FAR for dc in (0, 1)) + ((0, 1),)
FORWARD = ((1, 1, 1, 1), (1, 1, 1, 1), (1, 1, 1, 1))
NEAR = tuple((dx, dc) for dx in (2, 6, 1, 7) for dc in (0, 1)) + ((0, 1),)
BACK = ((4, 6, 0, 2), (4, 2, 1, 5), (5, 6, 0, 0), (5, 6, 1, 1), (3, 2, 0, 3), (3, 2, 1, 4))
FAR_ROW = tuple((dx, dc) for dx in (4, 3, 5) for dc in (0, 1))


def dot(a, b, dims):
    return lax.dot_general(a, b, (dims, ((), ())), preferred_element_type=F32)


def kernel(
    cot, routes, gates, gate_pre, up_pre, w_gate, w_up, w_down, out,
    g_v, ids_v, gat_v, w2, w13, sel_s, sel_in, rows_a, rows_b, base_v, base_o, base_in, m_v, m_in, uv, uv1, av1, coef, avt,
    xa, a2, yb, ha, hb, hd, dx, pa, pb, fa, fb, sa, sb, ra1, rb1, ta, tb, ra2, rb2,
    ld, snd, r_xa, r_yb, r_ha, r_hb, r_ha2, r_hb2, r_dx, r_fa, r_fb, r_ra1, r_rb1, r_ra2, r_rb2, r_one,
):
    p = lax.axis_index("pipe")
    r = lax.axis_index("dp")
    s = lax.axis_index("expert")
    y = s // 4
    xh = s % 4
    x = xh * 2 + r // 2
    c = r % 2
    lower = p < 7
    upper = p > 0
    up = jnp.minimum(p + 1, 7)
    down = jnp.maximum(p - 1, 0)
    mine = (r + y) % 4
    half = y // 4
    at = y % 4
    inner = (at == 1) | (at == 2)
    turn = jnp.where(at < 2, 1, -1)

    def dev(p_, x_, y_, c_):
        return (p_, (x_ % 2) * 2 + c_, y_ * 4 + x_ // 2)

    def send(src, dst, kind, recv, target):
        pltpu.make_async_remote_copy(
            src_ref=src, dst_ref=dst, send_sem=snd.at[kind], recv_sem=recv, device_id=target, device_id_type=MESH
        ).start()

    def arrived(like, sem):
        pltpu.make_async_copy(like, like, sem).wait()

    D1A, D1A1, D1B, D1B1, D2A, _, D2F, _, D2B, _, DX, R1A, R1B, R2A, R2B, UV, AV, SEL, BASE, MM = range(20)

    barrier = pltpu.get_barrier_semaphore()
    peers = [((x + ox) % 8, y, (c + oc) % 2, p) for ox, oc in ROW]
    peers += [(x, (y + oy) % 8, c, p) for oy in FAR]
    for x_, y_, c_, p_ in peers:
        pl.semaphore_signal(barrier, inc=1, device_id=dev(p_, x_, y_, c_), device_id_type=MESH)
    for there, p_ in ((lower, up), (upper, down)):
        @pl.when(there)
        def _(p_=p_):
            pl.semaphore_signal(barrier, inc=1, device_id=dev(p_, x, y, c), device_id_type=MESH)

    q0 = pl.multiple_of(r * Q, 128)
    loads = [
        pltpu.make_async_copy(routes.at[0], ids_v, ld.at[0]),
        pltpu.make_async_copy(gates.at[0], gat_v, ld.at[1]),
        pltpu.make_async_copy(cot.at[0], g_v, ld.at[2]),
        pltpu.make_async_copy(w_down.at[0, :, pl.ds(q0, Q)], w2, ld.at[3]),
        pltpu.make_async_copy(w_gate.at[0, pl.ds(q0, Q)], w13.at[:, 0:HID], ld.at[4]),
        pltpu.make_async_copy(w_up.at[0, pl.ds(q0, Q)], w13.at[:, HID : 2 * HID], ld.at[5]),
        pltpu.make_async_copy(gate_pre.at[0, 0, 0], uv.at[r, 0], ld.at[6]),
        pltpu.make_async_copy(up_pre.at[0, 0, 0], uv.at[r, 1], ld.at[7]),
        pltpu.make_async_copy(gate_pre.at[0, 1, 0], uv1.at[0], ld.at[8]),
        pltpu.make_async_copy(up_pre.at[0, 1, 0], uv1.at[1], ld.at[9]),
    ]
    for cp in loads:
        cp.start()

    loads[0].wait()
    loads[1].wait()
    row = lax.broadcasted_iota(jnp.int32, (8, TOK), 0)
    upto = (
        lax.broadcasted_iota(jnp.int32, (TOK, TOK), 0) <= lax.broadcasted_iota(jnp.int32, (TOK, TOK), 1)
    ).astype(F32).astype(BF)
    for t in range(2):
        ids = ids_v[t]
        gat = gat_v[t].astype(F32)
        hit = jnp.zeros((8, TOK), F32)
        gsum = jnp.zeros((8, TOK), F32)
        for e in range(2):
            match = (ids == e).astype(F32)
            of_e = (row >= 2 * e) & (row < 2 * e + 2)
            hit = jnp.where(of_e, jnp.sum(match, axis=0, keepdims=True), hit)
            gsum = jnp.where(of_e, jnp.sum(match * gat, axis=0, keepdims=True), gsum)
        rank = dot(hit.astype(BF), upto, ((1,), (0,))) - 1.0
        sel = hit * (rank == (row & 1).astype(F32)).astype(F32)
        if t == 0:
            sel_s[0] = sel.astype(BF)
        sel_s[1 + t] = (sel * gsum).astype(BF)

    loads[2].wait()
    rows = dot(sel_s[1], g_v[...], ((1,), (0,)))
    for e in range(2):
        for q in range(4):
            rows_a[0, q, e] = rows[2 * e : 2 * e + 2, q * Q : q * Q + HA].astype(BF)
            rows_b[0, e, :, q * HB : (q + 1) * HB] = rows[2 * e : 2 * e + 2, q * Q + HA : (q + 1) * Q].astype(BF)

    for k in range(K):
        if FORWARD[1][k]:
            zeros = jnp.zeros((8, HA), BF)
            ra1[k, (y + 4) % 8] = zeros
            for where, oy in ((1, 3), (2, 5)):
                @pl.when(at != where)
                def _(k=k, oy=oy):
                    ra1[k, (y + oy) % 8] = jnp.zeros((8, HA), BF)

            for where, slot in ((3, 0), (0, 1)):
                @pl.when(at == where)
                def _(k=k, slot=slot):
                    fa[k, slot] = jnp.zeros((8, HA), BF)

            for ox in (3, 4, 5):
                for c_ in range(2):
                    x_ = (x + ox) % 8
                    rb1[k, ((x_ % 2) * 2 + c_) * 4 + x_ // 2] = jnp.zeros((2, 2, HB), BF)

    @pl.when(lower & upper)
    def _():
        pl.semaphore_wait(barrier, len(peers) + 2)

    @pl.when(jnp.logical_not(lower & upper))
    def _():
        pl.semaphore_wait(barrier, len(peers) + 1)

    def first_a(t):
        for ox, oc in ROW:
            x_, c_ = (x + ox) % 8, (c + oc) % 2
            q_ = (x_ % 2) * 2 + c_
            send(rows_a.at[t, q_], xa.at[t, mine, xh], D1A + t, r_xa.at[t, mine], dev(p, x_, y, c_))
        xa[t, mine, xh] = rows_a[t, r]

    def first_b(t):
        for oy in FAR + (0,) * t:
            y_ = (y + oy) % 8
            send(
                rows_b.at[t, y_ // 4], yb.at[t, y % 4, half], D1B + t, r_yb.at[t, mine], dev((p, down)[t], x, y_, c)
            )
        if t == 0:
            yb[t, y % 4, half] = rows_b[t, half]

    def send_b(t, k, x_, c_, sem):
        v = (k + 4 - r) % 4
        columns = pl.ds(pl.multiple_of(((x_ % 2) * 2 + c_) * HB, 128), HB)
        send(yb.at[t, v, :, :, columns], hb.at[t, k, :, v, xh], D2B + t, sem.at[t, k], dev(p, x_, y, c_))

    def second(t, k):
        @pl.when(mine == k)
        def _():
            arrived(xa.at[t, k, 0:3], r_xa.at[t, k])

        @pl.when(mine != k)
        def _():
            arrived(xa.at[t, k], r_xa.at[t, k])

        for e in range(2):
            a2[t, k, e] = jnp.concatenate([xa[t, k, h, e] for h in range(4)], axis=0)
        for oy in (2, 6, 1, 7):
            y_ = (y + oy) % 8
            send(a2.at[t, k, y_ // 4], ha.at[t, k, y], D2A + t, r_ha.at[t, k], dev(p, x, y_, c))

        def direct_a(oy):
            y_ = (y + oy) % 8
            send(a2.at[t, k, y_ // 4], ha.at[t, k, y], D2F + t, r_ha2.at[t, k], dev(p, x, y_, c))

        if FORWARD[2 * t][k]:
            pl.when(at == 1)(functools.partial(direct_a, 3))
            pl.when(at == 2)(functools.partial(direct_a, 5))
        else:
            for oy in (4, 3, 5):
                direct_a(oy)
        ha[t, k, y] = a2[t, k, half]
        v = (k + 4 - r) % 4
        if t == 0:
            @pl.when(mine == k)
            def _():
                arrived(yb.at[t, k, 0], r_yb.at[t, k])

            @pl.when(mine != k)
            def _():
                arrived(yb.at[t, k], r_yb.at[t, k])
        else:
            arrived(yb.at[t, k], r_yb.at[t, k])
        for ox, oc in NEAR:
            send_b(t, k, (x + ox) % 8, (c + oc) % 2, r_hb)
        if not FORWARD[2 * t][k]:
            for ox, oc in FAR_ROW:
                send_b(t, k, (x + ox) % 8, (c + oc) % 2, r_hb2)
        hb[t, k, :, v, xh] = yb[t, v, :, :, pl.ds(pl.multiple_of(r * HB, 128), HB)]

    def landing(k, x_, c_):
        return (k + 4 - ((x_ % 2) * 2 + c_)) % 4, x_ // 2

    def forward(t, k):
        arrived(ha.at[t, k, 0:4], r_ha.at[t, k])

        def pass_a(oy_from, oy_to):
            i = (y + oy_from) % 8
            send(ha.at[t, k, i], ha.at[t, k, i], D2F + t, r_ha2.at[t, k], dev(p, x, (y + oy_to) % 8, c))

        pass_a(8 - 2 * turn, 8 + 2 * turn)
        pl.when(at != 3)(functools.partial(pass_a, 6, 1))
        pl.when(at != 0)(functools.partial(pass_a, 2, 7))
        arrived(nine, r_hb.at[t, k])
        for ox_from, ox_to, cores in ((6, 2, (0,)), (2, 6, (1,)), (7, 2, (0, 1)), (1, 6, (0, 1))):
            for c_ in cores:
                v, i = landing(k, (x + ox_from) % 8, c_)
                send(
                    hb.at[t, k, :, v, i], hb.at[t, k, :, v, i], D2B + t, r_hb2.at[t, k], dev(p, (x + ox_to) % 8, y, c)
                )

    nine, six, fifteen = rb1.at[0, 0:9], rb1.at[0, 0:6], rb1.at[:, 0:15]

    def dispatched(t, k):
        if not FORWARD[2 * t][k]:
            arrived(ha.at[t, k, 0:4], r_ha.at[t, k])
            arrived(nine, r_hb.at[t, k])
        arrived(ha.at[t, k, 0:3], r_ha2.at[t, k])
        arrived(six, r_hb2.at[t, k])
        hd[t, k] = hb[t, k].reshape(64, HB)

    others = [(ol, oc) for ol in (0, 1) for oc in (0, 1) if (ol, oc) != (0, 0)]

    def peer(ol, oc):
        return ((r // 2 + ol) % 2) * 2 + (c + oc) % 2

    first_a(0)
    first_b(0)
    @pl.when(lower)
    def _():
        send(sel_s.at[2], sel_in, SEL, r_one.at[0], dev(up, x, y, c))

    loads[6].wait()
    loads[7].wait()
    for ol, oc in others:
        send(uv.at[r], uv.at[r], UV, r_one.at[1], (p, peer(ol, oc), s))
    loads[8].wait()
    loads[9].wait()
    u, v = (uv1[h].astype(F32).reshape(TOK, HID) for h in range(2))
    av1[r] = (u * jax.nn.sigmoid(u) * v).astype(BF)
    for ol, oc in others:
        send(av1.at[r], av1.at[r], AV, r_one.at[4], (p, peer(ol, oc), s))
    for k in range(K):
        second(0, k)

    for k in range(K):
        if FORWARD[0][k]:
            forward(0, k)

    @pl.when(upper)
    def _():
        arrived(sel_in, r_one.at[0])
        base_v[...] = dot(sel_in[...], g_v[...], ((1,), (0,)))
        m_v[...] = dot(sel_in[...], sel_s[0], ((1,), (1,)))
        for e in range(2):
            for q in range(4):
                base_o[q, e] = base_v[2 * e : 2 * e + 2, q * Q : q * Q + HA]
        send(base_o, base_in, BASE, r_one.at[2], dev(down, x, y, c))
        send(m_v, m_in, MM, r_one.at[3], dev(down, x, y, c))

    arrived(uv.at[0:3], r_one.at[1])
    for k in range(K):
        u, v = (
            jnp.concatenate(
                [uv[(k - yy) % 4, h, 4 * yy : 4 * yy + 4].astype(F32).reshape(8, HID) for yy in range(8)], axis=0
            )
            for h in range(2)
        )
        sig = jax.nn.sigmoid(u)
        act = u * sig
        coef[k, 0] = v * (sig * (1.0 + u * (1.0 - sig)))
        coef[k, 1] = act
        av = (act * v).astype(BF)
        avt[0, k] = av.astype(F32).T.astype(BF)
    loads[3].wait()
    loads[4].wait()
    loads[5].wait()

    def hidden_gradient(k):
        d_a = dot(ha[0, k].reshape(64, HA), w2[:, 0:HA], ((1,), (1,))) + dot(hd[0, k], w2[:, HA:Q], ((1,), (1,)))
        dx[k, r] = d_a.astype(BF)
        for ol, oc in others:
            send(dx.at[k, r], dx.at[k, r], DX, r_dx.at[k], (p, peer(ol, oc), s))

    def input_gradient(k):
        arrived(dx.at[k, 0:3], r_dx.at[k])
        d_act = (dx[k, 0].astype(F32) + dx[k, 1].astype(F32)) + (dx[k, 2].astype(F32) + dx[k, 3].astype(F32))
        d_gu = jnp.concatenate([(d_act * coef[k, 0]).astype(BF), (d_act * coef[k, 1]).astype(BF)], axis=1)
        pa[k] = dot(d_gu, w13[0:HA, :], ((1,), (1,))).astype(BF).reshape(8, 8, HA)

        def far_a(oy_row, oy_to, slot):
            i = (y + oy_row) % 8
            send(pa.at[k, i], fa.at[k, slot], R1A, r_fa.at[k], dev(p, x, (y + oy_to) % 8, c))

        def near_a(oy):
            i = (y + oy) % 8
            send(pa.at[k, i], ra1.at[k, y], R1A, r_ra1.at[k], dev(p, x, i, c))

        if FORWARD[1][k]:
            far_a(4, 8 + 2 * turn, 2)
            pl.when(at != 0)(functools.partial(far_a, 5, 7, 0))
            pl.when(at == 0)(functools.partial(near_a, 5))
            pl.when(at != 3)(functools.partial(far_a, 3, 1, 1))
            pl.when(at == 3)(functools.partial(near_a, 3))
        else:
            for oy in (4, 3, 5, 2, 6):
                near_a(oy)
        near_a(1)
        near_a(7)
        ra1[k, y] = pa[k, y]
        pb[k] = dot(d_gu, w13[HA:Q, :], ((1,), (1,))).astype(BF).reshape(2, 4, 4, 2, HB)

        def near_b(x_, c_):
            v, i = landing(k, x_, c_)
            send(pb.at[k, :, v, i], rb1.at[k, r * 4 + xh], R1B, r_rb1.at[k], dev(p, x_, y, c_))

        if FORWARD[1][k]:
            for ox, ox_to, c_, slot in BACK:
                v, i = landing(k, (x + ox) % 8, c_)
                send(pb.at[k, :, v, i], fb.at[k, slot], R1B, r_fb.at[k], dev(p, (x + ox_to) % 8, y, c))
            for ox, c_ in ((6, 1), (2, 0), (0, 1 - c)):
                near_b((x + ox) % 8, c_)
        else:
            for ox, oc in ROW:
                near_b((x + ox) % 8, (c + oc) % 2)
        v, i = landing(k, x, c)
        rb1[k, r * 4 + xh] = pb[k, :, v, i]

    def forward_back(k):
        @pl.when(inner)
        def _():
            arrived(fa.at[k], r_fa.at[k])

        @pl.when(jnp.logical_not(inner))
        def _():
            arrived(fa.at[k, 0:2], r_fa.at[k])

        tie = fa[k, 2].astype(F32)
        for slot, oy, tied in ((0, 6, at < 2), (1, 2, at >= 2)):
            i = (y + oy) % 8
            acc = pa[k, i].astype(F32) + fa[k, slot].astype(F32) + jnp.where(tied, tie, 0.0)
            sa[k, slot] = acc.astype(BF)
            send(sa.at[k, slot], ra1.at[k, y], R1A, r_ra1.at[k], dev(p, x, i, c))
        arrived(fb.at[k], r_fb.at[k])
        for slot, ox, c_ in ((2, 6, 0), (5, 2, 1), (0, 7, 0), (1, 7, 1), (3, 1, 0), (4, 1, 1)):
            x_ = (x + ox) % 8
            v, i = landing(k, x_, c_)
            acc = pb[k, :, v, i].astype(F32) + fb[k, slot].astype(F32)
            sb[k, slot] = acc.astype(BF)
            send(sb.at[k, slot], rb1.at[k, r * 4 + xh], R1B, r_rb1.at[k], dev(p, x_, y, c_))

    def to_sources(k):
        if FORWARD[1][k]:
            @pl.when(inner)
            def _():
                arrived(ra1.at[k, 0:5], r_ra1.at[k])

            @pl.when(jnp.logical_not(inner))
            def _():
                arrived(ra1.at[k, 0:4], r_ra1.at[k])
        else:
            arrived(ra1.at[k, 0:7], r_ra1.at[k])
        for e in range(2):
            acc = ra1[k, 4 * e].astype(F32)
            for h in range(1, 4):
                acc = acc + ra1[k, 4 * e + h].astype(F32)
            for h in range(4):
                ta[k, h, e] = acc[2 * h : 2 * h + 2].astype(BF)
        r_ = (k + 8 - y) % 4
        for h in range(4):
            send(ta.at[k, h], ra2.at[r * 4 + xh], R2A, r_ra2, (down, r_, y * 4 + h))
        arrived(rb1.at[k, 0 : 9 if FORWARD[1][k] else 15], r_rb1.at[k])
        for q in range(4):
            acc = rb1[k, 4 * q].astype(F32)
            for h in range(1, 4):
                acc = acc + rb1[k, 4 * q + h].astype(F32)
            for h in range(2):
                tb[k, h, :, q * HB : (q + 1) * HB] = acc[h].astype(BF)
        v = (k + 4 - r) % 4
        for h in range(2):

            def go(h=h):
                send(tb.at[k, h], rb2.at[y], R2B, r_rb2, dev(p, x, v + 4 * h, c))

            pl.when(v + 4 * h != y)(go)

            @pl.when(v + 4 * h == y)
            def _(h=h):
                rb2[y] = tb[k, h]

    def mixed(e, base, m, back):
        for f in range(2):
            for h in range(2):
                base = base + m[2 * e : 2 * e + 2, 2 * f + h : 2 * f + h + 1] * back[f][h : h + 1, :]
        return base.astype(BF)

    def next_rows():
        @pl.when(upper)
        def _():
            arrived(rb2.at[0:7], r_rb2)
            back = []
            for f in range(2):
                acc = rb2[4 * f].astype(F32)
                for h in range(1, 4):
                    acc = acc + rb2[4 * f + h].astype(F32)
                back.append(acc)
            for q in range(4):
                for e in range(2):
                    rows_b[1, e, :, q * HB : (q + 1) * HB] = mixed(
                        e,
                        base_v[2 * e : 2 * e + 2, q * Q + HA : (q + 1) * Q],
                        m_v[...],
                        [b[:, q * HB : (q + 1) * HB] for b in back],
                    )
            first_b(1)

        @pl.when(lower)
        def _():
            arrived(ra2, r_ra2)
            for q in range(4):
                back = []
                for f in range(2):
                    acc = ra2[4 * q, f].astype(F32)
                    for h in range(1, 4):
                        acc = acc + ra2[4 * q + h, f].astype(F32)
                    back.append(acc)
                for e in range(2):
                    rows_a[1, q, e] = mixed(e, base_in[q, e], m_in[...], back)
            first_a(1)

    def gather_rows(k):
        pl.when(mine == k)(next_rows)

    for k in range(K):
        dispatched(0, k)
        pl.when(upper)(functools.partial(hidden_gradient, k))
    for k in range(K):
        pl.when(upper)(functools.partial(input_gradient, k))
    left = jnp.concatenate([avt[0, k] for k in range(K)], axis=1)
    out[0, :, 0:HA] = dot(left, ha[0].reshape(K * 64, HA), ((1,), (0,)))
    out[0, :, HA:Q] = dot(left, hd[0].reshape(K * 64, HB), ((1,), (0,)))
    for k in range(K):
        if FORWARD[1][k]:
            pl.when(upper)(functools.partial(forward_back, k))
    arrived(av1.at[0:3], r_one.at[4])
    for k in range(K):
        av = jnp.concatenate([av1[(k - yy) % 4, 8 * yy : 8 * yy + 8] for yy in range(8)], axis=0)
        avt[1, k] = av.astype(F32).T.astype(BF)

    @pl.when(lower)
    def _():
        arrived(base_in, r_one.at[2])
        arrived(m_in, r_one.at[3])

    def if_lower(step, *args):
        pl.when(lower)(functools.partial(step, *args))

    def finish(k):
        dispatched(1, k)
        out[0, :, 0:HA] += dot(avt[1, k], ha[1, k].reshape(64, HA), ((1,), (0,)))
        out[0, :, HA:Q] += dot(avt[1, k], hd[1, k], ((1,), (0,)))

    pl.when(upper)(functools.partial(to_sources, 0))
    pl.when(upper)(functools.partial(to_sources, 1))
    pl.when(upper)(functools.partial(to_sources, 2))
    pl.when(upper)(functools.partial(to_sources, 3))
    gather_rows(0)
    gather_rows(1)
    gather_rows(2)
    gather_rows(3)
    if_lower(second, 1, 0)
    if_lower(second, 1, 1)
    if_lower(second, 1, 2)
    if_lower(second, 1, 3)
    if FORWARD[2][0]:
        if_lower(forward, 1, 0)
    if FORWARD[2][1]:
        if_lower(forward, 1, 1)
    if FORWARD[2][2]:
        if_lower(forward, 1, 2)
    if FORWARD[2][3]:
        if_lower(forward, 1, 3)
    for k in range(K):
        if_lower(finish, k)

    arrived(ra2.at[0:15], snd.at[D1A])
    arrived(rb2.at[0:7], snd.at[D1B])
    arrived(uv.at[0:3], snd.at[UV])
    arrived(av1.at[0:3], snd.at[AV])

    def drain_second(t):
        arrived(ha.at[0, :, 0:4], snd.at[D2A + t])
        direct = FORWARD[2 * t].count(0)
        if direct:
            arrived(ha.at[0, 0:direct, 0:3], snd.at[D2F + t])
        if direct < K:
            @pl.when(inner)
            def _():
                arrived(ha.at[0, direct:K, 0:4], snd.at[D2F + t])

            @pl.when(jnp.logical_not(inner))
            def _():
                arrived(ha.at[0, direct:K, 0:2], snd.at[D2F + t])

        arrived(fifteen, snd.at[D2B + t])

    drain_second(0)

    @pl.when(lower)
    def _():
        drain_second(1)
        arrived(ra2.at[0:15], snd.at[D1A1])
        arrived(sel_in, snd.at[SEL])

    @pl.when(upper)
    def _():
        arrived(rb2, snd.at[D1B1])
        arrived(dx.at[:, 0:3], snd.at[DX])
        arrived(ra1.at[:, 0:7], snd.at[R1A])
        arrived(fifteen, snd.at[R1B])
        arrived(ra2, snd.at[R2A])
        arrived(rb2.at[0:7], snd.at[R2B])
        arrived(base_in, snd.at[BASE])
        arrived(m_in, snd.at[MM])


def body(cotangent, routes, gates, *others):
    hbm = pl.BlockSpec(memory_space=pl.ANY)
    dma = pltpu.SemaphoreType.DMA
    vmem = pltpu.VMEM
    return pl.pallas_call(
        kernel,
        out_shape=vmem((1, HID, Q), F32),
        in_specs=[hbm] * 8,
        out_specs=pl.BlockSpec(memory_space=vmem),
        scratch_shapes=[
            vmem((TOK, D), BF),
            vmem((2, 8, TOK), jnp.int32),
            vmem((2, 8, TOK), BF),
            vmem((HID, Q), BF),
            vmem((Q, 2 * HID), BF),
            vmem((3, 8, TOK), BF),
            vmem((8, TOK), BF),
            vmem((2, 4, 2, 2, HA), BF),
            vmem((2, 2, 2, 4 * HB), BF),
            vmem((8, D), F32),
            vmem((4, 2, 2, HA), F32),
            vmem((4, 2, 2, HA), F32),
            vmem((8, 8), F32),
            vmem((8, 8), F32),
            vmem((4, 2, 32, 2, HID), BF),
            vmem((2, 32, 2, HID), BF),
            vmem((4, TOK, HID), BF),
            vmem((K, 2, 64, HID), F32),
            vmem((2, K, HID, 64), BF),
            vmem((2, K, 4, 2, 2, HA), BF),
            vmem((2, K, 2, 8, HA), BF),
            vmem((2, 4, 2, 2, 4 * HB), BF),
            vmem((2, K, 8, 8, HA), BF),
            vmem((2, K, 2, 4, 4, 2, HB), BF),
            vmem((2, K, 64, HB), BF),
            vmem((K, 4, 64, HID), BF),
            vmem((K, 8, 8, HA), BF),
            vmem((K, 2, 4, 4, 2, HB), BF),
            vmem((K, 3, 8, HA), BF),
            vmem((K, 6, 2, 2, HB), BF),
            vmem((K, 2, 8, HA), BF),
            vmem((K, 6, 2, 2, HB), BF),
            vmem((K, 8, 8, HA), BF),
            vmem((K, 16, 2, 2, HB), BF),
            vmem((K, 4, 2, 2, HA), BF),
            vmem((K, 2, 2, 4 * HB), BF),
            vmem((16, 2, 2, HA), BF),
            vmem((8, 2, 4 * HB), BF),
            dma((10,)),
            dma((20,)),
            dma((2, K)),
            dma((2, K)),
            dma((2, K)),
            dma((2, K)),
            dma((2, K)),
            dma((2, K)),
            dma((K,)),
            dma((K,)),
            dma((K,)),
            dma((K,)),
            dma((K,)),
            dma,
            dma,
            dma((5,)),
        ],
        compiler_params=pltpu.CompilerParams(collective_id=0, has_side_effects=True),
        name="cooldown",
    )(cotangent, jnp.swapaxes(routes, 2, 3), jnp.swapaxes(gates, 2, 3), *others)


def solution(mesh):
    in_specs = (
        P("pipe", ("dp", "expert"), None),
        P("pipe", None, ("dp", "expert"), None),
        P("pipe", None, ("dp", "expert"), None),
        P("pipe", None, "dp", None, None, "expert"),
        P("pipe", None, "dp", None, None, "expert"),
        P("pipe", None, "expert"),
        P("pipe", None, "expert"),
        P("pipe", "expert", None),
    )
    out_specs = P("pipe", "expert", "dp")
    return jax.shard_map(body, mesh=mesh, in_specs=in_specs, out_specs=out_specs, check_vma=False)
```

```python
import functools

import jax
import jax.numpy as jnp
from jax import lax
from jax.experimental import pallas as pl
from jax.experimental.pallas import tpu as pltpu
from jax.sharding import PartitionSpec as P

MESH = pl.DeviceIdType.MESH
BF = jnp.bfloat16
F32 = jnp.float32

D = 7168
TOK = 64
HID = 128
Q = 1792
HA = 896
HB = Q - HA
K = 4
FAR = (4, 3, 5, 2, 6, 1, 7)
ROW = tuple((dx, dc) for dx in FAR for dc in (0, 1)) + ((0, 1),)
FORWARD = ((1, 1, 1, 1), (1, 1, 1, 1), (1, 1, 1, 1))
NEAR = tuple((dx, dc) for dx in (2, 6, 1, 7) for dc in (0, 1)) + ((0, 1),)
BACK = ((4, 6, 0, 2), (4, 2, 1, 5), (5, 6, 0, 0), (5, 6, 1, 1), (3, 2, 0, 3), (3, 2, 1, 4))
FAR_ROW = tuple((dx, dc) for dx in (4, 3, 5) for dc in (0, 1))


def dot(a, b, dims):
    return lax.dot_general(a, b, (dims, ((), ())), preferred_element_type=F32)


def kernel(
    cot, routes, gates, gate_pre, up_pre, w_gate, w_up, w_down, out,
    g_v, ids_v, gat_v, w2, w13, sel_s, sel_in, rows_a, rows_b, base_v, base_o, base_in, m_v, m_in, uv, uv1, av1, coef, avt,
    xa, a2, yb, ha, hb, hd, dx, pa, pb, fa, fb, sa, sb, ra1, rb1, ta, tb, ra2, rb2,
    ld, snd, r_xa, r_yb, r_ha, r_hb, r_ha2, r_hb2, r_dx, r_fa, r_fb, r_ra1, r_rb1, r_ra2, r_rb2, r_one, ready,
):
    p = lax.axis_index("pipe")
    r = lax.axis_index("dp")
    s = lax.axis_index("expert")
    y = s // 4
    xh = s % 4
    x = xh * 2 + r // 2
    c = r % 2
    lower = p < 7
    upper = p > 0
    up = jnp.minimum(p + 1, 7)
    down = jnp.maximum(p - 1, 0)
    mine = (r + y) % 4
    half = y // 4
    at = y % 4
    inner = (at == 1) | (at == 2)
    turn = jnp.where(at < 2, 1, -1)

    def dev(p_, x_, y_, c_):
        return (p_, (x_ % 2) * 2 + c_, y_ * 4 + x_ // 2)

    def send(src, dst, kind, recv, target):
        pltpu.make_async_remote_copy(
            src_ref=src, dst_ref=dst, send_sem=snd.at[kind], recv_sem=recv, device_id=target, device_id_type=MESH
        ).start()

    def arrived(like, sem):
        pltpu.make_async_copy(like, like, sem).wait()

    D1A, D1A1, D1B, D1B1, D2A, _, D2F, _, D2B, _, DX, R1A, R1B, R2A, R2B, UV, AV, SEL, BASE, MM = range(20)

    barrier = pltpu.get_barrier_semaphore()
    peers = [((x + ox) % 8, y, (c + oc) % 2, p) for ox, oc in ROW]
    peers += [(x, (y + oy) % 8, c, p) for oy in FAR]
    for x_, y_, c_, p_ in peers:
        pl.semaphore_signal(barrier, inc=1, device_id=dev(p_, x_, y_, c_), device_id_type=MESH)

    @pl.when(lower & upper)
    def _():
        pl.semaphore_signal(barrier, inc=1, device_id=dev(up, x, y, c), device_id_type=MESH)

    @pl.when(p == 1)
    def _():
        pl.semaphore_signal(barrier, inc=1, device_id=dev(down, x, y, c), device_id_type=MESH)

    q0 = pl.multiple_of(r * Q, 128)
    loads = [
        pltpu.make_async_copy(routes.at[0], ids_v, ld.at[0]),
        pltpu.make_async_copy(gates.at[0], gat_v, ld.at[1]),
        pltpu.make_async_copy(cot.at[0], g_v, ld.at[2]),
        pltpu.make_async_copy(w_down.at[0, :, pl.ds(q0, Q)], w2, ld.at[3]),
        pltpu.make_async_copy(w_gate.at[0, pl.ds(q0, Q)], w13.at[:, 0:HID], ld.at[4]),
        pltpu.make_async_copy(w_up.at[0, pl.ds(q0, Q)], w13.at[:, HID : 2 * HID], ld.at[5]),
        pltpu.make_async_copy(gate_pre.at[0, 0, 0], uv.at[r, 0], ld.at[6]),
        pltpu.make_async_copy(up_pre.at[0, 0, 0], uv.at[r, 1], ld.at[7]),
        pltpu.make_async_copy(gate_pre.at[0, 1, 0], uv1.at[0], ld.at[8]),
        pltpu.make_async_copy(up_pre.at[0, 1, 0], uv1.at[1], ld.at[9]),
    ]
    for cp in loads:
        cp.start()

    loads[0].wait()
    loads[1].wait()
    row = lax.broadcasted_iota(jnp.int32, (8, TOK), 0)
    upto = (
        lax.broadcasted_iota(jnp.int32, (TOK, TOK), 0) <= lax.broadcasted_iota(jnp.int32, (TOK, TOK), 1)
    ).astype(F32).astype(BF)
    for t in range(2):
        ids = ids_v[t]
        gat = gat_v[t].astype(F32)
        hit = jnp.zeros((8, TOK), F32)
        gsum = jnp.zeros((8, TOK), F32)
        for e in range(2):
            match = (ids == e).astype(F32)
            of_e = (row >= 2 * e) & (row < 2 * e + 2)
            hit = jnp.where(of_e, jnp.sum(match, axis=0, keepdims=True), hit)
            gsum = jnp.where(of_e, jnp.sum(match * gat, axis=0, keepdims=True), gsum)
        rank = dot(hit.astype(BF), upto, ((1,), (0,))) - 1.0
        sel = hit * (rank == (row & 1).astype(F32)).astype(F32)
        if t == 0:
            sel_s[0] = sel.astype(BF)
        sel_s[1 + t] = (sel * gsum).astype(BF)

    loads[2].wait()
    rows = dot(sel_s[1], g_v[...], ((1,), (0,)))
    for e in range(2):
        for q in range(4):
            rows_a[0, q, e] = rows[2 * e : 2 * e + 2, q * Q : q * Q + HA].astype(BF)
            rows_b[0, e, :, q * HB : (q + 1) * HB] = rows[2 * e : 2 * e + 2, q * Q + HA : (q + 1) * Q].astype(BF)

    for k in range(K):
        if FORWARD[1][k]:
            zeros = jnp.zeros((8, HA), BF)
            ra1[k, (y + 4) % 8] = zeros
            for where, oy in ((1, 3), (2, 5)):
                @pl.when(at != where)
                def _(k=k, oy=oy):
                    ra1[k, (y + oy) % 8] = jnp.zeros((8, HA), BF)

            for where, slot in ((3, 0), (0, 1)):
                @pl.when(at == where)
                def _(k=k, slot=slot):
                    fa[k, slot] = jnp.zeros((8, HA), BF)

            for ox in (3, 4, 5):
                for c_ in range(2):
                    x_ = (x + ox) % 8
                    rb1[k, ((x_ % 2) * 2 + c_) * 4 + x_ // 2] = jnp.zeros((2, 2, HB), BF)

    @pl.when(p != 1)
    def _():
        pl.semaphore_wait(barrier, len(peers) + 1)

    @pl.when(p == 1)
    def _():
        pl.semaphore_wait(barrier, len(peers))

    @pl.when(p > 1)
    def _():
        pl.semaphore_signal(ready, inc=1, device_id=dev(down, x, y, c), device_id_type=MESH)

    def first_a(t):
        for ox, oc in ROW:
            x_, c_ = (x + ox) % 8, (c + oc) % 2
            q_ = (x_ % 2) * 2 + c_
            send(rows_a.at[t, q_], xa.at[t, mine, xh], D1A + t, r_xa.at[t, mine], dev(p, x_, y, c_))
        xa[t, mine, xh] = rows_a[t, r]

    def first_b(t):
        for oy in FAR + (0,) * t:
            y_ = (y + oy) % 8
            send(
                rows_b.at[t, y_ // 4], yb.at[t, y % 4, half], D1B + t, r_yb.at[t, mine], dev((p, down)[t], x, y_, c)
            )
        if t == 0:
            yb[t, y % 4, half] = rows_b[t, half]

    def send_b(t, k, x_, c_, sem):
        v = (k + 4 - r) % 4
        columns = pl.ds(pl.multiple_of(((x_ % 2) * 2 + c_) * HB, 128), HB)
        send(yb.at[t, v, :, :, columns], hb.at[t, k, :, v, xh], D2B + t, sem.at[t, k], dev(p, x_, y, c_))

    def direct_a(t, k, oy):
        y_ = (y + oy) % 8
        send(a2.at[t, k, y_ // 4], ha.at[t, k, y], D2F + t, r_ha2.at[t, k], dev(p, x, y_, c))

    def second(t, k):
        @pl.when(mine == k)
        def _():
            arrived(xa.at[t, k, 0:3], r_xa.at[t, k])

        @pl.when(mine != k)
        def _():
            arrived(xa.at[t, k], r_xa.at[t, k])

        for e in range(2):
            a2[t, k, e] = jnp.concatenate([xa[t, k, h, e] for h in range(4)], axis=0)
        for oy in (2, 6, 1, 7):
            y_ = (y + oy) % 8
            send(a2.at[t, k, y_ // 4], ha.at[t, k, y], D2A + t, r_ha.at[t, k], dev(p, x, y_, c))
        if not FORWARD[2 * t][k]:
            for oy in (4, 3, 5):
                direct_a(t, k, oy)
        ha[t, k, y] = a2[t, k, half]
        v = (k + 4 - r) % 4
        if t == 0:
            @pl.when(mine == k)
            def _():
                arrived(yb.at[t, k, 0], r_yb.at[t, k])

            @pl.when(mine != k)
            def _():
                arrived(yb.at[t, k], r_yb.at[t, k])
        else:
            arrived(yb.at[t, k], r_yb.at[t, k])
        for ox, oc in NEAR:
            send_b(t, k, (x + ox) % 8, (c + oc) % 2, r_hb)
        if not FORWARD[2 * t][k]:
            for ox, oc in FAR_ROW:
                send_b(t, k, (x + ox) % 8, (c + oc) % 2, r_hb2)
        hb[t, k, :, v, xh] = yb[t, v, :, :, pl.ds(pl.multiple_of(r * HB, 128), HB)]

    def landing(k, x_, c_):
        return (k + 4 - ((x_ % 2) * 2 + c_)) % 4, x_ // 2

    def forward(t, k):
        pl.when(at == 1)(functools.partial(direct_a, t, k, 3))
        pl.when(at == 2)(functools.partial(direct_a, t, k, 5))
        arrived(ha.at[t, k, 0:4], r_ha.at[t, k])

        def pass_a(oy_from, oy_to):
            i = (y + oy_from) % 8
            send(ha.at[t, k, i], ha.at[t, k, i], D2F + t, r_ha2.at[t, k], dev(p, x, (y + oy_to) % 8, c))

        pass_a(8 - 2 * turn, 8 + 2 * turn)
        pl.when(at != 3)(functools.partial(pass_a, 6, 1))
        pl.when(at != 0)(functools.partial(pass_a, 2, 7))
        arrived(nine, r_hb.at[t, k])
        for ox_from, ox_to, cores in ((6, 2, (0,)), (2, 6, (1,)), (7, 2, (0, 1)), (1, 6, (0, 1))):
            for c_ in cores:
                v, i = landing(k, (x + ox_from) % 8, c_)
                send(
                    hb.at[t, k, :, v, i], hb.at[t, k, :, v, i], D2B + t, r_hb2.at[t, k], dev(p, (x + ox_to) % 8, y, c)
                )

    nine, six, fifteen = rb1.at[0, 0:9], rb1.at[0, 0:6], rb1.at[:, 0:15]

    def dispatched(t, k):
        if not FORWARD[2 * t][k]:
            arrived(ha.at[t, k, 0:4], r_ha.at[t, k])
            arrived(nine, r_hb.at[t, k])
        arrived(ha.at[t, k, 0:3], r_ha2.at[t, k])
        arrived(six, r_hb2.at[t, k])
        hd[t, k] = hb[t, k].reshape(64, HB)

    others = [(ol, oc) for ol in (0, 1) for oc in (0, 1) if (ol, oc) != (0, 0)]

    def peer(ol, oc):
        return ((r // 2 + ol) % 2) * 2 + (c + oc) % 2

    first_a(0)
    first_b(0)
    loads[6].wait()
    loads[7].wait()
    for ol, oc in others:
        send(uv.at[r], uv.at[r], UV, r_one.at[1], (p, peer(ol, oc), s))
    loads[8].wait()
    loads[9].wait()
    u, v = (uv1[h].astype(F32).reshape(TOK, HID) for h in range(2))
    av1[r] = (u * jax.nn.sigmoid(u) * v).astype(BF)
    for ol, oc in others:
        send(av1.at[r], av1.at[r], AV, r_one.at[4], (p, peer(ol, oc), s))
    @pl.when(lower & upper)
    def _():
        pl.semaphore_wait(ready, 1)

    @pl.when(lower)
    def _():
        send(sel_s.at[2], sel_in, SEL, r_one.at[0], dev(up, x, y, c))

    for k in range(K):
        second(0, k)

    for k in range(K):
        if FORWARD[0][k]:
            forward(0, k)

    @pl.when(upper)
    def _():
        arrived(sel_in, r_one.at[0])
        base_v[...] = dot(sel_in[...], g_v[...], ((1,), (0,)))
        m_v[...] = dot(sel_in[...], sel_s[0], ((1,), (1,)))
        for e in range(2):
            for q in range(4):
                base_o[q, e] = base_v[2 * e : 2 * e + 2, q * Q : q * Q + HA]
        send(base_o, base_in, BASE, r_one.at[2], dev(down, x, y, c))
        send(m_v, m_in, MM, r_one.at[3], dev(down, x, y, c))

    arrived(uv.at[0:3], r_one.at[1])
    for k in range(K):
        u, v = (
            jnp.concatenate(
                [uv[(k - yy) % 4, h, 4 * yy : 4 * yy + 4].astype(F32).reshape(8, HID) for yy in range(8)], axis=0
            )
            for h in range(2)
        )
        sig = jax.nn.sigmoid(u)
        act = u * sig
        coef[k, 0] = v * (sig * (1.0 + u * (1.0 - sig)))
        coef[k, 1] = act
        av = (act * v).astype(BF)
        avt[0, k] = av.astype(F32).T.astype(BF)
    loads[3].wait()
    loads[4].wait()
    loads[5].wait()

    def hidden_gradient(k):
        d_a = dot(ha[0, k].reshape(64, HA), w2[:, 0:HA], ((1,), (1,))) + dot(hd[0, k], w2[:, HA:Q], ((1,), (1,)))
        dx[k, r] = d_a.astype(BF)
        for ol, oc in others:
            send(dx.at[k, r], dx.at[k, r], DX, r_dx.at[k], (p, peer(ol, oc), s))

    def near_a(k, oy):
        i = (y + oy) % 8
        send(pa.at[k, i], ra1.at[k, y], R1A, r_ra1.at[k], dev(p, x, i, c))

    def near_b(k, x_, c_):
        v, i = landing(k, x_, c_)
        send(pb.at[k, :, v, i], rb1.at[k, r * 4 + xh], R1B, r_rb1.at[k], dev(p, x_, y, c_))

    def input_gradient(k):
        arrived(dx.at[k, 0:3], r_dx.at[k])
        d_act = (dx[k, 0].astype(F32) + dx[k, 1].astype(F32)) + (dx[k, 2].astype(F32) + dx[k, 3].astype(F32))
        d_gu = jnp.concatenate([(d_act * coef[k, 0]).astype(BF), (d_act * coef[k, 1]).astype(BF)], axis=1)
        pa[k] = dot(d_gu, w13[0:HA, :], ((1,), (1,))).astype(BF).reshape(8, 8, HA)

        def far_a(oy_row, oy_to, slot):
            i = (y + oy_row) % 8
            send(pa.at[k, i], fa.at[k, slot], R1A, r_fa.at[k], dev(p, x, (y + oy_to) % 8, c))

        if FORWARD[1][k]:
            far_a(4, 8 + 2 * turn, 2)
            pl.when(at != 0)(functools.partial(far_a, 5, 7, 0))
            pl.when(at == 0)(functools.partial(near_a, k, 5))
            pl.when(at != 3)(functools.partial(far_a, 3, 1, 1))
            pl.when(at == 3)(functools.partial(near_a, k, 3))
        else:
            for oy in (4, 3, 5, 2, 6):
                near_a(k, oy)
            near_a(k, 1)
            near_a(k, 7)
        ra1[k, y] = pa[k, y]
        pb[k] = dot(d_gu, w13[HA:Q, :], ((1,), (1,))).astype(BF).reshape(2, 4, 4, 2, HB)

        if FORWARD[1][k]:
            for ox, ox_to, c_, slot in BACK:
                v, i = landing(k, (x + ox) % 8, c_)
                send(pb.at[k, :, v, i], fb.at[k, slot], R1B, r_fb.at[k], dev(p, (x + ox_to) % 8, y, c))
        else:
            for ox, oc in ROW:
                near_b(k, (x + ox) % 8, (c + oc) % 2)
        v, i = landing(k, x, c)
        rb1[k, r * 4 + xh] = pb[k, :, v, i]

    def forward_back(k):
        near_a(k, 1)
        near_a(k, 7)
        for ox, c_ in ((6, 1), (2, 0), (0, 1 - c)):
            near_b(k, (x + ox) % 8, c_)
        @pl.when(inner)
        def _():
            arrived(fa.at[k], r_fa.at[k])

        @pl.when(jnp.logical_not(inner))
        def _():
            arrived(fa.at[k, 0:2], r_fa.at[k])

        tie = fa[k, 2].astype(F32)
        for slot, oy, tied in ((0, 6, at < 2), (1, 2, at >= 2)):
            i = (y + oy) % 8
            acc = pa[k, i].astype(F32) + fa[k, slot].astype(F32) + jnp.where(tied, tie, 0.0)
            sa[k, slot] = acc.astype(BF)
            send(sa.at[k, slot], ra1.at[k, y], R1A, r_ra1.at[k], dev(p, x, i, c))
        arrived(fb.at[k], r_fb.at[k])
        for slot, ox, c_ in ((2, 6, 0), (5, 2, 1), (0, 7, 0), (1, 7, 1), (3, 1, 0), (4, 1, 1)):
            x_ = (x + ox) % 8
            v, i = landing(k, x_, c_)
            acc = pb[k, :, v, i].astype(F32) + fb[k, slot].astype(F32)
            sb[k, slot] = acc.astype(BF)
            send(sb.at[k, slot], rb1.at[k, r * 4 + xh], R1B, r_rb1.at[k], dev(p, x_, y, c_))

    def to_sources(k):
        if FORWARD[1][k]:
            @pl.when(inner)
            def _():
                arrived(ra1.at[k, 0:5], r_ra1.at[k])

            @pl.when(jnp.logical_not(inner))
            def _():
                arrived(ra1.at[k, 0:4], r_ra1.at[k])
        else:
            arrived(ra1.at[k, 0:7], r_ra1.at[k])
        for e in range(2):
            acc = ra1[k, 4 * e].astype(F32)
            for h in range(1, 4):
                acc = acc + ra1[k, 4 * e + h].astype(F32)
            for h in range(4):
                ta[k, h, e] = acc[2 * h : 2 * h + 2].astype(BF)
        r_ = (k + 8 - y) % 4
        for h in range(4):
            send(ta.at[k, h], ra2.at[r * 4 + xh], R2A, r_ra2, (down, r_, y * 4 + h))
        arrived(rb1.at[k, 0 : 9 if FORWARD[1][k] else 15], r_rb1.at[k])
        for q in range(4):
            acc = rb1[k, 4 * q].astype(F32)
            for h in range(1, 4):
                acc = acc + rb1[k, 4 * q + h].astype(F32)
            for h in range(2):
                tb[k, h, :, q * HB : (q + 1) * HB] = acc[h].astype(BF)
        v = (k + 4 - r) % 4
        for h in range(2):

            def go(h=h):
                send(tb.at[k, h], rb2.at[y], R2B, r_rb2, dev(p, x, v + 4 * h, c))

            pl.when(v + 4 * h != y)(go)

            @pl.when(v + 4 * h == y)
            def _(h=h):
                rb2[y] = tb[k, h]

    def mixed(e, base, m, back):
        for f in range(2):
            for h in range(2):
                base = base + m[2 * e : 2 * e + 2, 2 * f + h : 2 * f + h + 1] * back[f][h : h + 1, :]
        return base.astype(BF)

    def next_rows():
        @pl.when(upper)
        def _():
            arrived(rb2.at[0:7], r_rb2)
            back = []
            for f in range(2):
                acc = rb2[4 * f].astype(F32)
                for h in range(1, 4):
                    acc = acc + rb2[4 * f + h].astype(F32)
                back.append(acc)
            for q in range(4):
                for e in range(2):
                    rows_b[1, e, :, q * HB : (q + 1) * HB] = mixed(
                        e,
                        base_v[2 * e : 2 * e + 2, q * Q + HA : (q + 1) * Q],
                        m_v[...],
                        [b[:, q * HB : (q + 1) * HB] for b in back],
                    )
            first_b(1)

        @pl.when(lower)
        def _():
            arrived(ra2, r_ra2)
            for q in range(4):
                back = []
                for f in range(2):
                    acc = ra2[4 * q, f].astype(F32)
                    for h in range(1, 4):
                        acc = acc + ra2[4 * q + h, f].astype(F32)
                    back.append(acc)
                for e in range(2):
                    rows_a[1, q, e] = mixed(e, base_in[q, e], m_in[...], back)
            first_a(1)

    def gather_rows(k):
        pl.when(mine == k)(next_rows)

    for k in range(K):
        dispatched(0, k)
        pl.when(upper)(functools.partial(hidden_gradient, k))
    for k in range(K):
        pl.when(upper)(functools.partial(input_gradient, k))
    left = jnp.concatenate([avt[0, k] for k in range(K)], axis=1)
    out[0, :, 0:HA] = dot(left, ha[0].reshape(K * 64, HA), ((1,), (0,)))
    out[0, :, HA:Q] = dot(left, hd[0].reshape(K * 64, HB), ((1,), (0,)))
    for k in range(K):
        if FORWARD[1][k]:
            pl.when(upper)(functools.partial(forward_back, k))
    arrived(av1.at[0:3], r_one.at[4])
    for k in range(K):
        av = jnp.concatenate([av1[(k - yy) % 4, 8 * yy : 8 * yy + 8] for yy in range(8)], axis=0)
        avt[1, k] = av.astype(F32).T.astype(BF)

    @pl.when(lower)
    def _():
        arrived(base_in, r_one.at[2])
        arrived(m_in, r_one.at[3])

    def if_lower(step, *args):
        pl.when(lower)(functools.partial(step, *args))

    def finish(k):
        dispatched(1, k)
        out[0, :, 0:HA] += dot(avt[1, k], ha[1, k].reshape(64, HA), ((1,), (0,)))
        out[0, :, HA:Q] += dot(avt[1, k], hd[1, k], ((1,), (0,)))

    pl.when(upper)(functools.partial(to_sources, 0))
    pl.when(upper)(functools.partial(to_sources, 1))
    pl.when(upper)(functools.partial(to_sources, 2))
    pl.when(upper)(functools.partial(to_sources, 3))
    gather_rows(0)
    gather_rows(1)
    gather_rows(2)
    gather_rows(3)
    if_lower(second, 1, 0)
    if_lower(second, 1, 1)
    if_lower(second, 1, 2)
    if_lower(second, 1, 3)
    if FORWARD[2][0]:
        if_lower(forward, 1, 0)
    if FORWARD[2][1]:
        if_lower(forward, 1, 1)
    if FORWARD[2][2]:
        if_lower(forward, 1, 2)
    if FORWARD[2][3]:
        if_lower(forward, 1, 3)
    for k in range(K):
        if_lower(finish, k)

    arrived(ra2.at[0:15], snd.at[D1A])
    arrived(rb2.at[0:7], snd.at[D1B])
    arrived(uv.at[0:3], snd.at[UV])
    arrived(av1.at[0:3], snd.at[AV])

    def drain_second(t):
        arrived(ha.at[0, :, 0:4], snd.at[D2A + t])
        direct = FORWARD[2 * t].count(0)
        if direct:
            arrived(ha.at[0, 0:direct, 0:3], snd.at[D2F + t])
        if direct < K:
            @pl.when(inner)
            def _():
                arrived(ha.at[0, direct:K, 0:4], snd.at[D2F + t])

            @pl.when(jnp.logical_not(inner))
            def _():
                arrived(ha.at[0, direct:K, 0:2], snd.at[D2F + t])

        arrived(fifteen, snd.at[D2B + t])

    drain_second(0)

    @pl.when(lower)
    def _():
        drain_second(1)
        arrived(ra2.at[0:15], snd.at[D1A1])
        arrived(sel_in, snd.at[SEL])

    @pl.when(upper)
    def _():
        arrived(rb2, snd.at[D1B1])
        arrived(dx.at[:, 0:3], snd.at[DX])
        arrived(ra1.at[:, 0:7], snd.at[R1A])
        arrived(fifteen, snd.at[R1B])
        arrived(ra2, snd.at[R2A])
        arrived(rb2.at[0:7], snd.at[R2B])
        arrived(base_in, snd.at[BASE])
        arrived(m_in, snd.at[MM])


def body(cotangent, routes, gates, *others):
    hbm = pl.BlockSpec(memory_space=pl.ANY)
    dma = pltpu.SemaphoreType.DMA
    vmem = pltpu.VMEM
    return pl.pallas_call(
        kernel,
        out_shape=vmem((1, HID, Q), F32),
        in_specs=[hbm] * 8,
        out_specs=pl.BlockSpec(memory_space=vmem),
        scratch_shapes=[
            vmem((TOK, D), BF),
            vmem((2, 8, TOK), jnp.int32),
            vmem((2, 8, TOK), BF),
            vmem((HID, Q), BF),
            vmem((Q, 2 * HID), BF),
            vmem((3, 8, TOK), BF),
            vmem((8, TOK), BF),
            vmem((2, 4, 2, 2, HA), BF),
            vmem((2, 2, 2, 4 * HB), BF),
            vmem((8, D), F32),
            vmem((4, 2, 2, HA), F32),
            vmem((4, 2, 2, HA), F32),
            vmem((8, 8), F32),
            vmem((8, 8), F32),
            vmem((4, 2, 32, 2, HID), BF),
            vmem((2, 32, 2, HID), BF),
            vmem((4, TOK, HID), BF),
            vmem((K, 2, 64, HID), F32),
            vmem((2, K, HID, 64), BF),
            vmem((2, K, 4, 2, 2, HA), BF),
            vmem((2, K, 2, 8, HA), BF),
            vmem((2, 4, 2, 2, 4 * HB), BF),
            vmem((2, K, 8, 8, HA), BF),
            vmem((2, K, 2, 4, 4, 2, HB), BF),
            vmem((2, K, 64, HB), BF),
            vmem((K, 4, 64, HID), BF),
            vmem((K, 8, 8, HA), BF),
            vmem((K, 2, 4, 4, 2, HB), BF),
            vmem((K, 3, 8, HA), BF),
            vmem((K, 6, 2, 2, HB), BF),
            vmem((K, 2, 8, HA), BF),
            vmem((K, 6, 2, 2, HB), BF),
            vmem((K, 8, 8, HA), BF),
            vmem((K, 16, 2, 2, HB), BF),
            vmem((K, 4, 2, 2, HA), BF),
            vmem((K, 2, 2, 4 * HB), BF),
            vmem((16, 2, 2, HA), BF),
            vmem((8, 2, 4 * HB), BF),
            dma((10,)),
            dma((20,)),
            dma((2, K)),
            dma((2, K)),
            dma((2, K)),
            dma((2, K)),
            dma((2, K)),
            dma((2, K)),
            dma((K,)),
            dma((K,)),
            dma((K,)),
            dma((K,)),
            dma((K,)),
            dma,
            dma,
            dma((5,)),
            pltpu.SemaphoreType.REGULAR,
        ],
        compiler_params=pltpu.CompilerParams(collective_id=0, has_side_effects=True),
        name="cooldown",
    )(cotangent, jnp.swapaxes(routes, 2, 3), jnp.swapaxes(gates, 2, 3), *others)


def solution(mesh):
    in_specs = (
        P("pipe", ("dp", "expert"), None),
        P("pipe", None, ("dp", "expert"), None),
        P("pipe", None, ("dp", "expert"), None),
        P("pipe", None, "dp", None, None, "expert"),
        P("pipe", None, "dp", None, None, "expert"),
        P("pipe", None, "expert"),
        P("pipe", None, "expert"),
        P("pipe", "expert", None),
    )
    out_specs = P("pipe", "expert", "dp")
    return jax.shard_map(body, mesh=mesh, in_specs=in_specs, out_specs=out_specs, check_vma=False)
```

```python
import functools

import jax
import jax.numpy as jnp
from jax import lax
from jax.experimental import pallas as pl
from jax.experimental.pallas import tpu as pltpu
from jax.sharding import PartitionSpec as P

MESH = pl.DeviceIdType.MESH
BF = jnp.bfloat16
F32 = jnp.float32

D = 7168
TOK = 64
HID = 128
Q = 1792
HA = HB = 896
K = 4
FAR = (4, 3, 5, 2, 6, 1, 7)
ROW = tuple((dx, dc) for dx in FAR for dc in (0, 1)) + ((0, 1),)
NEAR = tuple((dx, dc) for dx in (2, 6, 1, 7) for dc in (0, 1)) + ((0, 1),)
BACK = ((4, 6, 0, 2), (4, 2, 1, 5), (5, 6, 0, 0), (5, 6, 1, 1), (3, 2, 0, 3), (3, 2, 1, 4))
A8, B4, ROWS2, DX64, UV128 = 14, 7, 14, 16, 32


def dot(a, b, dims):
    return lax.dot_general(a, b, (dims, ((), ())), preferred_element_type=F32)


def kernel(
    cot, routes, gates, gate_pre, up_pre, w_gate, w_up, w_down, out,
    g_v, ids_v, gat_v, w2, w13, w2t, w13t, sel_s, sel_in, rows_a, rows_b, base_v, base_o, base_in, m_v, m_in, uv, uv1, av1, coef, avt,
    void, xa, a2, yb, ha, hb, hd, dx, pa, pb, fa, fb, sa, sb, ra1, rb1, ta, tb, ra2, rb2,
    ld, snd, r_x, r_near, r_far, r_dx, r_f, r_back, r_ra2, r_rb2, r_one, ready, r_x2, r_near2, r_f2, r_back2,
):
    p = lax.axis_index("pipe")
    r = lax.axis_index("dp")
    s = lax.axis_index("expert")
    y = s // 4
    xh = s % 4
    x = xh * 2 + r // 2
    c = r % 2
    lower = p < 7
    upper = p > 0
    up = jnp.minimum(p + 1, 7)
    down = jnp.maximum(p - 1, 0)
    mine = (r + y) % 4
    half = y // 4
    at = y % 4
    inner = (at == 1) | (at == 2)
    turn = jnp.where(at < 2, 1, -1)

    def dev(p_, x_, y_, c_):
        return (p_, (x_ % 2) * 2 + c_, y_ * 4 + x_ // 2)

    def send(src, dst, kind, recv, target):
        pltpu.make_async_remote_copy(
            src_ref=src, dst_ref=dst, send_sem=snd.at[kind], recv_sem=recv, device_id=target, device_id_type=MESH
        ).start()

    def arrived(like, sem):
        pltpu.make_async_copy(like, like, sem).wait()

    def arrived_kib(size, sem):
        arrived(void.at[0:size], sem)

    ALL, LOWER, UPPER, SEL, MM = range(5)

    barrier = pltpu.get_barrier_semaphore()
    peers = [((x + ox) % 8, y, (c + oc) % 2, p) for ox, oc in ROW]
    peers += [(x, (y + oy) % 8, c, p) for oy in FAR]
    for x_, y_, c_, p_ in peers:
        pl.semaphore_signal(barrier, inc=1, device_id=dev(p_, x_, y_, c_), device_id_type=MESH)

    @pl.when(lower & upper)
    def _():
        pl.semaphore_signal(barrier, inc=1, device_id=dev(up, x, y, c), device_id_type=MESH)

    @pl.when(p == 1)
    def _():
        pl.semaphore_signal(barrier, inc=1, device_id=dev(down, x, y, c), device_id_type=MESH)

    q0 = pl.multiple_of(r * Q, 128)
    loads = [
        pltpu.make_async_copy(routes.at[0], ids_v, ld.at[0]),
        pltpu.make_async_copy(gates.at[0], gat_v, ld.at[1]),
        pltpu.make_async_copy(cot.at[0], g_v, ld.at[2]),
        pltpu.make_async_copy(w_down.at[0, :, pl.ds(q0, Q)], w2, ld.at[3]),
        pltpu.make_async_copy(w_gate.at[0, pl.ds(q0, Q)], w13.at[:, 0:HID], ld.at[3]),
        pltpu.make_async_copy(w_up.at[0, pl.ds(q0, Q)], w13.at[:, HID : 2 * HID], ld.at[3]),
        pltpu.make_async_copy(gate_pre.at[0, 0, 0], uv.at[r, 0], ld.at[4]),
        pltpu.make_async_copy(up_pre.at[0, 0, 0], uv.at[r, 1], ld.at[4]),
        pltpu.make_async_copy(gate_pre.at[0, 1, 0], uv1.at[0], ld.at[4]),
        pltpu.make_async_copy(up_pre.at[0, 1, 0], uv1.at[1], ld.at[4]),
    ]
    for cp in loads:
        cp.start()

    loads[0].wait()
    loads[1].wait()
    row = lax.broadcasted_iota(jnp.int32, (8, TOK), 0)
    upto = (
        lax.broadcasted_iota(jnp.int32, (TOK, TOK), 0) <= lax.broadcasted_iota(jnp.int32, (TOK, TOK), 1)
    ).astype(F32).astype(BF)
    for t in range(2):
        ids = ids_v[t]
        gat = gat_v[t].astype(F32)
        hit = jnp.zeros((8, TOK), F32)
        gsum = jnp.zeros((8, TOK), F32)
        for e in range(2):
            match = (ids == e).astype(F32)
            of_e = (row >= 2 * e) & (row < 2 * e + 2)
            hit = jnp.where(of_e, jnp.sum(match, axis=0, keepdims=True), hit)
            gsum = jnp.where(of_e, jnp.sum(match * gat, axis=0, keepdims=True), gsum)
        rank = dot(hit.astype(BF), upto, ((1,), (0,))) - 1.0
        sel = hit * (rank == (row & 1).astype(F32)).astype(F32)
        if t == 0:
            sel_s[0] = sel.astype(BF)
        sel_s[1 + t] = (sel * gsum).astype(BF)

    loads[2].wait()
    rows = dot(sel_s[1], g_v[...], ((1,), (0,)))
    for e in range(2):
        for q in range(4):
            rows_a[0, q, e] = rows[2 * e : 2 * e + 2, q * Q : q * Q + HA].astype(BF)
            rows_b[0, e, :, q * HB : (q + 1) * HB] = rows[2 * e : 2 * e + 2, q * Q + HA : (q + 1) * Q].astype(BF)

    for k in range(K):
        ra1[k, (y + 4) % 8] = jnp.zeros((8, HA), BF)
        for where, oy in ((1, 3), (2, 5)):
            @pl.when(at != where)
            def _(k=k, oy=oy):
                ra1[k, (y + oy) % 8] = jnp.zeros((8, HA), BF)

        for where, slot in ((3, 0), (0, 1)):
            @pl.when(at == where)
            def _(k=k, slot=slot):
                fa[k, slot] = jnp.zeros((8, HA), BF)

        for ox in (3, 4, 5):
            for c_ in range(2):
                x_ = (x + ox) % 8
                rb1[k, ((x_ % 2) * 2 + c_) * 4 + x_ // 2] = jnp.zeros((2, 2, HB), BF)

    @pl.when(p != 1)
    def _():
        pl.semaphore_wait(barrier, len(peers) + 1)

    @pl.when(p == 1)
    def _():
        pl.semaphore_wait(barrier, len(peers))

    @pl.when(p > 1)
    def _():
        pl.semaphore_signal(ready, inc=1, device_id=dev(down, x, y, c), device_id_type=MESH)

    def first_a(t):
        for ox, oc in ROW:
            x_, c_ = (x + ox) % 8, (c + oc) % 2
            q_ = (x_ % 2) * 2 + c_
            send(rows_a.at[t, q_], xa.at[t, mine, xh], (ALL, LOWER)[t], r_x.at[t, mine], dev(p, x_, y, c_))
        xa[t, mine, xh] = rows_a[t, r]

    def first_b(t):
        for oy in FAR + (0,) * t:
            y_ = (y + oy) % 8
            send(
                rows_b.at[t, y_ // 4], yb.at[t, y % 4, half], (ALL, UPPER)[t], r_x2.at[t, mine], dev((p, down)[t], x, y_, c)
            )
        if t == 0:
            yb[t, y % 4, half] = rows_b[t, half]

    def send_b(t, k, x_, c_):
        v = (k + 4 - r) % 4
        columns = pl.ds(pl.multiple_of(((x_ % 2) * 2 + c_) * HB, 128), HB)
        send(yb.at[t, v, :, :, columns], hb.at[t, k, :, v, xh], (ALL, LOWER)[t], r_near2.at[t, k], dev(p, x_, y, c_))

    def direct_a(t, k, oy):
        y_ = (y + oy) % 8
        send(a2.at[t, k, y_ // 4], ha.at[t, k, y], (ALL, LOWER)[t], r_far.at[t, k], dev(p, x, y_, c))

    def second(t, k):
        @pl.when(mine == k)
        def _():
            arrived_kib(3 * B4, r_x.at[t, k])

        @pl.when(mine != k)
        def _():
            arrived_kib(4 * B4, r_x.at[t, k])

        for e in range(2):
            a2[t, k, e] = jnp.concatenate([xa[t, k, h, e] for h in range(4)], axis=0)
        for oy in (2, 6, 1, 7):
            y_ = (y + oy) % 8
            send(a2.at[t, k, y_ // 4], ha.at[t, k, y], (ALL, LOWER)[t], r_near.at[t, k], dev(p, x, y_, c))
        ha[t, k, y] = a2[t, k, half]
        if t == 0:
            @pl.when(mine == k)
            def _():
                arrived_kib(ROWS2, r_x2.at[t, k])

            @pl.when(mine != k)
            def _():
                arrived_kib(2 * ROWS2, r_x2.at[t, k])
        else:
            arrived_kib(2 * ROWS2, r_x2.at[t, k])
        v = (k + 4 - r) % 4
        for ox, oc in NEAR:
            send_b(t, k, (x + ox) % 8, (c + oc) % 2)
        hb[t, k, :, v, xh] = yb[t, v, :, :, pl.ds(pl.multiple_of(r * HB, 128), HB)]

    def landing(k, x_, c_):
        return (k + 4 - ((x_ % 2) * 2 + c_)) % 4, x_ // 2

    def forward(t, k):
        pl.when(at == 1)(functools.partial(direct_a, t, k, 3))
        pl.when(at == 2)(functools.partial(direct_a, t, k, 5))
        arrived_kib(4 * A8, r_near.at[t, k])

        def pass_a(oy_from, oy_to):
            i = (y + oy_from) % 8
            send(ha.at[t, k, i], ha.at[t, k, i], (ALL, LOWER)[t], r_far.at[t, k], dev(p, x, (y + oy_to) % 8, c))

        pass_a(8 - 2 * turn, 8 + 2 * turn)
        pl.when(at != 3)(functools.partial(pass_a, 6, 1))
        pl.when(at != 0)(functools.partial(pass_a, 2, 7))
        arrived_kib(9 * B4, r_near2.at[t, k])
        for ox_from, ox_to, cores in ((6, 2, (0,)), (2, 6, (1,)), (7, 2, (0, 1)), (1, 6, (0, 1))):
            for c_ in cores:
                v, i = landing(k, (x + ox_from) % 8, c_)
                send(
                    hb.at[t, k, :, v, i], hb.at[t, k, :, v, i], (ALL, LOWER)[t], r_far.at[t, k], dev(p, (x + ox_to) % 8, y, c)
                )

    def dispatched(t, k):
        arrived_kib(3 * A8 + 6 * B4, r_far.at[t, k])
        hd[t, k] = hb[t, k].reshape(64, HB)

    others = [(ol, oc) for ol in (0, 1) for oc in (0, 1) if (ol, oc) != (0, 0)]

    def peer(ol, oc):
        return ((r // 2 + ol) % 2) * 2 + (c + oc) % 2

    first_a(0)
    first_b(0)
    arrived_kib(2 * UV128, ld.at[4])
    for ol, oc in others:
        send(uv.at[r], uv.at[r], ALL, r_one.at[1], (p, peer(ol, oc), s))
    u, v = (uv1[h].astype(F32).reshape(TOK, HID) for h in range(2))
    av1[r] = (u * jax.nn.sigmoid(u) * v).astype(BF)
    for ol, oc in others:
        send(av1.at[r], av1.at[r], ALL, r_one.at[4], (p, peer(ol, oc), s))
    @pl.when(lower & upper)
    def _():
        pl.semaphore_wait(ready, 1)

    @pl.when(lower)
    def _():
        send(sel_s.at[2], sel_in, SEL, r_one.at[0], dev(up, x, y, c))

    for k in range(K):
        second(0, k)

    arrived_kib(3 * Q // 4, ld.at[3])
    w2t[...] = w2[...].astype(F32).T.astype(BF)
    w13t[...] = w13[...].astype(F32).T.astype(BF)
    for k in range(K):
        forward(0, k)

    @pl.when(upper)
    def _():
        arrived(sel_in, r_one.at[0])
        base_v[...] = dot(sel_in[...], g_v[...], ((1,), (0,)))
        m_v[...] = dot(sel_in[...], sel_s[0], ((1,), (1,)))
        for e in range(2):
            for q in range(4):
                base_o[q, e] = base_v[2 * e : 2 * e + 2, q * Q : q * Q + HA]
        send(base_o, base_in, UPPER, r_one.at[2], dev(down, x, y, c))
        send(m_v, m_in, MM, r_one.at[3], dev(down, x, y, c))

    arrived(uv.at[0:3], r_one.at[1])
    for k in range(K):
        u, v = (
            jnp.concatenate(
                [uv[(k - yy) % 4, h, 4 * yy : 4 * yy + 4].astype(F32).reshape(8, HID) for yy in range(8)], axis=0
            )
            for h in range(2)
        )
        sig = jax.nn.sigmoid(u)
        act = u * sig
        coef[k, 0] = v * (sig * (1.0 + u * (1.0 - sig)))
        coef[k, 1] = act
        av = (act * v).astype(BF)
        avt[0, k] = av.astype(F32).T.astype(BF)

    def hidden_gradient(k):
        d_a = dot(ha[0, k].reshape(64, HA), w2t[0:HA], ((1,), (0,))) + dot(hd[0, k], w2t[HA:Q], ((1,), (0,)))
        dx[k, r] = d_a.astype(BF)
        for ol, oc in others:
            send(dx.at[k, r], dx.at[k, r], UPPER, r_dx.at[k], (p, peer(ol, oc), s))

    def near_a(k, oy):
        i = (y + oy) % 8
        send(pa.at[k, i], ra1.at[k, y], UPPER, r_back.at[k], dev(p, x, i, c))

    def near_b(k, x_, c_):
        v, i = landing(k, x_, c_)
        send(pb.at[k, :, v, i], rb1.at[k, r * 4 + xh], UPPER, r_back2.at[k], dev(p, x_, y, c_))

    def input_gradient(k):
        arrived(dx.at[k, 0:3], r_dx.at[k])
        d_act = (dx[k, 0].astype(F32) + dx[k, 1].astype(F32)) + (dx[k, 2].astype(F32) + dx[k, 3].astype(F32))
        d_gu = jnp.concatenate([(d_act * coef[k, 0]).astype(BF), (d_act * coef[k, 1]).astype(BF)], axis=1)
        pa[k] = dot(d_gu, w13t[:, 0:HA], ((1,), (0,))).astype(BF).reshape(8, 8, HA)

        def far_a(oy_row, oy_to, slot):
            i = (y + oy_row) % 8
            send(pa.at[k, i], fa.at[k, slot], UPPER, r_f.at[k], dev(p, x, (y + oy_to) % 8, c))

        far_a(4, 8 + 2 * turn, 2)
        pl.when(at != 0)(functools.partial(far_a, 5, 7, 0))
        pl.when(at == 0)(functools.partial(near_a, k, 5))
        pl.when(at != 3)(functools.partial(far_a, 3, 1, 1))
        pl.when(at == 3)(functools.partial(near_a, k, 3))
        ra1[k, y] = pa[k, y]
        pb[k] = dot(d_gu, w13t[:, HA:Q], ((1,), (0,))).astype(BF).reshape(2, 4, 4, 2, HB)

        for ox, ox_to, c_, slot in BACK:
            v, i = landing(k, (x + ox) % 8, c_)
            send(pb.at[k, :, v, i], fb.at[k, slot], UPPER, r_f2.at[k], dev(p, (x + ox_to) % 8, y, c))
        v, i = landing(k, x, c)
        rb1[k, r * 4 + xh] = pb[k, :, v, i]

    def forward_back(k):
        near_a(k, 1)
        near_a(k, 7)
        for ox, c_ in ((6, 1), (2, 0), (0, 1 - c)):
            near_b(k, (x + ox) % 8, c_)
        @pl.when(inner)
        def _():
            arrived_kib(3 * A8, r_f.at[k])

        @pl.when(jnp.logical_not(inner))
        def _():
            arrived_kib(2 * A8, r_f.at[k])

        tie = fa[k, 2].astype(F32)
        for slot, oy, tied in ((0, 6, at < 2), (1, 2, at >= 2)):
            i = (y + oy) % 8
            acc = pa[k, i].astype(F32) + fa[k, slot].astype(F32) + jnp.where(tied, tie, 0.0)
            sa[k, slot] = acc.astype(BF)
            send(sa.at[k, slot], ra1.at[k, y], UPPER, r_back.at[k], dev(p, x, i, c))
        arrived_kib(6 * B4, r_f2.at[k])
        for slot, ox, c_ in ((2, 6, 0), (5, 2, 1), (0, 7, 0), (1, 7, 1), (3, 1, 0), (4, 1, 1)):
            x_ = (x + ox) % 8
            v, i = landing(k, x_, c_)
            acc = pb[k, :, v, i].astype(F32) + fb[k, slot].astype(F32)
            sb[k, slot] = acc.astype(BF)
            send(sb.at[k, slot], rb1.at[k, r * 4 + xh], UPPER, r_back2.at[k], dev(p, x_, y, c_))

    def to_sources(k):
        @pl.when(inner)
        def _():
            arrived_kib(5 * A8, r_back.at[k])

        @pl.when(jnp.logical_not(inner))
        def _():
            arrived_kib(4 * A8, r_back.at[k])

        for e in range(2):
            acc = ra1[k, 4 * e].astype(F32)
            for h in range(1, 4):
                acc = acc + ra1[k, 4 * e + h].astype(F32)
            for h in range(4):
                ta[k, h, e] = acc[2 * h : 2 * h + 2].astype(BF)
        r_ = (k + 8 - y) % 4
        for h in range(4):
            send(ta.at[k, h], ra2.at[r * 4 + xh], UPPER, r_ra2, (down, r_, y * 4 + h))
        arrived_kib(9 * B4, r_back2.at[k])
        for q in range(4):
            acc = rb1[k, 4 * q].astype(F32)
            for h in range(1, 4):
                acc = acc + rb1[k, 4 * q + h].astype(F32)
            for h in range(2):
                tb[k, h, :, q * HB : (q + 1) * HB] = acc[h].astype(BF)
        v = (k + 4 - r) % 4
        for h in range(2):

            def go(h=h):
                send(tb.at[k, h], rb2.at[y], UPPER, r_rb2, dev(p, x, v + 4 * h, c))

            pl.when(v + 4 * h != y)(go)

            @pl.when(v + 4 * h == y)
            def _(h=h):
                rb2[y] = tb[k, h]

    def mixed(e, base, m, back):
        for f in range(2):
            for h in range(2):
                base = base + m[2 * e : 2 * e + 2, 2 * f + h : 2 * f + h + 1] * back[f][h : h + 1, :]
        return base.astype(BF)

    def next_rows():
        @pl.when(upper)
        def _():
            arrived(rb2.at[0:7], r_rb2)
            back = []
            for f in range(2):
                acc = rb2[4 * f].astype(F32)
                for h in range(1, 4):
                    acc = acc + rb2[4 * f + h].astype(F32)
                back.append(acc)
            for q in range(4):
                for e in range(2):
                    rows_b[1, e, :, q * HB : (q + 1) * HB] = mixed(
                        e,
                        base_v[2 * e : 2 * e + 2, q * Q + HA : (q + 1) * Q],
                        m_v[...],
                        [b[:, q * HB : (q + 1) * HB] for b in back],
                    )
            first_b(1)

        @pl.when(lower)
        def _():
            arrived(ra2, r_ra2)
            for q in range(4):
                back = []
                for f in range(2):
                    acc = ra2[4 * q, f].astype(F32)
                    for h in range(1, 4):
                        acc = acc + ra2[4 * q + h, f].astype(F32)
                    back.append(acc)
                for e in range(2):
                    rows_a[1, q, e] = mixed(e, base_in[q, e], m_in[...], back)
            first_a(1)

    def gather_rows(k):
        pl.when(mine == k)(next_rows)

    for k in range(K):
        dispatched(0, k)
        pl.when(upper)(functools.partial(hidden_gradient, k))
    for k in range(K):
        pl.when(upper)(functools.partial(input_gradient, k))
    left = jnp.concatenate([avt[0, k] for k in range(K)], axis=1)
    out[0, :, 0:HA] = dot(left, ha[0].reshape(K * 64, HA), ((1,), (0,)))
    out[0, :, HA:Q] = dot(left, hd[0].reshape(K * 64, HB), ((1,), (0,)))
    for k in range(K):
        pl.when(upper)(functools.partial(forward_back, k))
    arrived(av1.at[0:3], r_one.at[4])
    for k in range(K):
        av = jnp.concatenate([av1[(k - yy) % 4, 8 * yy : 8 * yy + 8] for yy in range(8)], axis=0)
        avt[1, k] = av.astype(F32).T.astype(BF)

    @pl.when(lower)
    def _():
        arrived(base_in, r_one.at[2])
        arrived(m_in, r_one.at[3])

    def if_lower(step, *args):
        pl.when(lower)(functools.partial(step, *args))

    def finish(k):
        dispatched(1, k)
        out[0, :, 0:HA] += dot(avt[1, k], ha[1, k].reshape(64, HA), ((1,), (0,)))
        out[0, :, HA:Q] += dot(avt[1, k], hd[1, k], ((1,), (0,)))

    pl.when(upper)(functools.partial(to_sources, 0))
    pl.when(upper)(functools.partial(to_sources, 1))
    pl.when(upper)(functools.partial(to_sources, 2))
    pl.when(upper)(functools.partial(to_sources, 3))
    gather_rows(0)
    gather_rows(1)
    gather_rows(2)
    gather_rows(3)
    if_lower(second, 1, 0)
    if_lower(second, 1, 1)
    if_lower(second, 1, 2)
    if_lower(second, 1, 3)
    if_lower(forward, 1, 0)
    if_lower(forward, 1, 1)
    if_lower(forward, 1, 2)
    if_lower(forward, 1, 3)
    for k in range(K):
        if_lower(finish, k)

    def second_size(forwards):
        return 16 * A8 + K * forwards * A8 + 60 * B4

    first_a_size, first_b_size = 15 * B4, 7 * ROWS2
    all_size = first_a_size + first_b_size + 3 * UV128 + 3 * DX64
    for chosen, forwards in ((inner, 4), (jnp.logical_not(inner), 2)):
        @pl.when(chosen)
        def _(forwards=forwards):
            arrived_kib(all_size + second_size(forwards), snd.at[ALL])

        @pl.when(chosen & lower)
        def _(forwards=forwards):
            arrived_kib(first_a_size + second_size(forwards), snd.at[LOWER])

    @pl.when(lower)
    def _():
        arrived(sel_in, snd.at[SEL])

    @pl.when(upper)
    def _():
        arrived_kib(8 * ROWS2 + 12 * DX64 + 28 * A8 + 60 * B4 + 16 * B4 + 7 * ROWS2 + 56, snd.at[UPPER])
        arrived(m_in, snd.at[MM])


def body(cotangent, routes, gates, *others):
    hbm = pl.BlockSpec(memory_space=pl.ANY)
    dma = pltpu.SemaphoreType.DMA
    vmem = pltpu.VMEM
    return pl.pallas_call(
        kernel,
        out_shape=vmem((1, HID, Q), F32),
        in_specs=[hbm] * 8,
        out_specs=pl.BlockSpec(memory_space=vmem),
        scratch_shapes=[
            vmem((TOK, D), BF),
            vmem((2, 8, TOK), jnp.int32),
            vmem((2, 8, TOK), BF),
            vmem((HID, Q), BF),
            vmem((Q, 2 * HID), BF),
            vmem((Q, HID), BF),
            vmem((2 * HID, Q), BF),
            vmem((3, 8, TOK), BF),
            vmem((8, TOK), BF),
            vmem((2, 4, 2, 2, HA), BF),
            vmem((2, 2, 2, 4 * HB), BF),
            vmem((8, D), F32),
            vmem((4, 2, 2, HA), F32),
            vmem((4, 2, 2, HA), F32),
            vmem((8, 8), F32),
            vmem((8, 8), F32),
            vmem((4, 2, 32, 2, HID), BF),
            vmem((2, 32, 2, HID), BF),
            vmem((4, TOK, HID), BF),
            vmem((K, 2, 64, HID), F32),
            vmem((2, K, HID, 64), BF),
            vmem((1536, 4, 128), BF),
            vmem((2, K, 4, 2, 2, HA), BF),
            vmem((2, K, 2, 8, HA), BF),
            vmem((2, 4, 2, 2, 4 * HB), BF),
            vmem((2, K, 8, 8, HA), BF),
            vmem((2, K, 2, 4, 4, 2, HB), BF),
            vmem((2, K, 64, HB), BF),
            vmem((K, 4, 64, HID), BF),
            vmem((K, 8, 8, HA), BF),
            vmem((K, 2, 4, 4, 2, HB), BF),
            vmem((K, 3, 8, HA), BF),
            vmem((K, 6, 2, 2, HB), BF),
            vmem((K, 2, 8, HA), BF),
            vmem((K, 6, 2, 2, HB), BF),
            vmem((K, 8, 8, HA), BF),
            vmem((K, 16, 2, 2, HB), BF),
            vmem((K, 4, 2, 2, HA), BF),
            vmem((K, 2, 2, 4 * HB), BF),
            vmem((16, 2, 2, HA), BF),
            vmem((8, 2, 4 * HB), BF),
            dma((5,)),
            dma((5,)),
            dma((2, K)),
            dma((2, K)),
            dma((2, K)),
            dma((K,)),
            dma((K,)),
            dma((K,)),
            dma,
            dma,
            dma((5,)),
            pltpu.SemaphoreType.REGULAR,
            dma((2, K)),
            dma((2, K)),
            dma((K,)),
            dma((K,)),
        ],
        compiler_params=pltpu.CompilerParams(collective_id=0, has_side_effects=True),
        name="cooldown",
    )(cotangent, jnp.swapaxes(routes, 2, 3), jnp.swapaxes(gates, 2, 3), *others)


def solution(mesh):
    in_specs = (
        P("pipe", ("dp", "expert"), None),
        P("pipe", None, ("dp", "expert"), None),
        P("pipe", None, ("dp", "expert"), None),
        P("pipe", None, "dp", None, None, "expert"),
        P("pipe", None, "dp", None, None, "expert"),
        P("pipe", None, "expert"),
        P("pipe", None, "expert"),
        P("pipe", "expert", None),
    )
    out_specs = P("pipe", "expert", "dp")
    return jax.shard_map(body, mesh=mesh, in_specs=in_specs, out_specs=out_specs, check_vma=False)
```

```python
import functools

import jax
import jax.numpy as jnp
from jax import lax
from jax.experimental import pallas as pl
from jax.experimental.pallas import tpu as pltpu
from jax.sharding import PartitionSpec as P

MESH = pl.DeviceIdType.MESH
BF = jnp.bfloat16
F32 = jnp.float32

D = 7168
TOK = 64
HID = 128
Q = 1792
HA = HB = 896
K = 4
FAR = (4, 3, 5, 2, 6, 1, 7)
ROW = tuple((dx, dc) for dx in FAR for dc in (0, 1)) + ((0, 1),)
NEAR = tuple((dx, dc) for dx in (2, 6, 1, 7) for dc in (0, 1)) + ((0, 1),)
BACK = ((4, 6, 0, 2), (4, 2, 1, 5), (5, 6, 0, 0), (5, 6, 1, 1), (3, 2, 0, 3), (3, 2, 1, 4))
A8, B4, ROWS2, DX64, UV128 = 14, 7, 14, 16, 32


def dot(a, b, dims):
    return lax.dot_general(a, b, (dims, ((), ())), preferred_element_type=F32)


def kernel(
    cot, routes, gates, gate_pre, up_pre, w_gate, w_up, w_down, out,
    g_v, ids_v, gat_v, w2, w13, w2t, w13t, sel_s, sel_in, rows_a, rows_b, base_v, base_o, base_in, m_v, m_in, uv, uv1, av1, coef, avt,
    void, xa, a2, yb, ha, hb, hd, dx, pa, pb, fa, fb, sa, sb, ra1, rb1, ta, tb, ra2, rb2,
    ld, snd, r_x, r_near, r_far, r_dx, r_f, r_back, r_ra2, r_rb2, r_one, ready, r_x2, r_near2, r_f2, r_back2,
):
    p = lax.axis_index("pipe")
    r = lax.axis_index("dp")
    s = lax.axis_index("expert")
    y = s // 4
    xh = s % 4
    x = xh * 2 + r // 2
    c = r % 2
    lower = p < 7
    upper = p > 0
    up = jnp.minimum(p + 1, 7)
    down = jnp.maximum(p - 1, 0)
    mine = (r + y) % 4
    half = y // 4
    at = y % 4
    inner = (at == 1) | (at == 2)
    turn = jnp.where(at < 2, 1, -1)

    def dev(p_, x_, y_, c_):
        return (p_, (x_ % 2) * 2 + c_, y_ * 4 + x_ // 2)

    def send(src, dst, kind, recv, target):
        pltpu.make_async_remote_copy(
            src_ref=src, dst_ref=dst, send_sem=snd.at[kind], recv_sem=recv, device_id=target, device_id_type=MESH
        ).start()

    def arrived(like, sem):
        pltpu.make_async_copy(like, like, sem).wait()

    def arrived_kib(size, sem):
        arrived(void.at[0:size], sem)

    ALL, LOWER, UPPER, SEL, MM = range(5)

    barrier = pltpu.get_barrier_semaphore()
    peers = [((x + ox) % 8, y, (c + oc) % 2, p) for ox, oc in ROW]
    peers += [(x, (y + oy) % 8, c, p) for oy in FAR]
    for x_, y_, c_, p_ in peers:
        pl.semaphore_signal(barrier, inc=1, device_id=dev(p_, x_, y_, c_), device_id_type=MESH)

    @pl.when(lower & upper)
    def _():
        pl.semaphore_signal(barrier, inc=1, device_id=dev(up, x, y, c), device_id_type=MESH)

    @pl.when(p == 1)
    def _():
        pl.semaphore_signal(barrier, inc=1, device_id=dev(down, x, y, c), device_id_type=MESH)

    q0 = pl.multiple_of(r * Q, 128)
    loads = [
        pltpu.make_async_copy(routes.at[0], ids_v, ld.at[0]),
        pltpu.make_async_copy(gates.at[0], gat_v, ld.at[1]),
        pltpu.make_async_copy(cot.at[0], g_v, ld.at[2]),
        pltpu.make_async_copy(w_down.at[0, :, pl.ds(q0, Q)], w2, ld.at[3]),
        pltpu.make_async_copy(w_gate.at[0, pl.ds(q0, Q)], w13.at[:, 0:HID], ld.at[3]),
        pltpu.make_async_copy(w_up.at[0, pl.ds(q0, Q)], w13.at[:, HID : 2 * HID], ld.at[3]),
        pltpu.make_async_copy(gate_pre.at[0, 0, 0], uv.at[r, 0], ld.at[4]),
        pltpu.make_async_copy(up_pre.at[0, 0, 0], uv.at[r, 1], ld.at[4]),
        pltpu.make_async_copy(gate_pre.at[0, 1, 0], uv1.at[0], ld.at[4]),
        pltpu.make_async_copy(up_pre.at[0, 1, 0], uv1.at[1], ld.at[4]),
    ]
    for cp in loads:
        cp.start()

    loads[0].wait()
    loads[1].wait()
    row = lax.broadcasted_iota(jnp.int32, (8, TOK), 0)
    upto = (
        lax.broadcasted_iota(jnp.int32, (TOK, TOK), 0) <= lax.broadcasted_iota(jnp.int32, (TOK, TOK), 1)
    ).astype(F32).astype(BF)
    for t in range(2):
        ids = ids_v[t]
        gat = gat_v[t].astype(F32)
        hit = jnp.zeros((8, TOK), F32)
        gsum = jnp.zeros((8, TOK), F32)
        for e in range(2):
            match = (ids == e).astype(F32)
            of_e = (row >= 2 * e) & (row < 2 * e + 2)
            hit = jnp.where(of_e, jnp.sum(match, axis=0, keepdims=True), hit)
            gsum = jnp.where(of_e, jnp.sum(match * gat, axis=0, keepdims=True), gsum)
        rank = dot(hit.astype(BF), upto, ((1,), (0,))) - 1.0
        sel = hit * (rank == (row & 1).astype(F32)).astype(F32)
        if t == 0:
            sel_s[0] = sel.astype(BF)
        sel_s[1 + t] = (sel * gsum).astype(BF)

    loads[2].wait()
    rows = dot(sel_s[1], g_v[...], ((1,), (0,)))
    for e in range(2):
        for q in range(4):
            rows_a[0, q, e] = rows[2 * e : 2 * e + 2, q * Q : q * Q + HA].astype(BF)
            rows_b[0, e, :, q * HB : (q + 1) * HB] = rows[2 * e : 2 * e + 2, q * Q + HA : (q + 1) * Q].astype(BF)

    for k in range(K):
        ra1[k, (y + 4) % 8] = jnp.zeros((8, HA), BF)
        for where, oy in ((1, 3), (2, 5)):
            @pl.when(at != where)
            def _(k=k, oy=oy):
                ra1[k, (y + oy) % 8] = jnp.zeros((8, HA), BF)

        for where, slot in ((3, 0), (0, 1)):
            @pl.when(at == where)
            def _(k=k, slot=slot):
                fa[k, slot] = jnp.zeros((8, HA), BF)

        for ox in (3, 4, 5):
            for c_ in range(2):
                x_ = (x + ox) % 8
                rb1[k, ((x_ % 2) * 2 + c_) * 4 + x_ // 2] = jnp.zeros((2, 2, HB), BF)

    @pl.when(p != 1)
    def _():
        pl.semaphore_wait(barrier, len(peers) + 1)

    @pl.when(p == 1)
    def _():
        pl.semaphore_wait(barrier, len(peers))

    @pl.when(p > 1)
    def _():
        pl.semaphore_signal(ready, inc=1, device_id=dev(down, x, y, c), device_id_type=MESH)

    def first_a(t):
        for ox, oc in ROW:
            x_, c_ = (x + ox) % 8, (c + oc) % 2
            q_ = (x_ % 2) * 2 + c_
            send(rows_a.at[t, q_], xa.at[t, mine, xh], (ALL, LOWER)[t], r_x.at[t, mine], dev(p, x_, y, c_))
        xa[t, mine, xh] = rows_a[t, r]

    def first_b(t):
        for oy in FAR + (0,) * t:
            y_ = (y + oy) % 8
            send(
                rows_b.at[t, y_ // 4], yb.at[t, y % 4, half], (ALL, UPPER)[t], r_x2.at[t, mine], dev((p, down)[t], x, y_, c)
            )
        if t == 0:
            yb[t, y % 4, half] = rows_b[t, half]

    def send_b(t, k, x_, c_):
        v = (k + 4 - r) % 4
        columns = pl.ds(pl.multiple_of(((x_ % 2) * 2 + c_) * HB, 128), HB)
        send(yb.at[t, v, :, :, columns], hb.at[t, k, :, v, xh], (ALL, LOWER)[t], r_near2.at[t, k], dev(p, x_, y, c_))

    def direct_a(t, k, oy):
        y_ = (y + oy) % 8
        send(a2.at[t, k, y_ // 4], ha.at[t, k, y], (ALL, LOWER)[t], r_far.at[t, k], dev(p, x, y_, c))

    def second(t, k):
        @pl.when(mine == k)
        def _():
            arrived_kib(3 * B4, r_x.at[t, k])

        @pl.when(mine != k)
        def _():
            arrived_kib(4 * B4, r_x.at[t, k])

        for e in range(2):
            a2[t, k, e] = jnp.concatenate([xa[t, k, h, e] for h in range(4)], axis=0)
        for oy in (2, 6, 1, 7):
            y_ = (y + oy) % 8
            send(a2.at[t, k, y_ // 4], ha.at[t, k, y], (ALL, LOWER)[t], r_near.at[t, k], dev(p, x, y_, c))
        ha[t, k, y] = a2[t, k, half]
        if t == 0:
            @pl.when(mine == k)
            def _():
                arrived_kib(ROWS2, r_x2.at[t, k])

            @pl.when(mine != k)
            def _():
                arrived_kib(2 * ROWS2, r_x2.at[t, k])
        else:
            arrived_kib(2 * ROWS2, r_x2.at[t, k])
        v = (k + 4 - r) % 4
        for ox, oc in NEAR:
            send_b(t, k, (x + ox) % 8, (c + oc) % 2)
        hb[t, k, :, v, xh] = yb[t, v, :, :, pl.ds(pl.multiple_of(r * HB, 128), HB)]

    def landing(k, x_, c_):
        return (k + 4 - ((x_ % 2) * 2 + c_)) % 4, x_ // 2

    def forward(t, k):
        pl.when(at == 1)(functools.partial(direct_a, t, k, 3))
        pl.when(at == 2)(functools.partial(direct_a, t, k, 5))
        arrived_kib(4 * A8, r_near.at[t, k])

        def pass_a(oy_from, oy_to):
            i = (y + oy_from) % 8
            send(ha.at[t, k, i], ha.at[t, k, i], (ALL, LOWER)[t], r_far.at[t, k], dev(p, x, (y + oy_to) % 8, c))

        pass_a(8 - 2 * turn, 8 + 2 * turn)
        pl.when(at != 3)(functools.partial(pass_a, 6, 1))
        pl.when(at != 0)(functools.partial(pass_a, 2, 7))
        arrived_kib(9 * B4, r_near2.at[t, k])
        for ox_from, ox_to, cores in ((6, 2, (0,)), (2, 6, (1,)), (7, 2, (0, 1)), (1, 6, (0, 1))):
            for c_ in cores:
                v, i = landing(k, (x + ox_from) % 8, c_)
                send(
                    hb.at[t, k, :, v, i], hb.at[t, k, :, v, i], (ALL, LOWER)[t], r_far.at[t, k], dev(p, (x + ox_to) % 8, y, c)
                )

    def dispatched(t, k):
        arrived_kib(3 * A8 + 6 * B4, r_far.at[t, k])
        hd[t, k] = hb[t, k].reshape(64, HB)

    others = ((1, 0), (1, 1), (0, 1))

    def peer(ol, oc):
        return ((r // 2 + ol) % 2) * 2 + (c + oc) % 2

    first_a(0)
    first_b(0)
    arrived_kib(2 * UV128, ld.at[4])
    for ol, oc in others:
        send(uv.at[r], uv.at[r], ALL, r_one.at[1], (p, peer(ol, oc), s))
    u, v = (uv1[h].astype(F32).reshape(TOK, HID) for h in range(2))
    av1[r] = (u * jax.nn.sigmoid(u) * v).astype(BF)
    for ol, oc in others:
        send(av1.at[r], av1.at[r], ALL, r_one.at[4], (p, peer(ol, oc), s))
    @pl.when(lower & upper)
    def _():
        pl.semaphore_wait(ready, 1)

    @pl.when(lower)
    def _():
        send(sel_s.at[2], sel_in, SEL, r_one.at[0], dev(up, x, y, c))

    for k in range(K):
        second(0, k)

    arrived_kib(3 * Q // 4, ld.at[3])
    w2t[...] = w2[...].astype(F32).T.astype(BF)
    w13t[...] = w13[...].astype(F32).T.astype(BF)
    for k in range(K):
        forward(0, k)

    @pl.when(upper)
    def _():
        arrived(sel_in, r_one.at[0])
        base_v[...] = dot(sel_in[...], g_v[...], ((1,), (0,)))
        m_v[...] = dot(sel_in[...], sel_s[0], ((1,), (1,)))
        for e in range(2):
            for q in range(4):
                base_o[q, e] = base_v[2 * e : 2 * e + 2, q * Q : q * Q + HA]
        send(base_o, base_in, UPPER, r_one.at[2], dev(down, x, y, c))
        send(m_v, m_in, MM, r_one.at[3], dev(down, x, y, c))

    arrived(uv.at[0:3], r_one.at[1])
    for k in range(K):
        u, v = (
            jnp.concatenate(
                [uv[(k - yy) % 4, h, 4 * yy : 4 * yy + 4].astype(F32).reshape(8, HID) for yy in range(8)], axis=0
            )
            for h in range(2)
        )
        sig = jax.nn.sigmoid(u)
        act = u * sig
        coef[k, 0] = v * (sig * (1.0 + u * (1.0 - sig)))
        coef[k, 1] = act
        av = (act * v).astype(BF)
        avt[0, k] = av.astype(F32).T.astype(BF)

    def hidden_gradient(k):
        d_a = dot(ha[0, k].reshape(64, HA), w2t[0:HA], ((1,), (0,))) + dot(hd[0, k], w2t[HA:Q], ((1,), (0,)))
        dx[k, r] = d_a.astype(BF)
        for ol, oc in others:
            send(dx.at[k, r], dx.at[k, r], UPPER, r_dx.at[k], (p, peer(ol, oc), s))

    def near_a(k, oy):
        i = (y + oy) % 8
        send(pa.at[k, i], ra1.at[k, y], UPPER, r_back.at[k], dev(p, x, i, c))

    def near_b(k, x_, c_):
        v, i = landing(k, x_, c_)
        send(pb.at[k, :, v, i], rb1.at[k, r * 4 + xh], UPPER, r_back2.at[k], dev(p, x_, y, c_))

    def input_gradient(k):
        arrived(dx.at[k, 0:3], r_dx.at[k])
        d_act = (dx[k, 0].astype(F32) + dx[k, 1].astype(F32)) + (dx[k, 2].astype(F32) + dx[k, 3].astype(F32))
        d_gu = jnp.concatenate([(d_act * coef[k, 0]).astype(BF), (d_act * coef[k, 1]).astype(BF)], axis=1)
        pa[k] = dot(d_gu, w13t[:, 0:HA], ((1,), (0,))).astype(BF).reshape(8, 8, HA)

        def far_a(oy_row, oy_to, slot):
            i = (y + oy_row) % 8
            send(pa.at[k, i], fa.at[k, slot], UPPER, r_f.at[k], dev(p, x, (y + oy_to) % 8, c))

        far_a(4, 8 + 2 * turn, 2)
        pl.when(at != 0)(functools.partial(far_a, 5, 7, 0))
        pl.when(at == 0)(functools.partial(near_a, k, 5))
        pl.when(at != 3)(functools.partial(far_a, 3, 1, 1))
        pl.when(at == 3)(functools.partial(near_a, k, 3))
        ra1[k, y] = pa[k, y]
        pb[k] = dot(d_gu, w13t[:, HA:Q], ((1,), (0,))).astype(BF).reshape(2, 4, 4, 2, HB)

        for ox, ox_to, c_, slot in BACK:
            v, i = landing(k, (x + ox) % 8, c_)
            send(pb.at[k, :, v, i], fb.at[k, slot], UPPER, r_f2.at[k], dev(p, (x + ox_to) % 8, y, c))
        v, i = landing(k, x, c)
        rb1[k, r * 4 + xh] = pb[k, :, v, i]

    def forward_back(k):
        near_a(k, 1)
        near_a(k, 7)
        for ox, c_ in ((6, 1), (2, 0), (0, 1 - c)):
            near_b(k, (x + ox) % 8, c_)
        @pl.when(inner)
        def _():
            arrived_kib(3 * A8, r_f.at[k])

        @pl.when(jnp.logical_not(inner))
        def _():
            arrived_kib(2 * A8, r_f.at[k])

        tie = fa[k, 2].astype(F32)
        for slot, oy, tied in ((0, 6, at < 2), (1, 2, at >= 2)):
            i = (y + oy) % 8
            acc = pa[k, i].astype(F32) + fa[k, slot].astype(F32) + jnp.where(tied, tie, 0.0)
            sa[k, slot] = acc.astype(BF)
            send(sa.at[k, slot], ra1.at[k, y], UPPER, r_back.at[k], dev(p, x, i, c))
        arrived_kib(6 * B4, r_f2.at[k])
        for slot, ox, c_ in ((2, 6, 0), (5, 2, 1), (0, 7, 0), (1, 7, 1), (3, 1, 0), (4, 1, 1)):
            x_ = (x + ox) % 8
            v, i = landing(k, x_, c_)
            acc = pb[k, :, v, i].astype(F32) + fb[k, slot].astype(F32)
            sb[k, slot] = acc.astype(BF)
            send(sb.at[k, slot], rb1.at[k, r * 4 + xh], UPPER, r_back2.at[k], dev(p, x_, y, c_))

    def to_sources(k):
        @pl.when(inner)
        def _():
            arrived_kib(5 * A8, r_back.at[k])

        @pl.when(jnp.logical_not(inner))
        def _():
            arrived_kib(4 * A8, r_back.at[k])

        for e in range(2):
            acc = ra1[k, 4 * e].astype(F32)
            for h in range(1, 4):
                acc = acc + ra1[k, 4 * e + h].astype(F32)
            for h in range(4):
                ta[k, h, e] = acc[2 * h : 2 * h + 2].astype(BF)
        r_ = (k + 8 - y) % 4
        side = 1 + 2 * (x % 2)
        for o in (2, side, 4 - side, 0):
            h_ = (xh + o) % 4
            send(ta.at[k, h_], ra2.at[r * 4 + xh], UPPER, r_ra2, (down, r_, y * 4 + h_))
        arrived_kib(9 * B4, r_back2.at[k])
        for q in range(4):
            acc = rb1[k, 4 * q].astype(F32)
            for h in range(1, 4):
                acc = acc + rb1[k, 4 * q + h].astype(F32)
            for h in range(2):
                tb[k, h, :, q * HB : (q + 1) * HB] = acc[h].astype(BF)
        v = (k + 4 - r) % 4
        d = (v + 8 - y) % 4
        far = (y + jnp.where(d < 2, d + 4, d)) % 8 // 4
        for h in (far, 1 - far):
            y_ = v + 4 * h

            def go(h=h, y_=y_):
                send(tb.at[k, h], rb2.at[y], UPPER, r_rb2, dev(p, x, y_, c))

            pl.when(y_ != y)(go)

            @pl.when(y_ == y)
            def _(h=h):
                rb2[y] = tb[k, h]

    def mixed(e, base, m, back):
        for f in range(2):
            for h in range(2):
                base = base + m[2 * e : 2 * e + 2, 2 * f + h : 2 * f + h + 1] * back[f][h : h + 1, :]
        return base.astype(BF)

    def next_rows():
        @pl.when(upper)
        def _():
            arrived(rb2.at[0:7], r_rb2)
            back = []
            for f in range(2):
                acc = rb2[4 * f].astype(F32)
                for h in range(1, 4):
                    acc = acc + rb2[4 * f + h].astype(F32)
                back.append(acc)
            for q in range(4):
                for e in range(2):
                    rows_b[1, e, :, q * HB : (q + 1) * HB] = mixed(
                        e,
                        base_v[2 * e : 2 * e + 2, q * Q + HA : (q + 1) * Q],
                        m_v[...],
                        [b[:, q * HB : (q + 1) * HB] for b in back],
                    )
            first_b(1)

        @pl.when(lower)
        def _():
            arrived(ra2, r_ra2)
            for q in range(4):
                back = []
                for f in range(2):
                    acc = ra2[4 * q, f].astype(F32)
                    for h in range(1, 4):
                        acc = acc + ra2[4 * q + h, f].astype(F32)
                    back.append(acc)
                for e in range(2):
                    rows_a[1, q, e] = mixed(e, base_in[q, e], m_in[...], back)
            first_a(1)

    def gather_rows(k):
        pl.when(mine == k)(next_rows)

    for k in range(K):
        dispatched(0, k)
        pl.when(upper)(functools.partial(hidden_gradient, k))
    for k in range(K):
        pl.when(upper)(functools.partial(input_gradient, k))
    left = jnp.concatenate([avt[0, k] for k in range(K)], axis=1)
    out[0, :, 0:HA] = dot(left, ha[0].reshape(K * 64, HA), ((1,), (0,)))
    out[0, :, HA:Q] = dot(left, hd[0].reshape(K * 64, HB), ((1,), (0,)))
    for k in range(K):
        pl.when(upper)(functools.partial(forward_back, k))
    arrived(av1.at[0:3], r_one.at[4])
    for k in range(K):
        av = jnp.concatenate([av1[(k - yy) % 4, 8 * yy : 8 * yy + 8] for yy in range(8)], axis=0)
        avt[1, k] = av.astype(F32).T.astype(BF)

    @pl.when(lower)
    def _():
        arrived(base_in, r_one.at[2])
        arrived(m_in, r_one.at[3])

    def if_lower(step, *args):
        pl.when(lower)(functools.partial(step, *args))

    def finish(k):
        dispatched(1, k)
        out[0, :, 0:HA] += dot(avt[1, k], ha[1, k].reshape(64, HA), ((1,), (0,)))
        out[0, :, HA:Q] += dot(avt[1, k], hd[1, k], ((1,), (0,)))

    pl.when(upper)(functools.partial(to_sources, 0))
    pl.when(upper)(functools.partial(to_sources, 1))
    pl.when(upper)(functools.partial(to_sources, 2))
    pl.when(upper)(functools.partial(to_sources, 3))
    gather_rows(0)
    gather_rows(1)
    gather_rows(2)
    gather_rows(3)
    if_lower(second, 1, 0)
    if_lower(second, 1, 1)
    if_lower(second, 1, 2)
    if_lower(second, 1, 3)
    if_lower(forward, 1, 0)
    if_lower(forward, 1, 1)
    if_lower(forward, 1, 2)
    if_lower(forward, 1, 3)
    for k in range(K):
        if_lower(finish, k)

    def second_size(forwards):
        return 16 * A8 + K * forwards * A8 + 60 * B4

    first_a_size, first_b_size = 15 * B4, 7 * ROWS2
    all_size = first_a_size + first_b_size + 3 * UV128 + 3 * DX64
    for chosen, forwards in ((inner, 4), (jnp.logical_not(inner), 2)):
        @pl.when(chosen)
        def _(forwards=forwards):
            arrived_kib(all_size + second_size(forwards), snd.at[ALL])

        @pl.when(chosen & lower)
        def _(forwards=forwards):
            arrived_kib(first_a_size + second_size(forwards), snd.at[LOWER])

    @pl.when(lower)
    def _():
        arrived(sel_in, snd.at[SEL])

    @pl.when(upper)
    def _():
        arrived_kib(8 * ROWS2 + 12 * DX64 + 28 * A8 + 60 * B4 + 16 * B4 + 7 * ROWS2 + 56, snd.at[UPPER])
        arrived(m_in, snd.at[MM])


def body(cotangent, routes, gates, *others):
    hbm = pl.BlockSpec(memory_space=pl.ANY)
    dma = pltpu.SemaphoreType.DMA
    vmem = pltpu.VMEM
    return pl.pallas_call(
        kernel,
        out_shape=vmem((1, HID, Q), F32),
        in_specs=[hbm] * 8,
        out_specs=pl.BlockSpec(memory_space=vmem),
        scratch_shapes=[
            vmem((TOK, D), BF),
            vmem((2, 8, TOK), jnp.int32),
            vmem((2, 8, TOK), BF),
            vmem((HID, Q), BF),
            vmem((Q, 2 * HID), BF),
            vmem((Q, HID), BF),
            vmem((2 * HID, Q), BF),
            vmem((3, 8, TOK), BF),
            vmem((8, TOK), BF),
            vmem((2, 4, 2, 2, HA), BF),
            vmem((2, 2, 2, 4 * HB), BF),
            vmem((8, D), F32),
            vmem((4, 2, 2, HA), F32),
            vmem((4, 2, 2, HA), F32),
            vmem((8, 8), F32),
            vmem((8, 8), F32),
            vmem((4, 2, 32, 2, HID), BF),
            vmem((2, 32, 2, HID), BF),
            vmem((4, TOK, HID), BF),
            vmem((K, 2, 64, HID), F32),
            vmem((2, K, HID, 64), BF),
            vmem((1536, 4, 128), BF),
            vmem((2, K, 4, 2, 2, HA), BF),
            vmem((2, K, 2, 8, HA), BF),
            vmem((2, 4, 2, 2, 4 * HB), BF),
            vmem((2, K, 8, 8, HA), BF),
            vmem((2, K, 2, 4, 4, 2, HB), BF),
            vmem((2, K, 64, HB), BF),
            vmem((K, 4, 64, HID), BF),
            vmem((K, 8, 8, HA), BF),
            vmem((K, 2, 4, 4, 2, HB), BF),
            vmem((K, 3, 8, HA), BF),
            vmem((K, 6, 2, 2, HB), BF),
            vmem((K, 2, 8, HA), BF),
            vmem((K, 6, 2, 2, HB), BF),
            vmem((K, 8, 8, HA), BF),
            vmem((K, 16, 2, 2, HB), BF),
            vmem((K, 4, 2, 2, HA), BF),
            vmem((K, 2, 2, 4 * HB), BF),
            vmem((16, 2, 2, HA), BF),
            vmem((8, 2, 4 * HB), BF),
            dma((5,)),
            dma((5,)),
            dma((2, K)),
            dma((2, K)),
            dma((2, K)),
            dma((K,)),
            dma((K,)),
            dma((K,)),
            dma,
            dma,
            dma((5,)),
            pltpu.SemaphoreType.REGULAR,
            dma((2, K)),
            dma((2, K)),
            dma((K,)),
            dma((K,)),
        ],
        compiler_params=pltpu.CompilerParams(collective_id=0, has_side_effects=True),
        name="cooldown",
    )(cotangent, jnp.swapaxes(routes, 2, 3), jnp.swapaxes(gates, 2, 3), *others)


def solution(mesh):
    in_specs = (
        P("pipe", ("dp", "expert"), None),
        P("pipe", None, ("dp", "expert"), None),
        P("pipe", None, ("dp", "expert"), None),
        P("pipe", None, "dp", None, None, "expert"),
        P("pipe", None, "dp", None, None, "expert"),
        P("pipe", None, "expert"),
        P("pipe", None, "expert"),
        P("pipe", "expert", None),
    )
    out_specs = P("pipe", "expert", "dp")
    return jax.shard_map(body, mesh=mesh, in_specs=in_specs, out_specs=out_specs, check_vma=False)
```

```python
import functools

import jax
import jax.numpy as jnp
from jax import lax
from jax.experimental import pallas as pl
from jax.experimental.pallas import tpu as pltpu
from jax.sharding import PartitionSpec as P

MESH = pl.DeviceIdType.MESH
BF = jnp.bfloat16
F32 = jnp.float32

D = 7168
TOK = 64
HID = 128
Q = 1792
HA = HB = 896
K = 4
FAR = (4, 3, 5, 2, 6, 1, 7)
ROW = tuple((dx, dc) for dx in FAR for dc in (0, 1)) + ((0, 1),)
NEAR = tuple((dx, dc) for dx in (2, 6, 1, 7) for dc in (0, 1)) + ((0, 1),)
BACK = ((4, 6, 0, 2), (4, 2, 1, 5), (5, 6, 0, 0), (5, 6, 1, 1), (3, 2, 0, 3), (3, 2, 1, 4))
A8, B4, ROWS2, DX64, UV128 = 14, 7, 14, 16, 32


def dot(a, b, dims):
    return lax.dot_general(a, b, (dims, ((), ())), preferred_element_type=F32)


def kernel(
    cot, routes, gates, gate_pre, up_pre, w_gate, w_up, w_down, out,
    g_v, ids_v, gat_v, w2, w13, w2t, w13t, sel_s, sel_in, rows_a, rows_b, base_v, base_o, base_in, m_v, m_in, uv, uv1, av1, coef, avt,
    void, xa, a2, yb, ha, hb, hd, dx, pa, pb, fa, fb, sa, sb, ra1, rb1, ta, tb, ra2, rb2,
    ld, snd, r_x, r_near, r_far, r_dx, r_f, r_back, r_ra2, r_rb2, r_one, ready, r_x2, r_near2, r_f2, r_back2,
):
    p = lax.axis_index("pipe")
    r = lax.axis_index("dp")
    s = lax.axis_index("expert")
    y = s // 4
    xh = s % 4
    x = xh * 2 + r // 2
    c = r % 2
    lower = p < 7
    upper = p > 0
    up = jnp.minimum(p + 1, 7)
    down = jnp.maximum(p - 1, 0)
    mine = (r + y) % 4
    half = y // 4
    at = y % 4
    inner = (at == 1) | (at == 2)
    turn = jnp.where(at < 2, 1, -1)

    def dev(p_, x_, y_, c_):
        return (p_, (x_ % 2) * 2 + c_, y_ * 4 + x_ // 2)

    def send(src, dst, kind, recv, target):
        pltpu.make_async_remote_copy(
            src_ref=src, dst_ref=dst, send_sem=snd.at[kind], recv_sem=recv, device_id=target, device_id_type=MESH
        ).start()

    def arrived(like, sem):
        pltpu.make_async_copy(like, like, sem).wait()

    def arrived_kib(size, sem):
        arrived(void.at[0:size], sem)

    ALL, LOWER, UPPER, SEL, MM = range(5)

    barrier = pltpu.get_barrier_semaphore()
    peers = [((x + ox) % 8, y, (c + oc) % 2, p) for ox, oc in ROW]
    peers += [(x, (y + oy) % 8, c, p) for oy in FAR]
    for x_, y_, c_, p_ in peers:
        pl.semaphore_signal(barrier, inc=1, device_id=dev(p_, x_, y_, c_), device_id_type=MESH)

    @pl.when(lower & upper)
    def _():
        pl.semaphore_signal(barrier, inc=1, device_id=dev(up, x, y, c), device_id_type=MESH)

    @pl.when(p == 1)
    def _():
        pl.semaphore_signal(barrier, inc=1, device_id=dev(down, x, y, c), device_id_type=MESH)

    q0 = pl.multiple_of(r * Q, 128)
    loads = [
        pltpu.make_async_copy(routes.at[0], ids_v, ld.at[0]),
        pltpu.make_async_copy(gates.at[0], gat_v, ld.at[1]),
        pltpu.make_async_copy(cot.at[0], g_v, ld.at[2]),
        pltpu.make_async_copy(w_down.at[0, :, pl.ds(q0, Q)], w2, ld.at[3]),
        pltpu.make_async_copy(w_gate.at[0, pl.ds(q0, Q)], w13.at[:, 0:HID], ld.at[3]),
        pltpu.make_async_copy(w_up.at[0, pl.ds(q0, Q)], w13.at[:, HID : 2 * HID], ld.at[3]),
        pltpu.make_async_copy(gate_pre.at[0, 0, 0], uv.at[r, 0], ld.at[4]),
        pltpu.make_async_copy(up_pre.at[0, 0, 0], uv.at[r, 1], ld.at[4]),
        pltpu.make_async_copy(gate_pre.at[0, 1, 0], uv1.at[0], ld.at[4]),
        pltpu.make_async_copy(up_pre.at[0, 1, 0], uv1.at[1], ld.at[4]),
    ]
    for cp in loads:
        cp.start()

    loads[0].wait()
    loads[1].wait()
    row = lax.broadcasted_iota(jnp.int32, (8, TOK), 0)
    upto = (
        lax.broadcasted_iota(jnp.int32, (TOK, TOK), 0) <= lax.broadcasted_iota(jnp.int32, (TOK, TOK), 1)
    ).astype(F32).astype(BF)
    for t in range(2):
        ids = ids_v[t]
        gat = gat_v[t].astype(F32)
        hit = jnp.zeros((8, TOK), F32)
        gsum = jnp.zeros((8, TOK), F32)
        for e in range(2):
            match = (ids == e).astype(F32)
            of_e = (row >= 2 * e) & (row < 2 * e + 2)
            hit = jnp.where(of_e, jnp.sum(match, axis=0, keepdims=True), hit)
            gsum = jnp.where(of_e, jnp.sum(match * gat, axis=0, keepdims=True), gsum)
        rank = dot(hit.astype(BF), upto, ((1,), (0,))) - 1.0
        sel = hit * (rank == (row & 1).astype(F32)).astype(F32)
        if t == 0:
            sel_s[0] = sel.astype(BF)
        sel_s[1 + t] = (sel * gsum).astype(BF)

    loads[2].wait()
    rows = dot(sel_s[1], g_v[...], ((1,), (0,)))
    for e in range(2):
        for q in range(4):
            rows_a[0, q, e] = rows[2 * e : 2 * e + 2, q * Q : q * Q + HA].astype(BF)
            rows_b[0, e, :, q * HB : (q + 1) * HB] = rows[2 * e : 2 * e + 2, q * Q + HA : (q + 1) * Q].astype(BF)

    for k in range(K):
        ra1[k, (y + 4) % 8] = jnp.zeros((8, HA), BF)
        for where, oy in ((1, 3), (2, 5)):
            @pl.when(at != where)
            def _(k=k, oy=oy):
                ra1[k, (y + oy) % 8] = jnp.zeros((8, HA), BF)

        for where, slot in ((3, 0), (0, 1)):
            @pl.when(at == where)
            def _(k=k, slot=slot):
                fa[k, slot] = jnp.zeros((8, HA), BF)

        for ox in (3, 4, 5):
            for c_ in range(2):
                x_ = (x + ox) % 8
                rb1[k, ((x_ % 2) * 2 + c_) * 4 + x_ // 2] = jnp.zeros((2, 2, HB), BF)

    @pl.when(p != 1)
    def _():
        pl.semaphore_wait(barrier, len(peers) + 1)

    @pl.when(p == 1)
    def _():
        pl.semaphore_wait(barrier, len(peers))

    @pl.when(p > 1)
    def _():
        pl.semaphore_signal(ready, inc=1, device_id=dev(down, x, y, c), device_id_type=MESH)

    def first_a(t):
        for ox, oc in ROW:
            x_, c_ = (x + ox) % 8, (c + oc) % 2
            q_ = (x_ % 2) * 2 + c_
            send(rows_a.at[t, q_], xa.at[t, mine, xh], (ALL, LOWER)[t], r_x.at[t, mine], dev(p, x_, y, c_))
        xa[t, mine, xh] = rows_a[t, r]

    def first_b(t):
        for oy in FAR + (0,) * t:
            y_ = (y + oy) % 8
            send(
                rows_b.at[t, y_ // 4], yb.at[t, y % 4, half], (ALL, UPPER)[t], r_x2.at[t, mine], dev((p, down)[t], x, y_, c)
            )
        if t == 0:
            yb[t, y % 4, half] = rows_b[t, half]

    def send_b(t, k, x_, c_):
        v = (k + 4 - r) % 4
        columns = pl.ds(pl.multiple_of(((x_ % 2) * 2 + c_) * HB, 128), HB)
        send(yb.at[t, v, :, :, columns], hb.at[t, k, :, v, xh], (ALL, LOWER)[t], r_near2.at[t, k], dev(p, x_, y, c_))

    def direct_a(t, k, oy):
        y_ = (y + oy) % 8
        send(a2.at[t, k, y_ // 4], ha.at[t, k, y], (ALL, LOWER)[t], r_far.at[t, k], dev(p, x, y_, c))

    def second(t, k):
        @pl.when(mine == k)
        def _():
            arrived_kib(3 * B4, r_x.at[t, k])

        @pl.when(mine != k)
        def _():
            arrived_kib(4 * B4, r_x.at[t, k])

        for e in range(2):
            a2[t, k, e] = jnp.concatenate([xa[t, k, h, e] for h in range(4)], axis=0)
        for oy in (2, 6, 1, 7):
            y_ = (y + oy) % 8
            send(a2.at[t, k, y_ // 4], ha.at[t, k, y], (ALL, LOWER)[t], r_near.at[t, k], dev(p, x, y_, c))
        ha[t, k, y] = a2[t, k, half]
        if t == 0:
            @pl.when(mine == k)
            def _():
                arrived_kib(ROWS2, r_x2.at[t, k])

            @pl.when(mine != k)
            def _():
                arrived_kib(2 * ROWS2, r_x2.at[t, k])
        else:
            arrived_kib(2 * ROWS2, r_x2.at[t, k])
        v = (k + 4 - r) % 4
        for ox, oc in NEAR:
            send_b(t, k, (x + ox) % 8, (c + oc) % 2)
        hb[t, k, :, v, xh] = yb[t, v, :, :, pl.ds(pl.multiple_of(r * HB, 128), HB)]

    def landing(k, x_, c_):
        return (k + 4 - ((x_ % 2) * 2 + c_)) % 4, x_ // 2

    def forward(t, k):
        pl.when(at == 1)(functools.partial(direct_a, t, k, 3))
        pl.when(at == 2)(functools.partial(direct_a, t, k, 5))
        arrived_kib(4 * A8, r_near.at[t, k])

        def pass_a(oy_from, oy_to):
            i = (y + oy_from) % 8
            send(ha.at[t, k, i], ha.at[t, k, i], (ALL, LOWER)[t], r_far.at[t, k], dev(p, x, (y + oy_to) % 8, c))

        pass_a(8 - 2 * turn, 8 + 2 * turn)
        pl.when(at != 3)(functools.partial(pass_a, 6, 1))
        pl.when(at != 0)(functools.partial(pass_a, 2, 7))
        arrived_kib(9 * B4, r_near2.at[t, k])
        for ox_from, ox_to, cores in ((6, 2, (0,)), (2, 6, (1,)), (7, 2, (0, 1)), (1, 6, (0, 1))):
            for c_ in cores:
                v, i = landing(k, (x + ox_from) % 8, c_)
                send(
                    hb.at[t, k, :, v, i], hb.at[t, k, :, v, i], (ALL, LOWER)[t], r_far.at[t, k], dev(p, (x + ox_to) % 8, y, c)
                )

    def dispatched(t, k):
        arrived_kib(3 * A8 + 6 * B4, r_far.at[t, k])
        hd[t, k] = hb[t, k].reshape(64, HB)

    others = ((1, 0), (1, 1), (0, 1))

    def peer(ol, oc):
        return ((r // 2 + ol) % 2) * 2 + (c + oc) % 2

    first_a(0)
    first_b(0)
    arrived_kib(2 * UV128, ld.at[4])
    for ol, oc in others:
        send(uv.at[r], uv.at[r], ALL, r_one.at[1], (p, peer(ol, oc), s))
    u, v = (uv1[h].astype(F32).reshape(TOK, HID) for h in range(2))
    av1[r] = (u * jax.nn.sigmoid(u) * v).astype(BF)
    for ol, oc in others:
        send(av1.at[r], av1.at[r], ALL, r_one.at[4], (p, peer(ol, oc), s))
    arrived_kib(3 * Q // 4, ld.at[3])
    w2t[...] = w2[...].astype(F32).T.astype(BF)
    w13t[...] = w13[...].astype(F32).T.astype(BF)

    @pl.when(lower & upper)
    def _():
        pl.semaphore_wait(ready, 1)

    @pl.when(lower)
    def _():
        send(sel_s.at[2], sel_in, SEL, r_one.at[0], dev(up, x, y, c))

    for k in range(K):
        second(0, k)

    for k in range(K):
        forward(0, k)

    @pl.when(upper)
    def _():
        arrived(sel_in, r_one.at[0])
        base_v[...] = dot(sel_in[...], g_v[...], ((1,), (0,)))
        m_v[...] = dot(sel_in[...], sel_s[0], ((1,), (1,)))
        for e in range(2):
            for q in range(4):
                base_o[q, e] = base_v[2 * e : 2 * e + 2, q * Q : q * Q + HA]
        send(base_o, base_in, UPPER, r_one.at[2], dev(down, x, y, c))
        send(m_v, m_in, MM, r_one.at[3], dev(down, x, y, c))

    arrived(uv.at[0:3], r_one.at[1])
    for k in range(K):
        u, v = (
            jnp.concatenate(
                [uv[(k - yy) % 4, h, 4 * yy : 4 * yy + 4].astype(F32).reshape(8, HID) for yy in range(8)], axis=0
            )
            for h in range(2)
        )
        sig = jax.nn.sigmoid(u)
        act = u * sig
        coef[k, 0] = v * (sig * (1.0 + u * (1.0 - sig)))
        coef[k, 1] = act
        av = (act * v).astype(BF)
        avt[0, k] = av.astype(F32).T.astype(BF)

    def hidden_gradient(k):
        d_a = dot(ha[0, k].reshape(64, HA), w2t[0:HA], ((1,), (0,))) + dot(hd[0, k], w2t[HA:Q], ((1,), (0,)))
        dx[k, r] = d_a.astype(BF)
        for ol, oc in others:
            send(dx.at[k, r], dx.at[k, r], UPPER, r_dx.at[k], (p, peer(ol, oc), s))

    def near_a(k, oy):
        i = (y + oy) % 8
        send(pa.at[k, i], ra1.at[k, y], UPPER, r_back.at[k], dev(p, x, i, c))

    def near_b(k, x_, c_):
        v, i = landing(k, x_, c_)
        send(pb.at[k, :, v, i], rb1.at[k, r * 4 + xh], UPPER, r_back2.at[k], dev(p, x_, y, c_))

    def input_gradient(k):
        arrived(dx.at[k, 0:3], r_dx.at[k])
        d_act = (dx[k, 0].astype(F32) + dx[k, 1].astype(F32)) + (dx[k, 2].astype(F32) + dx[k, 3].astype(F32))
        d_gu = jnp.concatenate([(d_act * coef[k, 0]).astype(BF), (d_act * coef[k, 1]).astype(BF)], axis=1)
        pa[k] = dot(d_gu, w13t[:, 0:HA], ((1,), (0,))).astype(BF).reshape(8, 8, HA)

        def far_a(oy_row, oy_to, slot):
            i = (y + oy_row) % 8
            send(pa.at[k, i], fa.at[k, slot], UPPER, r_f.at[k], dev(p, x, (y + oy_to) % 8, c))

        far_a(4, 8 + 2 * turn, 2)
        pl.when(at != 0)(functools.partial(far_a, 5, 7, 0))
        pl.when(at == 0)(functools.partial(near_a, k, 5))
        pl.when(at != 3)(functools.partial(far_a, 3, 1, 1))
        pl.when(at == 3)(functools.partial(near_a, k, 3))
        ra1[k, y] = pa[k, y]
        pb[k] = dot(d_gu, w13t[:, HA:Q], ((1,), (0,))).astype(BF).reshape(2, 4, 4, 2, HB)

        for ox, ox_to, c_, slot in BACK:
            v, i = landing(k, (x + ox) % 8, c_)
            send(pb.at[k, :, v, i], fb.at[k, slot], UPPER, r_f2.at[k], dev(p, (x + ox_to) % 8, y, c))
        v, i = landing(k, x, c)
        rb1[k, r * 4 + xh] = pb[k, :, v, i]

    def forward_back(k):
        near_a(k, 1)
        near_a(k, 7)
        for ox, c_ in ((6, 1), (2, 0), (0, 1 - c)):
            near_b(k, (x + ox) % 8, c_)
        @pl.when(inner)
        def _():
            arrived_kib(3 * A8, r_f.at[k])

        @pl.when(jnp.logical_not(inner))
        def _():
            arrived_kib(2 * A8, r_f.at[k])

        tie = fa[k, 2].astype(F32)
        for slot, oy, tied in ((0, 6, at < 2), (1, 2, at >= 2)):
            i = (y + oy) % 8
            acc = pa[k, i].astype(F32) + fa[k, slot].astype(F32) + jnp.where(tied, tie, 0.0)
            sa[k, slot] = acc.astype(BF)
            send(sa.at[k, slot], ra1.at[k, y], UPPER, r_back.at[k], dev(p, x, i, c))
        arrived_kib(6 * B4, r_f2.at[k])
        for slot, ox, c_ in ((2, 6, 0), (5, 2, 1), (0, 7, 0), (1, 7, 1), (3, 1, 0), (4, 1, 1)):
            x_ = (x + ox) % 8
            v, i = landing(k, x_, c_)
            acc = pb[k, :, v, i].astype(F32) + fb[k, slot].astype(F32)
            sb[k, slot] = acc.astype(BF)
            send(sb.at[k, slot], rb1.at[k, r * 4 + xh], UPPER, r_back2.at[k], dev(p, x_, y, c_))

    def to_sources(k):
        @pl.when(inner)
        def _():
            arrived_kib(5 * A8, r_back.at[k])

        @pl.when(jnp.logical_not(inner))
        def _():
            arrived_kib(4 * A8, r_back.at[k])

        for e in range(2):
            acc = ra1[k, 4 * e].astype(F32)
            for h in range(1, 4):
                acc = acc + ra1[k, 4 * e + h].astype(F32)
            for h in range(4):
                ta[k, h, e] = acc[2 * h : 2 * h + 2].astype(BF)
        r_ = (k + 8 - y) % 4
        side = 1 + 2 * (x % 2)
        for o in (2, side, 4 - side, 0):
            h_ = (xh + o) % 4
            send(ta.at[k, h_], ra2.at[r * 4 + xh], UPPER, r_ra2, (down, r_, y * 4 + h_))
        arrived_kib(9 * B4, r_back2.at[k])
        for q in range(4):
            acc = rb1[k, 4 * q].astype(F32)
            for h in range(1, 4):
                acc = acc + rb1[k, 4 * q + h].astype(F32)
            for h in range(2):
                tb[k, h, :, q * HB : (q + 1) * HB] = acc[h].astype(BF)
        v = (k + 4 - r) % 4
        d = (v + 8 - y) % 4
        far = (y + jnp.where(d < 2, d + 4, d)) % 8 // 4
        for h in (far, 1 - far):
            y_ = v + 4 * h

            def go(h=h, y_=y_):
                send(tb.at[k, h], rb2.at[y], UPPER, r_rb2, dev(p, x, y_, c))

            pl.when(y_ != y)(go)

            @pl.when(y_ == y)
            def _(h=h):
                rb2[y] = tb[k, h]

    def mixed(e, base, m, back):
        for f in range(2):
            for h in range(2):
                base = base + m[2 * e : 2 * e + 2, 2 * f + h : 2 * f + h + 1] * back[f][h : h + 1, :]
        return base.astype(BF)

    def next_rows():
        @pl.when(upper)
        def _():
            arrived(rb2.at[0:7], r_rb2)
            back = []
            for f in range(2):
                acc = rb2[4 * f].astype(F32)
                for h in range(1, 4):
                    acc = acc + rb2[4 * f + h].astype(F32)
                back.append(acc)
            for q in range(4):
                for e in range(2):
                    rows_b[1, e, :, q * HB : (q + 1) * HB] = mixed(
                        e,
                        base_v[2 * e : 2 * e + 2, q * Q + HA : (q + 1) * Q],
                        m_v[...],
                        [b[:, q * HB : (q + 1) * HB] for b in back],
                    )
            first_b(1)

        @pl.when(lower)
        def _():
            arrived(ra2, r_ra2)
            for q in range(4):
                back = []
                for f in range(2):
                    acc = ra2[4 * q, f].astype(F32)
                    for h in range(1, 4):
                        acc = acc + ra2[4 * q + h, f].astype(F32)
                    back.append(acc)
                for e in range(2):
                    rows_a[1, q, e] = mixed(e, base_in[q, e], m_in[...], back)
            first_a(1)

    def gather_rows(k):
        pl.when(mine == k)(next_rows)

    for k in range(K):
        dispatched(0, k)
        pl.when(upper)(functools.partial(hidden_gradient, k))
    for k in range(K):
        pl.when(upper)(functools.partial(input_gradient, k))
    left = jnp.concatenate([avt[0, k] for k in range(K)], axis=1)
    out[0, :, 0:HA] = dot(left, ha[0].reshape(K * 64, HA), ((1,), (0,)))
    out[0, :, HA:Q] = dot(left, hd[0].reshape(K * 64, HB), ((1,), (0,)))
    for k in range(K):
        pl.when(upper)(functools.partial(forward_back, k))
    arrived(av1.at[0:3], r_one.at[4])
    for k in range(K):
        av = jnp.concatenate([av1[(k - yy) % 4, 8 * yy : 8 * yy + 8] for yy in range(8)], axis=0)
        avt[1, k] = av.astype(F32).T.astype(BF)

    @pl.when(lower)
    def _():
        arrived(base_in, r_one.at[2])
        arrived(m_in, r_one.at[3])

    def if_lower(step, *args):
        pl.when(lower)(functools.partial(step, *args))

    def finish(k):
        dispatched(1, k)
        out[0, :, 0:HA] += dot(avt[1, k], ha[1, k].reshape(64, HA), ((1,), (0,)))
        out[0, :, HA:Q] += dot(avt[1, k], hd[1, k], ((1,), (0,)))

    pl.when(upper)(functools.partial(to_sources, 0))
    pl.when(upper)(functools.partial(to_sources, 1))
    pl.when(upper)(functools.partial(to_sources, 2))
    pl.when(upper)(functools.partial(to_sources, 3))
    gather_rows(0)
    gather_rows(1)
    gather_rows(2)
    gather_rows(3)
    if_lower(second, 1, 0)
    if_lower(second, 1, 1)
    if_lower(second, 1, 2)
    if_lower(second, 1, 3)
    if_lower(forward, 1, 0)
    if_lower(forward, 1, 1)
    if_lower(forward, 1, 2)
    if_lower(forward, 1, 3)
    for k in range(K):
        if_lower(finish, k)

    def second_size(forwards):
        return 16 * A8 + K * forwards * A8 + 60 * B4

    first_a_size, first_b_size = 15 * B4, 7 * ROWS2
    all_size = first_a_size + first_b_size + 3 * UV128 + 3 * DX64
    for chosen, forwards in ((inner, 4), (jnp.logical_not(inner), 2)):
        @pl.when(chosen)
        def _(forwards=forwards):
            arrived_kib(all_size + second_size(forwards), snd.at[ALL])

        @pl.when(chosen & lower)
        def _(forwards=forwards):
            arrived_kib(first_a_size + second_size(forwards), snd.at[LOWER])

    @pl.when(lower)
    def _():
        arrived(sel_in, snd.at[SEL])

    @pl.when(upper)
    def _():
        arrived_kib(8 * ROWS2 + 12 * DX64 + 28 * A8 + 60 * B4 + 16 * B4 + 7 * ROWS2 + 56, snd.at[UPPER])
        arrived(m_in, snd.at[MM])


def body(cotangent, routes, gates, *others):
    hbm = pl.BlockSpec(memory_space=pl.ANY)
    dma = pltpu.SemaphoreType.DMA
    vmem = pltpu.VMEM
    return pl.pallas_call(
        kernel,
        out_shape=vmem((1, HID, Q), F32),
        in_specs=[hbm] * 8,
        out_specs=pl.BlockSpec(memory_space=vmem),
        scratch_shapes=[
            vmem((TOK, D), BF),
            vmem((2, 8, TOK), jnp.int32),
            vmem((2, 8, TOK), BF),
            vmem((HID, Q), BF),
            vmem((Q, 2 * HID), BF),
            vmem((Q, HID), BF),
            vmem((2 * HID, Q), BF),
            vmem((3, 8, TOK), BF),
            vmem((8, TOK), BF),
            vmem((2, 4, 2, 2, HA), BF),
            vmem((2, 2, 2, 4 * HB), BF),
            vmem((8, D), F32),
            vmem((4, 2, 2, HA), F32),
            vmem((4, 2, 2, HA), F32),
            vmem((8, 8), F32),
            vmem((8, 8), F32),
            vmem((4, 2, 32, 2, HID), BF),
            vmem((2, 32, 2, HID), BF),
            vmem((4, TOK, HID), BF),
            vmem((K, 2, 64, HID), F32),
            vmem((2, K, HID, 64), BF),
            vmem((1536, 4, 128), BF),
            vmem((2, K, 4, 2, 2, HA), BF),
            vmem((2, K, 2, 8, HA), BF),
            vmem((2, 4, 2, 2, 4 * HB), BF),
            vmem((2, K, 8, 8, HA), BF),
            vmem((2, K, 2, 4, 4, 2, HB), BF),
            vmem((2, K, 64, HB), BF),
            vmem((K, 4, 64, HID), BF),
            vmem((K, 8, 8, HA), BF),
            vmem((K, 2, 4, 4, 2, HB), BF),
            vmem((K, 3, 8, HA), BF),
            vmem((K, 6, 2, 2, HB), BF),
            vmem((K, 2, 8, HA), BF),
            vmem((K, 6, 2, 2, HB), BF),
            vmem((K, 8, 8, HA), BF),
            vmem((K, 16, 2, 2, HB), BF),
            vmem((K, 4, 2, 2, HA), BF),
            vmem((K, 2, 2, 4 * HB), BF),
            vmem((16, 2, 2, HA), BF),
            vmem((8, 2, 4 * HB), BF),
            dma((5,)),
            dma((5,)),
            dma((2, K)),
            dma((2, K)),
            dma((2, K)),
            dma((K,)),
            dma((K,)),
            dma((K,)),
            dma,
            dma,
            dma((5,)),
            pltpu.SemaphoreType.REGULAR,
            dma((2, K)),
            dma((2, K)),
            dma((K,)),
            dma((K,)),
        ],
        compiler_params=pltpu.CompilerParams(collective_id=0, has_side_effects=True),
        name="cooldown",
    )(cotangent, jnp.swapaxes(routes, 2, 3), jnp.swapaxes(gates, 2, 3), *others)


def solution(mesh):
    in_specs = (
        P("pipe", ("dp", "expert"), None),
        P("pipe", None, ("dp", "expert"), None),
        P("pipe", None, ("dp", "expert"), None),
        P("pipe", None, "dp", None, None, "expert"),
        P("pipe", None, "dp", None, None, "expert"),
        P("pipe", None, "expert"),
        P("pipe", None, "expert"),
        P("pipe", "expert", None),
    )
    out_specs = P("pipe", "expert", "dp")
    return jax.shard_map(body, mesh=mesh, in_specs=in_specs, out_specs=out_specs, check_vma=False)
```

```python
import functools

import jax
import jax.numpy as jnp
from jax import lax
from jax.experimental import pallas as pl
from jax.experimental.pallas import tpu as pltpu
from jax.sharding import PartitionSpec as P

MESH = pl.DeviceIdType.MESH
BF = jnp.bfloat16
F32 = jnp.float32

D = 7168
TOK = 64
HID = 128
Q = 1792
HA = HB = 896
K = 4
FAR = (4, 3, 5, 2, 6, 1, 7)
ROW = tuple((dx, dc) for dx in FAR for dc in (0, 1)) + ((0, 1),)
NEAR = tuple((dx, dc) for dx in (2, 6, 1, 7) for dc in (0, 1)) + ((0, 1),)
BACK = ((4, 6, 0, 2), (4, 2, 1, 5), (5, 6, 0, 0), (5, 6, 1, 1), (3, 2, 0, 3), (3, 2, 1, 4))
A8, B4, ROWS2, DX64, UV128 = 14, 7, 14, 16, 32


def dot(a, b, dims):
    return lax.dot_general(a, b, (dims, ((), ())), preferred_element_type=F32)


def kernel(
    cot, routes, gates, gate_pre, up_pre, w_gate, w_up, w_down, out,
    g_v, ids_v, gat_v, w2, w13, w2t, w13t, sel_s, sel_in, rows_a, rows_b, base_v, base_o, base_in, m_v, m_in, uv, uv1, av1, coef, avt,
    void, xa, a2, yb, ha, hb, hd, dx, pa, pb, fa, fb, sa, sb, ra1, rb1, ta, tb, ra2, rb2,
    ld, snd, r_x, r_near, r_far, r_dx, r_f, r_back, r_ra2, r_rb2, r_one, ready, r_x2, r_near2, r_f2, r_back2,
):
    p = lax.axis_index("pipe")
    r = lax.axis_index("dp")
    s = lax.axis_index("expert")
    y = s // 4
    xh = s % 4
    x = xh * 2 + r // 2
    c = r % 2
    lower = p < 7
    upper = p > 0
    up = jnp.minimum(p + 1, 7)
    down = jnp.maximum(p - 1, 0)
    mine = (r + y) % 4
    half = y // 4
    at = y % 4
    inner = (at == 1) | (at == 2)
    turn = jnp.where(at < 2, 1, -1)

    def dev(p_, x_, y_, c_):
        return (p_, (x_ % 2) * 2 + c_, y_ * 4 + x_ // 2)

    def send(src, dst, kind, recv, target):
        pltpu.make_async_remote_copy(
            src_ref=src, dst_ref=dst, send_sem=snd.at[kind], recv_sem=recv, device_id=target, device_id_type=MESH
        ).start()

    def arrived(like, sem):
        pltpu.make_async_copy(like, like, sem).wait()

    def each_chunk(step):
        def turn_of(k, carry):
            step(k)
            return carry

        lax.fori_loop(0, K, turn_of, 0)

    def arrived_kib(size, sem):
        arrived(void.at[0:size], sem)

    ALL, LOWER, UPPER, SEL, MM = range(5)

    barrier = pltpu.get_barrier_semaphore()
    peers = [((x + ox) % 8, y, (c + oc) % 2, p) for ox, oc in ROW]
    peers += [(x, (y + oy) % 8, c, p) for oy in FAR]
    for x_, y_, c_, p_ in peers:
        pl.semaphore_signal(barrier, inc=1, device_id=dev(p_, x_, y_, c_), device_id_type=MESH)

    @pl.when(lower & upper)
    def _():
        pl.semaphore_signal(barrier, inc=1, device_id=dev(up, x, y, c), device_id_type=MESH)

    @pl.when(p == 1)
    def _():
        pl.semaphore_signal(barrier, inc=1, device_id=dev(down, x, y, c), device_id_type=MESH)

    q0 = pl.multiple_of(r * Q, 128)
    loads = [
        pltpu.make_async_copy(routes.at[0], ids_v, ld.at[0]),
        pltpu.make_async_copy(gates.at[0], gat_v, ld.at[1]),
        pltpu.make_async_copy(cot.at[0], g_v, ld.at[2]),
        pltpu.make_async_copy(w_down.at[0, :, pl.ds(q0, Q)], w2, ld.at[3]),
        pltpu.make_async_copy(w_gate.at[0, pl.ds(q0, Q)], w13.at[:, 0:HID], ld.at[3]),
        pltpu.make_async_copy(w_up.at[0, pl.ds(q0, Q)], w13.at[:, HID : 2 * HID], ld.at[3]),
        pltpu.make_async_copy(gate_pre.at[0, 0, 0], uv.at[r, 0], ld.at[4]),
        pltpu.make_async_copy(up_pre.at[0, 0, 0], uv.at[r, 1], ld.at[4]),
        pltpu.make_async_copy(gate_pre.at[0, 1, 0], uv1.at[0], ld.at[4]),
        pltpu.make_async_copy(up_pre.at[0, 1, 0], uv1.at[1], ld.at[4]),
    ]
    for cp in loads:
        cp.start()

    loads[0].wait()
    loads[1].wait()
    row = lax.broadcasted_iota(jnp.int32, (8, TOK), 0)
    upto = (
        lax.broadcasted_iota(jnp.int32, (TOK, TOK), 0) <= lax.broadcasted_iota(jnp.int32, (TOK, TOK), 1)
    ).astype(F32).astype(BF)
    for t in range(2):
        ids = ids_v[t]
        gat = gat_v[t].astype(F32)
        hit = jnp.zeros((8, TOK), F32)
        gsum = jnp.zeros((8, TOK), F32)
        for e in range(2):
            match = (ids == e).astype(F32)
            of_e = (row >= 2 * e) & (row < 2 * e + 2)
            hit = jnp.where(of_e, jnp.sum(match, axis=0, keepdims=True), hit)
            gsum = jnp.where(of_e, jnp.sum(match * gat, axis=0, keepdims=True), gsum)
        rank = dot(hit.astype(BF), upto, ((1,), (0,))) - 1.0
        sel = hit * (rank == (row & 1).astype(F32)).astype(F32)
        if t == 0:
            sel_s[0] = sel.astype(BF)
        sel_s[1 + t] = (sel * gsum).astype(BF)

    loads[2].wait()
    rows = dot(sel_s[1], g_v[...], ((1,), (0,)))
    for e in range(2):
        for q in range(4):
            rows_a[0, q, e] = rows[2 * e : 2 * e + 2, q * Q : q * Q + HA].astype(BF)
            rows_b[0, e, :, q * HB : (q + 1) * HB] = rows[2 * e : 2 * e + 2, q * Q + HA : (q + 1) * Q].astype(BF)

    for k in range(K):
        ra1[k, (y + 4) % 8] = jnp.zeros((8, HA), BF)
        for where, oy in ((1, 3), (2, 5)):
            @pl.when(at != where)
            def _(k=k, oy=oy):
                ra1[k, (y + oy) % 8] = jnp.zeros((8, HA), BF)

        for where, slot in ((3, 0), (0, 1)):
            @pl.when(at == where)
            def _(k=k, slot=slot):
                fa[k, slot] = jnp.zeros((8, HA), BF)

        for ox in (3, 4, 5):
            for c_ in range(2):
                x_ = (x + ox) % 8
                rb1[k, ((x_ % 2) * 2 + c_) * 4 + x_ // 2] = jnp.zeros((2, 2, HB), BF)

    @pl.when(p != 1)
    def _():
        pl.semaphore_wait(barrier, len(peers) + 1)

    @pl.when(p == 1)
    def _():
        pl.semaphore_wait(barrier, len(peers))

    @pl.when(p > 1)
    def _():
        pl.semaphore_signal(ready, inc=1, device_id=dev(down, x, y, c), device_id_type=MESH)

    def first_a(t):
        for ox, oc in ROW:
            x_, c_ = (x + ox) % 8, (c + oc) % 2
            q_ = (x_ % 2) * 2 + c_
            send(rows_a.at[t, q_], xa.at[t, mine, xh], (ALL, LOWER)[t], r_x.at[t, mine], dev(p, x_, y, c_))
        xa[t, mine, xh] = rows_a[t, r]

    def first_b(t):
        for oy in FAR + (0,) * t:
            y_ = (y + oy) % 8
            send(
                rows_b.at[t, y_ // 4], yb.at[t, y % 4, half], (ALL, UPPER)[t], r_x2.at[t, mine], dev((p, down)[t], x, y_, c)
            )
        if t == 0:
            yb[t, y % 4, half] = rows_b[t, half]

    def send_b(t, k, x_, c_):
        v = (k + 4 - r) % 4
        columns = pl.ds(pl.multiple_of(((x_ % 2) * 2 + c_) * HB, 128), HB)
        send(yb.at[t, v, :, :, columns], hb.at[t, k, :, v, xh], (ALL, LOWER)[t], r_near2.at[t, k], dev(p, x_, y, c_))

    def direct_a(t, k, oy):
        y_ = (y + oy) % 8
        send(a2.at[t, k, y_ // 4], ha.at[t, k, y], (ALL, LOWER)[t], r_far.at[t, k], dev(p, x, y_, c))

    def second(t, k):
        @pl.when(mine == k)
        def _():
            arrived_kib(3 * B4, r_x.at[t, k])

        @pl.when(mine != k)
        def _():
            arrived_kib(4 * B4, r_x.at[t, k])

        for e in range(2):
            a2[t, k, e] = jnp.concatenate([xa[t, k, h, e] for h in range(4)], axis=0)
        for oy in (2, 6, 1, 7):
            y_ = (y + oy) % 8
            send(a2.at[t, k, y_ // 4], ha.at[t, k, y], (ALL, LOWER)[t], r_near.at[t, k], dev(p, x, y_, c))
        ha[t, k, y] = a2[t, k, half]
        if t == 0:
            @pl.when(mine == k)
            def _():
                arrived_kib(ROWS2, r_x2.at[t, k])

            @pl.when(mine != k)
            def _():
                arrived_kib(2 * ROWS2, r_x2.at[t, k])
        else:
            arrived_kib(2 * ROWS2, r_x2.at[t, k])
        v = (k + 4 - r) % 4
        for ox, oc in NEAR:
            send_b(t, k, (x + ox) % 8, (c + oc) % 2)
        hb[t, k, :, v, xh] = yb[t, v, :, :, pl.ds(pl.multiple_of(r * HB, 128), HB)]

    def landing(k, x_, c_):
        return (k + 4 - ((x_ % 2) * 2 + c_)) % 4, x_ // 2

    def forward(t, k):
        pl.when(at == 1)(functools.partial(direct_a, t, k, 3))
        pl.when(at == 2)(functools.partial(direct_a, t, k, 5))
        arrived_kib(4 * A8, r_near.at[t, k])

        def pass_a(oy_from, oy_to):
            i = (y + oy_from) % 8
            send(ha.at[t, k, i], ha.at[t, k, i], (ALL, LOWER)[t], r_far.at[t, k], dev(p, x, (y + oy_to) % 8, c))

        pass_a(8 - 2 * turn, 8 + 2 * turn)
        pl.when(at != 3)(functools.partial(pass_a, 6, 1))
        pl.when(at != 0)(functools.partial(pass_a, 2, 7))
        arrived_kib(9 * B4, r_near2.at[t, k])
        for ox_from, ox_to, cores in ((6, 2, (0,)), (2, 6, (1,)), (7, 2, (0, 1)), (1, 6, (0, 1))):
            for c_ in cores:
                v, i = landing(k, (x + ox_from) % 8, c_)
                send(
                    hb.at[t, k, :, v, i], hb.at[t, k, :, v, i], (ALL, LOWER)[t], r_far.at[t, k], dev(p, (x + ox_to) % 8, y, c)
                )

    def dispatched(t, k):
        arrived_kib(3 * A8 + 6 * B4, r_far.at[t, k])
        hd[t, k] = hb[t, k].reshape(64, HB)

    others = [(ol, oc) for ol in (0, 1) for oc in (0, 1) if (ol, oc) != (0, 0)]

    def peer(ol, oc):
        return ((r // 2 + ol) % 2) * 2 + (c + oc) % 2

    first_a(0)
    first_b(0)
    arrived_kib(2 * UV128, ld.at[4])
    for ol, oc in others:
        send(uv.at[r], uv.at[r], ALL, r_one.at[1], (p, peer(ol, oc), s))
    u, v = (uv1[h].astype(F32).reshape(TOK, HID) for h in range(2))
    av1[r] = (u * jax.nn.sigmoid(u) * v).astype(BF)
    for ol, oc in others:
        send(av1.at[r], av1.at[r], ALL, r_one.at[4], (p, peer(ol, oc), s))
    @pl.when(lower & upper)
    def _():
        pl.semaphore_wait(ready, 1)

    @pl.when(lower)
    def _():
        send(sel_s.at[2], sel_in, SEL, r_one.at[0], dev(up, x, y, c))

    each_chunk(functools.partial(second, 0))
    arrived_kib(3 * Q // 4, ld.at[3])
    w2t[...] = w2[...].astype(F32).T.astype(BF)
    w13t[...] = w13[...].astype(F32).T.astype(BF)
    each_chunk(functools.partial(forward, 0))

    @pl.when(upper)
    def _():
        arrived(sel_in, r_one.at[0])
        base_v[...] = dot(sel_in[...], g_v[...], ((1,), (0,)))
        m_v[...] = dot(sel_in[...], sel_s[0], ((1,), (1,)))
        for e in range(2):
            for q in range(4):
                base_o[q, e] = base_v[2 * e : 2 * e + 2, q * Q : q * Q + HA]
        send(base_o, base_in, UPPER, r_one.at[2], dev(down, x, y, c))
        send(m_v, m_in, MM, r_one.at[3], dev(down, x, y, c))

    arrived(uv.at[0:3], r_one.at[1])
    for k in range(K):
        u, v = (
            jnp.concatenate(
                [uv[(k - yy) % 4, h, 4 * yy : 4 * yy + 4].astype(F32).reshape(8, HID) for yy in range(8)], axis=0
            )
            for h in range(2)
        )
        sig = jax.nn.sigmoid(u)
        act = u * sig
        coef[k, 0] = v * (sig * (1.0 + u * (1.0 - sig)))
        coef[k, 1] = act
        av = (act * v).astype(BF)
        avt[0, k] = av.astype(F32).T.astype(BF)

    def hidden_gradient(k):
        d_a = dot(ha[0, k].reshape(64, HA), w2t[0:HA], ((1,), (0,))) + dot(hd[0, k], w2t[HA:Q], ((1,), (0,)))
        dx[k, r] = d_a.astype(BF)
        for ol, oc in others:
            send(dx.at[k, r], dx.at[k, r], UPPER, r_dx.at[k], (p, peer(ol, oc), s))

    def near_a(k, oy):
        i = (y + oy) % 8
        send(pa.at[k, i], ra1.at[k, y], UPPER, r_back.at[k], dev(p, x, i, c))

    def near_b(k, x_, c_):
        v, i = landing(k, x_, c_)
        send(pb.at[k, :, v, i], rb1.at[k, r * 4 + xh], UPPER, r_back2.at[k], dev(p, x_, y, c_))

    def input_gradient(k):
        arrived(dx.at[k, 0:3], r_dx.at[k])
        d_act = (dx[k, 0].astype(F32) + dx[k, 1].astype(F32)) + (dx[k, 2].astype(F32) + dx[k, 3].astype(F32))
        d_gu = jnp.concatenate([(d_act * coef[k, 0]).astype(BF), (d_act * coef[k, 1]).astype(BF)], axis=1)
        pa[k] = dot(d_gu, w13t[:, 0:HA], ((1,), (0,))).astype(BF).reshape(8, 8, HA)

        def far_a(oy_row, oy_to, slot):
            i = (y + oy_row) % 8
            send(pa.at[k, i], fa.at[k, slot], UPPER, r_f.at[k], dev(p, x, (y + oy_to) % 8, c))

        far_a(4, 8 + 2 * turn, 2)
        pl.when(at != 0)(functools.partial(far_a, 5, 7, 0))
        pl.when(at == 0)(functools.partial(near_a, k, 5))
        pl.when(at != 3)(functools.partial(far_a, 3, 1, 1))
        pl.when(at == 3)(functools.partial(near_a, k, 3))
        ra1[k, y] = pa[k, y]
        pb[k] = dot(d_gu, w13t[:, HA:Q], ((1,), (0,))).astype(BF).reshape(2, 4, 4, 2, HB)

        for ox, ox_to, c_, slot in BACK:
            v, i = landing(k, (x + ox) % 8, c_)
            send(pb.at[k, :, v, i], fb.at[k, slot], UPPER, r_f2.at[k], dev(p, (x + ox_to) % 8, y, c))
        v, i = landing(k, x, c)
        rb1[k, r * 4 + xh] = pb[k, :, v, i]

    def forward_back(k):
        near_a(k, 1)
        near_a(k, 7)
        for ox, c_ in ((6, 1), (2, 0), (0, 1 - c)):
            near_b(k, (x + ox) % 8, c_)
        @pl.when(inner)
        def _():
            arrived_kib(3 * A8, r_f.at[k])

        @pl.when(jnp.logical_not(inner))
        def _():
            arrived_kib(2 * A8, r_f.at[k])

        tie = fa[k, 2].astype(F32)
        for slot, oy, tied in ((0, 6, at < 2), (1, 2, at >= 2)):
            i = (y + oy) % 8
            acc = pa[k, i].astype(F32) + fa[k, slot].astype(F32) + jnp.where(tied, tie, 0.0)
            sa[k, slot] = acc.astype(BF)
            send(sa.at[k, slot], ra1.at[k, y], UPPER, r_back.at[k], dev(p, x, i, c))
        arrived_kib(6 * B4, r_f2.at[k])
        for slot, ox, c_ in ((2, 6, 0), (5, 2, 1), (0, 7, 0), (1, 7, 1), (3, 1, 0), (4, 1, 1)):
            x_ = (x + ox) % 8
            v, i = landing(k, x_, c_)
            acc = pb[k, :, v, i].astype(F32) + fb[k, slot].astype(F32)
            sb[k, slot] = acc.astype(BF)
            send(sb.at[k, slot], rb1.at[k, r * 4 + xh], UPPER, r_back2.at[k], dev(p, x_, y, c_))

    def to_sources(k):
        @pl.when(inner)
        def _():
            arrived_kib(5 * A8, r_back.at[k])

        @pl.when(jnp.logical_not(inner))
        def _():
            arrived_kib(4 * A8, r_back.at[k])

        for e in range(2):
            acc = ra1[k, 4 * e].astype(F32)
            for h in range(1, 4):
                acc = acc + ra1[k, 4 * e + h].astype(F32)
            for h in range(4):
                ta[k, h, e] = acc[2 * h : 2 * h + 2].astype(BF)
        r_ = (k + 8 - y) % 4
        for h in range(4):
            send(ta.at[k, h], ra2.at[r * 4 + xh], UPPER, r_ra2, (down, r_, y * 4 + h))
        arrived_kib(9 * B4, r_back2.at[k])
        for q in range(4):
            acc = rb1[k, 4 * q].astype(F32)
            for h in range(1, 4):
                acc = acc + rb1[k, 4 * q + h].astype(F32)
            for h in range(2):
                tb[k, h, :, q * HB : (q + 1) * HB] = acc[h].astype(BF)
        v = (k + 4 - r) % 4
        for h in range(2):

            def go(h=h):
                send(tb.at[k, h], rb2.at[y], UPPER, r_rb2, dev(p, x, v + 4 * h, c))

            pl.when(v + 4 * h != y)(go)

            @pl.when(v + 4 * h == y)
            def _(h=h):
                rb2[y] = tb[k, h]

    def mixed(e, base, m, back):
        for f in range(2):
            for h in range(2):
                base = base + m[2 * e : 2 * e + 2, 2 * f + h : 2 * f + h + 1] * back[f][h : h + 1, :]
        return base.astype(BF)

    def next_rows():
        @pl.when(upper)
        def _():
            arrived(rb2.at[0:7], r_rb2)
            back = []
            for f in range(2):
                acc = rb2[4 * f].astype(F32)
                for h in range(1, 4):
                    acc = acc + rb2[4 * f + h].astype(F32)
                back.append(acc)
            for q in range(4):
                for e in range(2):
                    rows_b[1, e, :, q * HB : (q + 1) * HB] = mixed(
                        e,
                        base_v[2 * e : 2 * e + 2, q * Q + HA : (q + 1) * Q],
                        m_v[...],
                        [b[:, q * HB : (q + 1) * HB] for b in back],
                    )
            first_b(1)

        @pl.when(lower)
        def _():
            arrived(ra2, r_ra2)
            for q in range(4):
                back = []
                for f in range(2):
                    acc = ra2[4 * q, f].astype(F32)
                    for h in range(1, 4):
                        acc = acc + ra2[4 * q + h, f].astype(F32)
                    back.append(acc)
                for e in range(2):
                    rows_a[1, q, e] = mixed(e, base_in[q, e], m_in[...], back)
            first_a(1)

    def to_hidden(k):
        dispatched(0, k)
        pl.when(upper)(functools.partial(hidden_gradient, k))

    each_chunk(to_hidden)
    pl.when(upper)(functools.partial(each_chunk, input_gradient))
    left = jnp.concatenate([avt[0, k] for k in range(K)], axis=1)
    out[0, :, 0:HA] = dot(left, ha[0].reshape(K * 64, HA), ((1,), (0,)))
    out[0, :, HA:Q] = dot(left, hd[0].reshape(K * 64, HB), ((1,), (0,)))
    pl.when(upper)(functools.partial(each_chunk, forward_back))
    arrived(av1.at[0:3], r_one.at[4])
    for k in range(K):
        av = jnp.concatenate([av1[(k - yy) % 4, 8 * yy : 8 * yy + 8] for yy in range(8)], axis=0)
        avt[1, k] = av.astype(F32).T.astype(BF)

    @pl.when(lower)
    def _():
        arrived(base_in, r_one.at[2])
        arrived(m_in, r_one.at[3])

    def finish(k):
        dispatched(1, k)
        out[0, :, 0:HA] += dot(avt[1, k], ha[1, k].reshape(64, HA), ((1,), (0,)))
        out[0, :, HA:Q] += dot(avt[1, k], hd[1, k], ((1,), (0,)))

    pl.when(upper)(functools.partial(each_chunk, to_sources))
    next_rows()

    @pl.when(lower)
    def _():
        each_chunk(functools.partial(second, 1))
        each_chunk(functools.partial(forward, 1))
        each_chunk(finish)

    def second_size(forwards):
        return 16 * A8 + K * forwards * A8 + 60 * B4

    first_a_size, first_b_size = 15 * B4, 7 * ROWS2
    all_size = first_a_size + first_b_size + 3 * UV128 + 3 * DX64
    for chosen, forwards in ((inner, 4), (jnp.logical_not(inner), 2)):
        @pl.when(chosen)
        def _(forwards=forwards):
            arrived_kib(all_size + second_size(forwards), snd.at[ALL])

        @pl.when(chosen & lower)
        def _(forwards=forwards):
            arrived_kib(first_a_size + second_size(forwards), snd.at[LOWER])

    @pl.when(lower)
    def _():
        arrived(sel_in, snd.at[SEL])

    @pl.when(upper)
    def _():
        arrived_kib(8 * ROWS2 + 12 * DX64 + 28 * A8 + 60 * B4 + 16 * B4 + 7 * ROWS2 + 56, snd.at[UPPER])
        arrived(m_in, snd.at[MM])


def body(cotangent, routes, gates, *others):
    hbm = pl.BlockSpec(memory_space=pl.ANY)
    dma = pltpu.SemaphoreType.DMA
    vmem = pltpu.VMEM
    return pl.pallas_call(
        kernel,
        out_shape=vmem((1, HID, Q), F32),
        in_specs=[hbm] * 8,
        out_specs=pl.BlockSpec(memory_space=vmem),
        scratch_shapes=[
            vmem((TOK, D), BF),
            vmem((2, 8, TOK), jnp.int32),
            vmem((2, 8, TOK), BF),
            vmem((HID, Q), BF),
            vmem((Q, 2 * HID), BF),
            vmem((Q, HID), BF),
            vmem((2 * HID, Q), BF),
            vmem((3, 8, TOK), BF),
            vmem((8, TOK), BF),
            vmem((2, 4, 2, 2, HA), BF),
            vmem((2, 2, 2, 4 * HB), BF),
            vmem((8, D), F32),
            vmem((4, 2, 2, HA), F32),
            vmem((4, 2, 2, HA), F32),
            vmem((8, 8), F32),
            vmem((8, 8), F32),
            vmem((4, 2, 32, 2, HID), BF),
            vmem((2, 32, 2, HID), BF),
            vmem((4, TOK, HID), BF),
            vmem((K, 2, 64, HID), F32),
            vmem((2, K, HID, 64), BF),
            vmem((1536, 4, 128), BF),
            vmem((2, K, 4, 2, 2, HA), BF),
            vmem((2, K, 2, 8, HA), BF),
            vmem((2, 4, 2, 2, 4 * HB), BF),
            vmem((2, K, 8, 8, HA), BF),
            vmem((2, K, 2, 4, 4, 2, HB), BF),
            vmem((2, K, 64, HB), BF),
            vmem((K, 4, 64, HID), BF),
            vmem((K, 8, 8, HA), BF),
            vmem((K, 2, 4, 4, 2, HB), BF),
            vmem((K, 3, 8, HA), BF),
            vmem((K, 6, 2, 2, HB), BF),
            vmem((K, 2, 8, HA), BF),
            vmem((K, 6, 2, 2, HB), BF),
            vmem((K, 8, 8, HA), BF),
            vmem((K, 16, 2, 2, HB), BF),
            vmem((K, 4, 2, 2, HA), BF),
            vmem((K, 2, 2, 4 * HB), BF),
            vmem((16, 2, 2, HA), BF),
            vmem((8, 2, 4 * HB), BF),
            dma((5,)),
            dma((5,)),
            dma((2, K)),
            dma((2, K)),
            dma((2, K)),
            dma((K,)),
            dma((K,)),
            dma((K,)),
            dma,
            dma,
            dma((5,)),
            pltpu.SemaphoreType.REGULAR,
            dma((2, K)),
            dma((2, K)),
            dma((K,)),
            dma((K,)),
        ],
        compiler_params=pltpu.CompilerParams(collective_id=0, has_side_effects=True),
        name="cooldown",
    )(cotangent, jnp.swapaxes(routes, 2, 3), jnp.swapaxes(gates, 2, 3), *others)


def solution(mesh):
    in_specs = (
        P("pipe", ("dp", "expert"), None),
        P("pipe", None, ("dp", "expert"), None),
        P("pipe", None, ("dp", "expert"), None),
        P("pipe", None, "dp", None, None, "expert"),
        P("pipe", None, "dp", None, None, "expert"),
        P("pipe", None, "expert"),
        P("pipe", None, "expert"),
        P("pipe", "expert", None),
    )
    out_specs = P("pipe", "expert", "dp")
    return jax.shard_map(body, mesh=mesh, in_specs=in_specs, out_specs=out_specs, check_vma=False)
```
